32 devices in a mesh: fsdp: 8 (over y, x, core), dp: 4 (over z).
Axes of the slice: x: 2, y: 2, z: 4, core: 2. Of those that a mesh axis runs over, the one named last changes fastest.
Arguments:
- incoming_word_states: bfloat16 [512, 64, 768], P(('fsdp', 'dp')), may hold values from -6 to 6
- sentence_number_per_word: int32 [512, 64], P(('fsdp', 'dp')), may hold values from 0 to 3, never falling along the last dimension, each value on 1 to 28 neighbouring positions
- described_picture: int32 [2048], P(('fsdp', 'dp')), may hold values from 0 to 255
- lookup_matrices: bfloat16 [768, 2304], P('fsdp'), may hold values from -0.21875 to 0.21875
- mixer_exit_matrix: bfloat16 [768, 768], P('fsdp'), may hold values from -0.875 to 0.875
- widening_matrix: bfloat16 [768, 3072], P('fsdp'), may hold values from -0.21875 to 0.21875
- narrowing_matrix: bfloat16 [3072, 768], P('fsdp'), may hold values from -0.109375 to 0.109375
- normalizer_multipliers: bfloat16 [2, 768], P(None, 'fsdp'), may hold values from 0.5 to 1.5
- word_offsets: bfloat16 [6, 768], P(None, 'fsdp'), may hold values from -1.25 to 1.25
- widened_offset: bfloat16 [3072], P('fsdp'), may hold values from -1.25 to 1.25
- picture_patches: bfloat16 [256, 50, 768], P(('fsdp', 'dp')), may hold values from -6 to 6
- picture_lookup_matrices: bfloat16 [768, 2304], replicated, may hold values from -0.21875 to 0.21875
- picture_mixer_exit_matrix: bfloat16 [768, 768], replicated, may hold values from -1.5 to 1.5
- picture_widening_matrix: bfloat16 [768, 3072], replicated, may hold values from -0.21875 to 0.21875
- picture_narrowing_matrix: bfloat16 [3072, 768], replicated, may hold values from -0.109375 to 0.109375
- picture_normalizer_multipliers: bfloat16 [2, 768], replicated, may hold values from 0.5 to 1.5
- picture_offsets: bfloat16 [6, 768], replicated, may hold values from -1.25 to 1.25
- picture_widened_offset: bfloat16 [3072], replicated, may hold values from -1.25 to 1.25
- sharpness_coefficient: float32 [1], replicated, may hold values from 0.5 to 2
- objective_offset: float32 [1], replicated, may hold values from -3 to -1
Outputs:
- grad_qkv: float32 [768, 2304], P('fsdp')
- grad_out: float32 [768, 768], P('fsdp')
- grad_up: float32 [768, 3072], P('fsdp')
- grad_down: float32 [3072, 768], P('fsdp')
- grad_gains: float32 [2, 768], P(None, 'fsdp')
- grad_biases: float32 [6, 768], P(None, 'fsdp')
- grad_up_bias: float32 [3072], P('fsdp')
- grad_input: bfloat16 [512, 64, 768], P(('fsdp', 'dp'))
- loss: float32 [2048], P(('fsdp', 'dp'))
The draws below stay inside these ranges and needn't reach their ends.
Inputs may be any that keep to these rules, and one draw needn't show every extreme that they name: `sentence_number_per_word`: in each text row the segment ids number its 4 captions in order, never falling; every caption has at least one token. described_picture(r * 4 + c) is the image of the caption with segment id c in text row r.
All inputs are finite; a program needn't handle non-finite values.
Results may differ from the reference program's by a relative error of at most 0.011.
Values may be sent and summed in bfloat16 or wider, within the bound.
A program may use at most 192 MiB of HBM per device.

```python
import math
import jax
import jax.numpy as jnp
import numpy as np
from jax import lax

EMBED_SIZE = 768
HEAD_DIM = 64
FF = 3072
SEQ = 64
CAPS = 4
MOST = 28
IMG_SEQ = 50
TROWS = 512
CAPTIONS = 2048
IMAGES = 256


def place_ends(drawn, rng, least, top_value):
    dims = drawn.shape
    index_at = [jax.random.randint(jax.random.fold_in(rng, axis), (), 0, dims[axis]) for axis in range(len(dims))]
    drawn = drawn.at[tuple(index_at)].set(least)
    longest = dims.index(max(dims))
    index_at[longest] = (index_at[longest] + 1) % dims[longest]
    return drawn.at[tuple(index_at)].set(top_value)


def level_of(own_key, shape, cuts, least, largest):
    def one(axis_at, shards_of):
        heights = jax.random.uniform(jax.random.fold_in(jax.random.fold_in(own_key, 6), axis_at), (shards_of,), jnp.float32, least / len(cuts), largest / len(cuts))
        return jnp.repeat(jnp.exp(heights), shape[axis_at] // shards_of).reshape((-1,) + (1,) * (len(shape) - axis_at - 1))

    level = one(*cuts[0])
    for cut in cuts[1:]:
        level = level * one(*cut)
    return level


def split_up(number_of, total, reach, skew):
    weights = [(1 << 20) // math.isqrt(standing ** skew) + 1 for standing in range(2, number_of + 1)]
    rest, given = total - reach - (number_of - 1), [1] * (number_of - 1)
    while rest > 0:
        candidates = [i for i in range(number_of - 1) if given[i] < reach]
        pool, left = sum([weights[i] for i in candidates]), rest
        for i in candidates:
            extra = min(reach - given[i], max(1, left * weights[i] // pool), rest)
            given[i] = given[i] + extra
            rest = rest - extra
    return np.array([reach] + given)


def uneven(own_key, number_of, total, most, lean):
    if number_of == 2:
        one = jax.random.randint(own_key, (), max(1, total - most), min(most, total - 1) + 1)
        return jnp.stack([one, total - one])
    sizes = jnp.asarray(split_up(number_of, total, most, lean), jnp.int32)
    pairs = (number_of - 1) // 2
    giver, sink = sizes[1:1 + 2 * pairs:2], sizes[2:2 + 2 * pairs:2]
    margin = jnp.minimum(giver - 1, most - sink)
    shifted = jax.random.randint(jax.random.fold_in(own_key, 1), (pairs,), 0, 1 << 20) % (margin + 1)
    sizes = sizes.at[1:1 + 2 * pairs:2].set(giver - shifted).at[2:2 + 2 * pairs:2].set(sink + shifted)
    return sizes[jax.random.permutation(jax.random.fold_in(own_key, 2), number_of)]


def gaussian(key, shape, scale, reach, cuts=(), kind=jnp.bfloat16):
    level = level_of(key, shape, cuts, -0.22, 0.18) if cuts else 1.0
    values = jax.random.normal(key, shape, jnp.float32) * scale * level
    return jnp.minimum(jnp.maximum(values, -reach), reach).astype(kind)


def setup_inputs(seed: int = 0) -> dict:
    key_list = jax.random.split(jax.random.key(seed), 21)
    incoming_word_states = gaussian(key_list[0], (TROWS, SEQ, EMBED_SIZE), 1.0, 6.0, ((0, 32),))
    sentence_number_per_word = jax.vmap(lambda own: jnp.searchsorted(jnp.cumsum(uneven(own, CAPS, SEQ, MOST, 0)), jnp.arange(SEQ), side="right"))(jax.random.split(key_list[1], TROWS)).reshape((TROWS, SEQ)).astype(jnp.int32)
    described_picture = place_ends(jax.random.randint(key_list[2], (CAPTIONS,), 0, IMAGES), jax.random.fold_in(key_list[2], 1), 0, IMAGES - 1).astype(jnp.int32)
    lookup_matrices = gaussian(key_list[3], (EMBED_SIZE, 3 * EMBED_SIZE), EMBED_SIZE ** -0.5, 0.21875, ((0, 8),))
    mixer_exit_matrix = gaussian(key_list[4], (EMBED_SIZE, EMBED_SIZE), (EMBED_SIZE // 16) ** -0.5, 0.875, ((0, 8),))
    widening_matrix = gaussian(key_list[5], (EMBED_SIZE, FF), EMBED_SIZE ** -0.5, 0.21875, ((0, 8),))
    narrowing_matrix = gaussian(key_list[6], (FF, EMBED_SIZE), FF ** -0.5, 0.109375, ((0, 8),))
    normalizer_multipliers = jnp.clip(1.0 + 0.1 * jax.random.normal(key_list[7], (2, EMBED_SIZE), jnp.float32), 0.5, 1.5).astype(jnp.bfloat16)
    word_offsets = gaussian(key_list[8], (6, EMBED_SIZE), 0.2, 1.25, ((1, 8),))
    widened_offset = gaussian(key_list[9], (FF,), 0.2, 1.25, ((0, 8),))
    picture_patches = gaussian(key_list[10], (IMAGES, IMG_SEQ, EMBED_SIZE), 1.0, 6.0, ((0, 32),))
    picture_lookup_matrices = gaussian(key_list[11], (EMBED_SIZE, 3 * EMBED_SIZE), EMBED_SIZE ** -0.5, 0.21875)
    picture_mixer_exit_matrix = gaussian(key_list[12], (EMBED_SIZE, EMBED_SIZE), (EMBED_SIZE // 48) ** -0.5, 1.5)
    picture_widening_matrix = gaussian(key_list[13], (EMBED_SIZE, FF), EMBED_SIZE ** -0.5, 0.21875)
    picture_narrowing_matrix = gaussian(key_list[14], (FF, EMBED_SIZE), FF ** -0.5, 0.109375)
    picture_normalizer_multipliers = jnp.clip(1.0 + 0.1 * jax.random.normal(key_list[15], (2, EMBED_SIZE), jnp.float32), 0.5, 1.5).astype(jnp.bfloat16)
    picture_offsets = gaussian(key_list[16], (6, EMBED_SIZE), 0.2, 1.25)
    picture_widened_offset = gaussian(key_list[17], (FF,), 0.2, 1.25)
    sharpness_coefficient = jnp.clip(jnp.exp(jax.random.uniform(key_list[18], (1,), jnp.float32, math.log(0.5), math.log(2.0))), 0.5, 2.0)
    objective_offset = jnp.clip(jax.random.uniform(key_list[19], (1,), jnp.float32, -3.0, -1.0), -3.0, -1.0)
    return {"incoming_word_states": incoming_word_states, "sentence_number_per_word": sentence_number_per_word, "described_picture": described_picture, "lookup_matrices": lookup_matrices, "mixer_exit_matrix": mixer_exit_matrix, "widening_matrix": widening_matrix, "narrowing_matrix": narrowing_matrix, "normalizer_multipliers": normalizer_multipliers, "word_offsets": word_offsets, "widened_offset": widened_offset, "picture_patches": picture_patches, "picture_lookup_matrices": picture_lookup_matrices, "picture_mixer_exit_matrix": picture_mixer_exit_matrix, "picture_widening_matrix": picture_widening_matrix, "picture_narrowing_matrix": picture_narrowing_matrix, "picture_normalizer_multipliers": picture_normalizer_multipliers, "picture_offsets": picture_offsets, "picture_widened_offset": picture_widened_offset, "sharpness_coefficient": sharpness_coefficient, "objective_offset": objective_offset}


@jax.custom_vjp
def low(v):
    return lax.optimization_barrier(v.astype(jnp.bfloat16)).astype(jnp.float32)

@jax.custom_vjp
def low_back(v):
    return v

def low_keep(v):
    return (low(v), None)

def low_pass(kept, grad):
    return (grad,)

def back_keep(v):
    return (v, None)

def back_low(kept, grad):
    return (low(grad),)
low.defvjp(low_keep, low_pass)
low_back.defvjp(back_keep, back_low)
highest = lax.Precision.HIGHEST

def matmul(left, right):
    return jnp.dot(left, right, precision=highest, preferred_element_type=jnp.float32)

def layer_norm(values, gain, shift):
    centred = values - lax.optimization_barrier(jnp.mean(values, axis=-1, keepdims=True))
    scaled = centred * lax.rsqrt(lax.optimization_barrier(jnp.mean(centred * centred, axis=-1, keepdims=True)) + 1e-06)
    return scaled * gain + shift

def unit_rows(values):
    return values * lax.rsqrt(lax.optimization_barrier(jnp.mean(values * values, axis=-1, keepdims=True)) + 1e-06)

def block(flat, rows, length, mask, qkv_w, out_w, up_w, down_w, gains, biases, up_b):
    channel_count = flat.shape[-1]
    heads = channel_count // HEAD_DIM
    scale = 1.0 / math.sqrt(HEAD_DIM)
    normed = low(layer_norm(flat, gains[0], biases[4]))
    mixed = matmul(normed, qkv_w)
    query = low(low_back((mixed[:, :channel_count] + biases[0]) * scale)).reshape(rows, length, heads, HEAD_DIM)
    key_part = low(low_back(mixed[:, channel_count:2 * channel_count])).reshape(rows, length, heads, HEAD_DIM)
    value_part = low(low_back(mixed[:, 2 * channel_count:] + biases[1])).reshape(rows, length, heads, HEAD_DIM)
    scores = low_back(jnp.einsum('rqhd,rkhd->rhqk', query, key_part, precision=highest))
    if mask is not None:
        scores = jnp.where(mask[:, None], scores, -1e+30)
    probs = low(jax.nn.softmax(scores, axis=-1))
    attended = low(low_back(jnp.einsum('rhqk,rkhd->rqhd', probs, value_part, precision=highest)))
    attended = attended.reshape(rows * length, channel_count)
    middle = flat + low_back(matmul(attended, out_w) + biases[2])
    normed_two = low(layer_norm(middle, gains[1], biases[5]))
    hidden = low_back(matmul(normed_two, up_w) + up_b)
    active = low(jax.nn.gelu(hidden, approximate=False))
    return middle + low_back(matmul(active, down_w) + biases[3])

def reference(incoming_word_states, sentence_number_per_word, described_picture, lookup_matrices, mixer_exit_matrix, widening_matrix, narrowing_matrix, normalizer_multipliers, word_offsets, widened_offset, picture_patches, picture_lookup_matrices, picture_mixer_exit_matrix, picture_widening_matrix, picture_narrowing_matrix, picture_normalizer_multipliers, picture_offsets, picture_widened_offset, sharpness_coefficient, objective_offset):
    image_params = tuple((a.astype(jnp.float32) for a in (picture_lookup_matrices, picture_mixer_exit_matrix, picture_widening_matrix, picture_narrowing_matrix, picture_normalizer_multipliers, picture_offsets, picture_widened_offset)))
    image_flat = picture_patches.astype(jnp.float32).reshape(IMAGES * IMG_SEQ, EMBED_SIZE)
    image_result = block(image_flat, IMAGES, IMG_SEQ, None, *image_params)
    image_embed = low(unit_rows(image_result.reshape(IMAGES, IMG_SEQ, EMBED_SIZE)[:, 0, :]))

    def text_group(rows_in, rows_seg, params):
        rows = rows_in.shape[0]
        mask = rows_seg[:, :, None] == rows_seg[:, None, :]
        result = block(rows_in.reshape(rows * SEQ, EMBED_SIZE), rows, SEQ, mask, *params).reshape(rows, SEQ, EMBED_SIZE)
        member = (rows_seg[:, :, None] == jnp.arange(CAPS, dtype=jnp.int32)).astype(jnp.float32)
        counts = lax.optimization_barrier(jnp.sum(member, axis=1))
        pooled = jnp.einsum('rsc,rsd->rcd', member, result, precision=highest) / counts[:, :, None]
        return pooled.reshape(rows * CAPS, EMBED_SIZE)

    def objective(text_in, params):
        group = math.gcd(TROWS, 64)
        count = TROWS // group
        stacked = (text_in.reshape(count, group, SEQ, EMBED_SIZE), sentence_number_per_word.reshape(count, group, SEQ))

        def one_group(pieces):
            return text_group(pieces[0], pieces[1], params)
        pooled = lax.map(jax.checkpoint(one_group), stacked)
        embed = low(unit_rows(pooled.reshape(CAPTIONS, EMBED_SIZE)))
        unscaled_similarity = low_back(matmul(embed, image_embed.T))
        match_similarity = sharpness_coefficient[0] * unscaled_similarity / math.sqrt(EMBED_SIZE) + objective_offset[0]
        labels = jnp.where(described_picture[:, None] == jnp.arange(IMAGES, dtype=jnp.int32)[None, :], 1.0, -1.0)
        terms = jax.nn.softplus(-labels * match_similarity)
        per_caption = lax.optimization_barrier(jnp.sum(terms, axis=1)) / IMAGES
        return (jnp.sum(terms), per_caption)
    text_params = tuple((a.astype(jnp.float32) for a in (lookup_matrices, mixer_exit_matrix, widening_matrix, narrowing_matrix, normalizer_multipliers, word_offsets, widened_offset)))
    total, pullback, per_caption = jax.vjp(objective, incoming_word_states.astype(jnp.float32), text_params, has_aux=True)
    grad_text, grads = pullback(jnp.ones((), jnp.float32))
    return (grads[0], grads[1], grads[2], grads[3], grads[4], grads[5], grads[6], grad_text.astype(jnp.bfloat16), per_caption)
```

```python
import math

import jax
import jax.numpy as jnp
from jax import lax
from jax.sharding import PartitionSpec as P

HEAD_DIM = 64
CAPS = 4


def layer_norm(values, gain, shift):
    centred = values - jnp.mean(values, axis=-1, keepdims=True)
    inverse = lax.rsqrt(jnp.mean(centred * centred, axis=-1, keepdims=True) + 1e-06)
    scaled = centred * inverse
    return (scaled * gain + shift, scaled, inverse)


def norm_back(grad_scaled, scaled, inverse):
    first_mean = jnp.mean(grad_scaled, axis=-1, keepdims=True)
    second_mean = jnp.mean(grad_scaled * scaled, axis=-1, keepdims=True)
    return inverse * (grad_scaled - first_mean - scaled * second_mean)


def gelu_exact(values):
    return jax.nn.gelu(values, approximate=False)


def forward_block(flat, rows, length, mask, weights):
    qkv_w, out_w, up_w, down_w, gains_low, biases_low, up_b = weights
    gains = gains_low.astype(jnp.float32)
    biases = biases_low.astype(jnp.float32)
    channel_count = flat.shape[-1]
    heads = channel_count // HEAD_DIM
    scale = 1.0 / math.sqrt(HEAD_DIM)
    first, scaled_one, inverse_one = layer_norm(flat, gains[0], biases[4])
    first_low = first.astype(jnp.bfloat16)
    mixed = jnp.dot(first_low, qkv_w, preferred_element_type=jnp.float32)
    query = (
        ((mixed[:, :channel_count] + biases[0]) * scale)
        .astype(jnp.bfloat16)
        .reshape(rows, length, heads, HEAD_DIM)
    )
    key_low = (
        mixed[:, channel_count : 2 * channel_count]
        .astype(jnp.bfloat16)
        .reshape(rows, length, heads, HEAD_DIM)
    )
    value_low = (
        (mixed[:, 2 * channel_count :] + biases[1])
        .astype(jnp.bfloat16)
        .reshape(rows, length, heads, HEAD_DIM)
    )
    scores = jnp.einsum("rqhd,rkhd->rhqk", query, key_low, preferred_element_type=jnp.float32)
    if mask is not None:
        scores = jnp.where(mask[:, None], scores, -1e30)
    probs = jax.nn.softmax(scores, axis=-1)
    probs_low = probs.astype(jnp.bfloat16)
    attended = jnp.einsum(
        "rhqk,rkhd->rqhd", probs_low, value_low, preferred_element_type=jnp.float32
    )
    attended = attended.astype(jnp.bfloat16).reshape(rows * length, channel_count)
    middle = flat + (jnp.dot(attended, out_w, preferred_element_type=jnp.float32) + biases[2])
    second, scaled_two, inverse_two = layer_norm(middle, gains[1], biases[5])
    second_low = second.astype(jnp.bfloat16)
    hidden = jnp.dot(second_low, up_w, preferred_element_type=jnp.float32) + up_b.astype(
        jnp.float32
    )
    active = gelu_exact(hidden).astype(jnp.bfloat16)
    output = middle + (jnp.dot(active, down_w, preferred_element_type=jnp.float32) + biases[3])
    saved = (
        scaled_one,
        inverse_one,
        first_low,
        query,
        key_low,
        value_low,
        probs,
        probs_low,
        attended,
        scaled_two,
        inverse_two,
        second_low,
        hidden,
        active,
    )
    return (output, saved)


def backward_block(grad_output, saved, weights, rows, length):
    qkv_w, out_w, up_w, down_w, gains_low, biases_low, up_b = weights
    gains = gains_low.astype(jnp.float32)
    (
        scaled_one,
        inverse_one,
        first_low,
        query,
        key_low,
        value_low,
        probs,
        probs_low,
        attended,
        scaled_two,
        inverse_two,
        second_low,
        hidden,
        active,
    ) = saved
    channel_count = grad_output.shape[-1]
    heads = channel_count // HEAD_DIM
    scale = 1.0 / math.sqrt(HEAD_DIM)
    count = rows * length
    down_grad = grad_output.astype(jnp.bfloat16)
    grad_down_bias = jnp.sum(down_grad, axis=0, dtype=jnp.float32)
    grad_down_w = jnp.einsum("nf,nd->fd", active, down_grad, preferred_element_type=jnp.float32)
    active_grad = jnp.einsum("nd,fd->nf", down_grad, down_w, preferred_element_type=jnp.float32)
    gelu_back = jax.vjp(gelu_exact, hidden)[1]
    hidden_grad = gelu_back(active_grad)[0].astype(jnp.bfloat16)
    grad_up_bias = jnp.sum(hidden_grad, axis=0, dtype=jnp.float32)
    grad_up_w = jnp.einsum("nd,nf->df", second_low, hidden_grad, preferred_element_type=jnp.float32)
    second_grad = jnp.einsum("nf,df->nd", hidden_grad, up_w, preferred_element_type=jnp.float32)
    grad_gain_two = jnp.sum(second_grad * scaled_two, axis=0)
    grad_shift_two = jnp.sum(second_grad, axis=0)
    middle_grad = grad_output + norm_back(second_grad * gains[1], scaled_two, inverse_two)
    branch_grad = middle_grad.astype(jnp.bfloat16)
    grad_out_bias = jnp.sum(branch_grad, axis=0, dtype=jnp.float32)
    grad_out_w = jnp.einsum("nd,ne->de", attended, branch_grad, preferred_element_type=jnp.float32)
    attended_grad = jnp.einsum("ne,de->nd", branch_grad, out_w, preferred_element_type=jnp.float32)
    attended_grad = attended_grad.astype(jnp.bfloat16).reshape(rows, length, heads, HEAD_DIM)
    probs_grad = jnp.einsum(
        "rqhd,rkhd->rhqk", attended_grad, value_low, preferred_element_type=jnp.float32
    )
    value_grad = jnp.einsum(
        "rhqk,rqhd->rkhd", probs_low, attended_grad, preferred_element_type=jnp.float32
    ).astype(jnp.bfloat16)
    score_grad = probs * (probs_grad - jnp.sum(probs * probs_grad, axis=-1, keepdims=True))
    score_grad = score_grad.astype(jnp.bfloat16)
    query_grad = jnp.einsum(
        "rhqk,rkhd->rqhd", score_grad, key_low, preferred_element_type=jnp.float32
    ).astype(jnp.bfloat16)
    key_grad = jnp.einsum(
        "rhqk,rqhd->rkhd", score_grad, query, preferred_element_type=jnp.float32
    ).astype(jnp.bfloat16)
    query_flat = query_grad.reshape(count, channel_count) * scale
    value_flat = value_grad.reshape(count, channel_count)
    mixed_grad = jnp.concatenate(
        [query_flat, key_grad.reshape(count, channel_count), value_flat], axis=1
    )
    grad_query_bias = jnp.sum(query_flat, axis=0, dtype=jnp.float32)
    grad_value_bias = jnp.sum(value_flat, axis=0, dtype=jnp.float32)
    grad_qkv_w = jnp.einsum("nd,ne->de", first_low, mixed_grad, preferred_element_type=jnp.float32)
    first_grad = jnp.einsum("ne,de->nd", mixed_grad, qkv_w, preferred_element_type=jnp.float32)
    grad_gain_one = jnp.sum(first_grad * scaled_one, axis=0)
    grad_shift_one = jnp.sum(first_grad, axis=0)
    input_grad = middle_grad + norm_back(first_grad * gains[0], scaled_one, inverse_one)
    grad_gains = jnp.stack([grad_gain_one, grad_gain_two])
    grad_biases = jnp.stack(
        [
            grad_query_bias,
            grad_value_bias,
            grad_out_bias,
            grad_down_bias,
            grad_shift_one,
            grad_shift_two,
        ]
    )
    return (
        input_grad,
        (grad_qkv_w, grad_out_w, grad_up_w, grad_down_w, grad_gains, grad_biases, grad_up_bias),
    )


def image_first_token(patches, qkv_w, out_w, up_w, down_w, gains_low, biases_low, up_b):
    rows, length, channel_count = patches.shape
    gains = gains_low.astype(jnp.float32)
    biases = biases_low.astype(jnp.float32)
    heads = channel_count // HEAD_DIM
    scale = 1.0 / math.sqrt(HEAD_DIM)
    first_low = layer_norm(patches.astype(jnp.float32), gains[0], biases[4])[0].astype(jnp.bfloat16)
    flat_low = first_low.reshape(rows * length, channel_count)
    query = (
        (jnp.dot(first_low[:, 0], qkv_w[:, :channel_count], preferred_element_type=jnp.float32) + biases[0])
        * scale
    ).astype(jnp.bfloat16).reshape(rows, heads, HEAD_DIM)
    mixed = jnp.dot(flat_low, qkv_w[:, channel_count:], preferred_element_type=jnp.float32)
    key_low = mixed[:, :channel_count].astype(jnp.bfloat16).reshape(rows, length, heads, HEAD_DIM)
    value_low = (
        (mixed[:, channel_count:] + biases[1]).astype(jnp.bfloat16).reshape(rows, length, heads, HEAD_DIM)
    )
    scores = jnp.einsum("rhd,rkhd->rhk", query, key_low, preferred_element_type=jnp.float32)
    probs_low = jax.nn.softmax(scores, axis=-1).astype(jnp.bfloat16)
    attended = jnp.einsum("rhk,rkhd->rhd", probs_low, value_low, preferred_element_type=jnp.float32)
    attended = attended.astype(jnp.bfloat16).reshape(rows, channel_count)
    middle = patches[:, 0].astype(jnp.float32) + (
        jnp.dot(attended, out_w, preferred_element_type=jnp.float32) + biases[2]
    )
    second_low = layer_norm(middle, gains[1], biases[5])[0].astype(jnp.bfloat16)
    hidden = jnp.dot(second_low, up_w, preferred_element_type=jnp.float32) + up_b.astype(jnp.float32)
    active = gelu_exact(hidden).astype(jnp.bfloat16)
    return middle + (jnp.dot(active, down_w, preferred_element_type=jnp.float32) + biases[3])


def per_device(
    incoming_word_states,
    sentence_number_per_word,
    described_picture,
    lookup_matrices,
    mixer_exit_matrix,
    widening_matrix,
    narrowing_matrix,
    normalizer_multipliers,
    word_offsets,
    widened_offset,
    picture_patches,
    picture_lookup_matrices,
    picture_mixer_exit_matrix,
    picture_widening_matrix,
    picture_narrowing_matrix,
    picture_normalizer_multipliers,
    picture_offsets,
    picture_widened_offset,
    sharpness_coefficient,
    objective_offset,
):
    rows, length, channel_count = incoming_word_states.shape
    whole = (
        lax.all_gather(lookup_matrices, "fsdp", axis=0, tiled=True),
        lax.all_gather(mixer_exit_matrix, "fsdp", axis=0, tiled=True),
        lax.all_gather(widening_matrix, "fsdp", axis=0, tiled=True),
        lax.all_gather(narrowing_matrix, "fsdp", axis=0, tiled=True),
        lax.all_gather(normalizer_multipliers, "fsdp", axis=1, tiled=True),
        lax.all_gather(word_offsets, "fsdp", axis=1, tiled=True),
        lax.all_gather(widened_offset, "fsdp", axis=0, tiled=True),
    )
    image_rows, image_length = (picture_patches.shape[0], picture_patches.shape[1])
    image_token = image_first_token(
        picture_patches,
        picture_lookup_matrices,
        picture_mixer_exit_matrix,
        picture_widening_matrix,
        picture_narrowing_matrix,
        picture_normalizer_multipliers,
        picture_offsets,
        picture_widened_offset,
    )
    image_embed = (
        image_token * lax.rsqrt(jnp.mean(image_token * image_token, axis=-1, keepdims=True) + 1e-06)
    ).astype(jnp.bfloat16)
    mask = sentence_number_per_word[:, :, None] == sentence_number_per_word[:, None, :]
    flat = incoming_word_states.astype(jnp.float32).reshape(rows * length, channel_count)
    text_result, saved = forward_block(flat, rows, length, mask, whole)
    member = (sentence_number_per_word[:, :, None] == jnp.arange(CAPS, dtype=jnp.int32)).astype(
        jnp.float32
    )
    counts = jnp.sum(member, axis=1)[:, :, None]
    pooled = (
        jnp.einsum(
            "rsc,rsd->rcd",
            member,
            text_result.reshape(rows, length, channel_count),
            precision=lax.Precision.HIGHEST,
        )
        / counts
    )
    pooled = pooled.reshape(rows * CAPS, channel_count)
    inverse = lax.rsqrt(jnp.mean(pooled * pooled, axis=-1, keepdims=True) + 1e-06)
    embed = pooled * inverse
    embed_low = embed.astype(jnp.bfloat16)
    multiplier_amount = sharpness_coefficient[0] / math.sqrt(channel_count)
    piece = lax.all_gather(image_embed, ("fsdp", "dp"), axis=0, tiled=True)
    unscaled_similarity = jnp.einsum(
        "cd,nd->cn", embed_low, piece, preferred_element_type=jnp.float32
    )
    match_similarity = multiplier_amount * unscaled_similarity + objective_offset[0]
    positive = described_picture[:, None] == jnp.arange(piece.shape[0], dtype=jnp.int32)[None, :]
    labels = jnp.where(positive, 1.0, -1.0)
    total = jnp.sum(jax.nn.softplus(-labels * match_similarity), axis=1)
    slope = (
        (jax.nn.sigmoid(match_similarity) - positive.astype(jnp.float32)) * multiplier_amount
    ).astype(jnp.bfloat16)
    grad_embed = jnp.einsum("cn,nd->cd", slope, piece, preferred_element_type=jnp.float32)
    images_all = image_rows * lax.axis_size("fsdp") * lax.axis_size("dp")
    loss = total / images_all
    pooled_grad = inverse * (
        grad_embed - embed * jnp.mean(grad_embed * embed, axis=-1, keepdims=True)
    )
    per_caption = pooled_grad.reshape(rows, CAPS, channel_count) / counts
    token_grad = jnp.einsum(
        "rsc,rcd->rsd", member, per_caption, precision=lax.Precision.HIGHEST
    ).reshape(rows * length, channel_count)
    input_grad, grads = backward_block(token_grad, saved, whole, rows, length)
    owned = [
        lax.psum(
            lax.psum_scatter(piece_grad.astype(jnp.bfloat16), "fsdp", scatter_dimension=0, tiled=True), "dp"
        ).astype(jnp.float32)
        for piece_grad in grads[:4]
    ]
    small = jnp.concatenate([grads[4], grads[5], grads[6].reshape(-1, channel_count)], axis=0)
    small = lax.psum(small, ("fsdp", "dp"))
    place = lax.axis_index("fsdp")
    width = normalizer_multipliers.shape[1]
    columns = lax.dynamic_slice_in_dim(small[:8], place * width, width, axis=1)
    hidden_width = widened_offset.shape[0]
    hidden_part = lax.dynamic_slice_in_dim(small[8:].reshape(-1), place * hidden_width, hidden_width)
    summed = (*owned, columns[:2], columns[2:8], hidden_part)
    grad_input = input_grad.astype(jnp.bfloat16).reshape(rows, length, channel_count)
    return (
        summed[0],
        summed[1],
        summed[2],
        summed[3],
        summed[4],
        summed[5],
        summed[6],
        grad_input,
        loss,
    )


def solution(mesh):
    return jax.shard_map(
        per_device,
        mesh=mesh,
        in_specs=(
            P(("fsdp", "dp"), None, None),
            P(("fsdp", "dp"), None),
            P(("fsdp", "dp")),
            P("fsdp", None),
            P("fsdp", None),
            P("fsdp", None),
            P("fsdp", None),
            P(None, "fsdp"),
            P(None, "fsdp"),
            P("fsdp"),
            P(("fsdp", "dp"), None, None),
            P(),
            P(),
            P(),
            P(),
            P(),
            P(),
            P(),
            P(),
            P(),
        ),
        out_specs=(
            P("fsdp", None),
            P("fsdp", None),
            P("fsdp", None),
            P("fsdp", None),
            P(None, "fsdp"),
            P(None, "fsdp"),
            P("fsdp"),
            P(("fsdp", "dp"), None, None),
            P(("fsdp", "dp")),
        ),
        check_vma=False,
    )
```

```python
import math

import jax
import jax.numpy as jnp
from jax import lax
from jax.experimental import pallas as pl
from jax.experimental.pallas import tpu as pltpu
from jax.sharding import PartitionSpec as P

HEAD_DIM = 64
CAPS = 4


def layer_norm(values, gain, shift):
    centred = values - jnp.mean(values, axis=-1, keepdims=True)
    inverse = lax.rsqrt(jnp.mean(centred * centred, axis=-1, keepdims=True) + 1e-06)
    scaled = centred * inverse
    return (scaled * gain + shift, scaled, inverse)


def norm_back(grad_scaled, scaled, inverse):
    first_mean = jnp.mean(grad_scaled, axis=-1, keepdims=True)
    second_mean = jnp.mean(grad_scaled * scaled, axis=-1, keepdims=True)
    return inverse * (grad_scaled - first_mean - scaled * second_mean)


def gelu_exact(values):
    return jax.nn.gelu(values, approximate=False)


def forward_block(flat, rows, length, mask, weights):
    qkv_w, out_w, up_w, down_w, gains_low, biases_low, up_b = weights
    gains = gains_low.astype(jnp.float32)
    biases = biases_low.astype(jnp.float32)
    channel_count = flat.shape[-1]
    heads = channel_count // HEAD_DIM
    scale = 1.0 / math.sqrt(HEAD_DIM)
    first, scaled_one, inverse_one = layer_norm(flat, gains[0], biases[4])
    first_low = first.astype(jnp.bfloat16)
    mixed = jnp.dot(first_low, qkv_w, preferred_element_type=jnp.float32)
    query = (
        ((mixed[:, :channel_count] + biases[0]) * scale)
        .astype(jnp.bfloat16)
        .reshape(rows, length, heads, HEAD_DIM)
    )
    key_low = (
        mixed[:, channel_count : 2 * channel_count]
        .astype(jnp.bfloat16)
        .reshape(rows, length, heads, HEAD_DIM)
    )
    value_low = (
        (mixed[:, 2 * channel_count :] + biases[1])
        .astype(jnp.bfloat16)
        .reshape(rows, length, heads, HEAD_DIM)
    )
    scores = jnp.einsum("rqhd,rkhd->rhqk", query, key_low, preferred_element_type=jnp.float32)
    if mask is not None:
        scores = jnp.where(mask[:, None], scores, -1e30)
    probs = jax.nn.softmax(scores, axis=-1)
    probs_low = probs.astype(jnp.bfloat16)
    attended = jnp.einsum(
        "rhqk,rkhd->rqhd", probs_low, value_low, preferred_element_type=jnp.float32
    )
    attended = attended.astype(jnp.bfloat16).reshape(rows * length, channel_count)
    middle = flat + (jnp.dot(attended, out_w, preferred_element_type=jnp.float32) + biases[2])
    second, scaled_two, inverse_two = layer_norm(middle, gains[1], biases[5])
    second_low = second.astype(jnp.bfloat16)
    hidden = jnp.dot(second_low, up_w, preferred_element_type=jnp.float32) + up_b.astype(
        jnp.float32
    )
    active = gelu_exact(hidden).astype(jnp.bfloat16)
    output = middle + (jnp.dot(active, down_w, preferred_element_type=jnp.float32) + biases[3])
    saved = (
        scaled_one,
        inverse_one,
        first_low,
        query,
        key_low,
        value_low,
        probs,
        probs_low,
        attended,
        scaled_two,
        inverse_two,
        second_low,
        hidden,
        active,
    )
    return (output, saved)


def backward_block(grad_output, saved, weights, rows, length):
    qkv_w, out_w, up_w, down_w, gains_low, biases_low, up_b = weights
    gains = gains_low.astype(jnp.float32)
    (
        scaled_one,
        inverse_one,
        first_low,
        query,
        key_low,
        value_low,
        probs,
        probs_low,
        attended,
        scaled_two,
        inverse_two,
        second_low,
        hidden,
        active,
    ) = saved
    channel_count = grad_output.shape[-1]
    heads = channel_count // HEAD_DIM
    scale = 1.0 / math.sqrt(HEAD_DIM)
    count = rows * length
    down_grad = grad_output.astype(jnp.bfloat16)
    grad_down_bias = jnp.sum(down_grad, axis=0, dtype=jnp.float32)
    grad_down_w = jnp.einsum("nf,nd->fd", active, down_grad, preferred_element_type=jnp.float32)
    active_grad = jnp.einsum("nd,fd->nf", down_grad, down_w, preferred_element_type=jnp.float32)
    gelu_back = jax.vjp(gelu_exact, hidden)[1]
    hidden_grad = gelu_back(active_grad)[0].astype(jnp.bfloat16)
    grad_up_bias = jnp.sum(hidden_grad, axis=0, dtype=jnp.float32)
    grad_up_w = jnp.einsum("nd,nf->df", second_low, hidden_grad, preferred_element_type=jnp.float32)
    second_grad = jnp.einsum("nf,df->nd", hidden_grad, up_w, preferred_element_type=jnp.float32)
    grad_gain_two = jnp.sum(second_grad * scaled_two, axis=0)
    grad_shift_two = jnp.sum(second_grad, axis=0)
    middle_grad = grad_output + norm_back(second_grad * gains[1], scaled_two, inverse_two)
    branch_grad = middle_grad.astype(jnp.bfloat16)
    grad_out_bias = jnp.sum(branch_grad, axis=0, dtype=jnp.float32)
    grad_out_w = jnp.einsum("nd,ne->de", attended, branch_grad, preferred_element_type=jnp.float32)
    attended_grad = jnp.einsum("ne,de->nd", branch_grad, out_w, preferred_element_type=jnp.float32)
    attended_grad = attended_grad.astype(jnp.bfloat16).reshape(rows, length, heads, HEAD_DIM)
    probs_grad = jnp.einsum(
        "rqhd,rkhd->rhqk", attended_grad, value_low, preferred_element_type=jnp.float32
    )
    value_grad = jnp.einsum(
        "rhqk,rqhd->rkhd", probs_low, attended_grad, preferred_element_type=jnp.float32
    ).astype(jnp.bfloat16)
    score_grad = probs * (probs_grad - jnp.sum(probs * probs_grad, axis=-1, keepdims=True))
    score_grad = score_grad.astype(jnp.bfloat16)
    query_grad = jnp.einsum(
        "rhqk,rkhd->rqhd", score_grad, key_low, preferred_element_type=jnp.float32
    ).astype(jnp.bfloat16)
    key_grad = jnp.einsum(
        "rhqk,rqhd->rkhd", score_grad, query, preferred_element_type=jnp.float32
    ).astype(jnp.bfloat16)
    query_flat = query_grad.reshape(count, channel_count) * scale
    value_flat = value_grad.reshape(count, channel_count)
    mixed_grad = jnp.concatenate(
        [query_flat, key_grad.reshape(count, channel_count), value_flat], axis=1
    )
    grad_query_bias = jnp.sum(query_flat, axis=0, dtype=jnp.float32)
    grad_value_bias = jnp.sum(value_flat, axis=0, dtype=jnp.float32)
    grad_qkv_w = jnp.einsum("nd,ne->de", first_low, mixed_grad, preferred_element_type=jnp.float32)
    first_grad = jnp.einsum("ne,de->nd", mixed_grad, qkv_w, preferred_element_type=jnp.float32)
    grad_gain_one = jnp.sum(first_grad * scaled_one, axis=0)
    grad_shift_one = jnp.sum(first_grad, axis=0)
    input_grad = middle_grad + norm_back(first_grad * gains[0], scaled_one, inverse_one)
    grad_gains = jnp.stack([grad_gain_one, grad_gain_two])
    grad_biases = jnp.stack(
        [
            grad_query_bias,
            grad_value_bias,
            grad_out_bias,
            grad_down_bias,
            grad_shift_one,
            grad_shift_two,
        ]
    )
    return (
        input_grad,
        (grad_qkv_w, grad_out_w, grad_up_w, grad_down_w, grad_gains, grad_biases, grad_up_bias),
    )


def image_first_token(patches, qkv_w, out_w, up_w, down_w, gains_low, biases_low, up_b):
    rows, length, channel_count = patches.shape
    gains = gains_low.astype(jnp.float32)
    biases = biases_low.astype(jnp.float32)
    heads = channel_count // HEAD_DIM
    scale = 1.0 / math.sqrt(HEAD_DIM)
    first_low = layer_norm(patches.astype(jnp.float32), gains[0], biases[4])[0].astype(jnp.bfloat16)
    flat_low = first_low.reshape(rows * length, channel_count)
    query = (
        (jnp.dot(first_low[:, 0], qkv_w[:, :channel_count], preferred_element_type=jnp.float32) + biases[0])
        * scale
    ).astype(jnp.bfloat16).reshape(rows, heads, HEAD_DIM)
    mixed = jnp.dot(flat_low, qkv_w[:, channel_count:], preferred_element_type=jnp.float32)
    key_low = mixed[:, :channel_count].astype(jnp.bfloat16).reshape(rows, length, heads, HEAD_DIM)
    value_low = (
        (mixed[:, channel_count:] + biases[1]).astype(jnp.bfloat16).reshape(rows, length, heads, HEAD_DIM)
    )
    scores = jnp.einsum("rhd,rkhd->rhk", query, key_low, preferred_element_type=jnp.float32)
    probs_low = jax.nn.softmax(scores, axis=-1).astype(jnp.bfloat16)
    attended = jnp.einsum("rhk,rkhd->rhd", probs_low, value_low, preferred_element_type=jnp.float32)
    attended = attended.astype(jnp.bfloat16).reshape(rows, channel_count)
    middle = patches[:, 0].astype(jnp.float32) + (
        jnp.dot(attended, out_w, preferred_element_type=jnp.float32) + biases[2]
    )
    second_low = layer_norm(middle, gains[1], biases[5])[0].astype(jnp.bfloat16)
    hidden = jnp.dot(second_low, up_w, preferred_element_type=jnp.float32) + up_b.astype(jnp.float32)
    active = gelu_exact(hidden).astype(jnp.bfloat16)
    return middle + (jnp.dot(active, down_w, preferred_element_type=jnp.float32) + biases[3])


def per_device(
    incoming_word_states,
    sentence_number_per_word,
    described_picture,
    lookup_matrices,
    mixer_exit_matrix,
    widening_matrix,
    narrowing_matrix,
    normalizer_multipliers,
    word_offsets,
    widened_offset,
    picture_patches,
    picture_lookup_matrices,
    picture_mixer_exit_matrix,
    picture_widening_matrix,
    picture_narrowing_matrix,
    picture_normalizer_multipliers,
    picture_offsets,
    picture_widened_offset,
    sharpness_coefficient,
    objective_offset,
):
    rows, length, channel_count = incoming_word_states.shape
    whole = (
        lax.all_gather(lookup_matrices, "fsdp", axis=0, tiled=True),
        lax.all_gather(mixer_exit_matrix, "fsdp", axis=0, tiled=True),
        lax.all_gather(widening_matrix, "fsdp", axis=0, tiled=True),
        lax.all_gather(narrowing_matrix, "fsdp", axis=0, tiled=True),
        lax.all_gather(normalizer_multipliers, "fsdp", axis=1, tiled=True),
        lax.all_gather(word_offsets, "fsdp", axis=1, tiled=True),
        lax.all_gather(widened_offset, "fsdp", axis=0, tiled=True),
    )
    image_rows, image_length = (picture_patches.shape[0], picture_patches.shape[1])
    image_token = image_first_token(
        picture_patches,
        picture_lookup_matrices,
        picture_mixer_exit_matrix,
        picture_widening_matrix,
        picture_narrowing_matrix,
        picture_normalizer_multipliers,
        picture_offsets,
        picture_widened_offset,
    )
    image_embed = (
        image_token * lax.rsqrt(jnp.mean(image_token * image_token, axis=-1, keepdims=True) + 1e-06)
    ).astype(jnp.bfloat16)
    mask = sentence_number_per_word[:, :, None] == sentence_number_per_word[:, None, :]
    flat = incoming_word_states.astype(jnp.float32).reshape(rows * length, channel_count)
    text_result, saved = forward_block(flat, rows, length, mask, whole)
    member = (sentence_number_per_word[:, :, None] == jnp.arange(CAPS, dtype=jnp.int32)).astype(
        jnp.float32
    )
    counts = jnp.sum(member, axis=1)[:, :, None]
    pooled = (
        jnp.einsum(
            "rsc,rsd->rcd",
            member,
            text_result.reshape(rows, length, channel_count),
            precision=lax.Precision.HIGHEST,
        )
        / counts
    )
    pooled = pooled.reshape(rows * CAPS, channel_count)
    inverse = lax.rsqrt(jnp.mean(pooled * pooled, axis=-1, keepdims=True) + 1e-06)
    embed = pooled * inverse
    embed_low = embed.astype(jnp.bfloat16)
    multiplier_amount = sharpness_coefficient[0] / math.sqrt(channel_count)
    piece = lax.all_gather(image_embed, ("fsdp", "dp"), axis=0, tiled=True)
    unscaled_similarity = jnp.einsum(
        "cd,nd->cn", embed_low, piece, preferred_element_type=jnp.float32
    )
    match_similarity = multiplier_amount * unscaled_similarity + objective_offset[0]
    positive = described_picture[:, None] == jnp.arange(piece.shape[0], dtype=jnp.int32)[None, :]
    labels = jnp.where(positive, 1.0, -1.0)
    total = jnp.sum(jax.nn.softplus(-labels * match_similarity), axis=1)
    slope = (
        (jax.nn.sigmoid(match_similarity) - positive.astype(jnp.float32)) * multiplier_amount
    ).astype(jnp.bfloat16)
    grad_embed = jnp.einsum("cn,nd->cd", slope, piece, preferred_element_type=jnp.float32)
    images_all = image_rows * lax.axis_size("fsdp") * lax.axis_size("dp")
    loss = total / images_all
    pooled_grad = inverse * (
        grad_embed - embed * jnp.mean(grad_embed * embed, axis=-1, keepdims=True)
    )
    per_caption = pooled_grad.reshape(rows, CAPS, channel_count) / counts
    token_grad = jnp.einsum(
        "rsc,rcd->rsd", member, per_caption, precision=lax.Precision.HIGHEST
    ).reshape(rows * length, channel_count)
    input_grad, grads = backward_block(token_grad, saved, whole, rows, length)
    owned = [
        lax.psum(
            lax.psum_scatter(piece_grad.astype(jnp.bfloat16), "fsdp", scatter_dimension=0, tiled=True), "dp"
        ).astype(jnp.float32)
        for piece_grad in grads[:4]
    ]
    small = jnp.concatenate([grads[4], grads[5], grads[6].reshape(-1, channel_count)], axis=0)
    small = lax.psum(small, ("fsdp", "dp"))
    place = lax.axis_index("fsdp")
    width = normalizer_multipliers.shape[1]
    columns = lax.dynamic_slice_in_dim(small[:8], place * width, width, axis=1)
    hidden_width = widened_offset.shape[0]
    hidden_part = lax.dynamic_slice_in_dim(small[8:].reshape(-1), place * hidden_width, hidden_width)
    summed = (*owned, columns[:2], columns[2:8], hidden_part)
    grad_input = input_grad.astype(jnp.bfloat16).reshape(rows, length, channel_count)
    return (
        summed[0],
        summed[1],
        summed[2],
        summed[3],
        summed[4],
        summed[5],
        summed[6],
        grad_input,
        loss,
    )


BF = jnp.bfloat16
F32 = jnp.float32
MESH_ID = pl.DeviceIdType.MESH
TILE = 256
N_AG = 11
D_UNIT = 8


def nn(a, b):
    return jnp.dot(a, b, preferred_element_type=F32)


def nt(a, b):
    return lax.dot_general(a, b, (((1,), (1,)), ((), ())), preferred_element_type=F32)


def tn(a, b):
    return lax.dot_general(a, b, (((0,), (0,)), ((), ())), preferred_element_type=F32)


def span(start, size, unit=16):
    if isinstance(start, int):
        return pl.ds(start, size)
    return pl.ds(pl.multiple_of(start, unit), size)


def norm_rows(values):
    centred = values - jnp.mean(values, axis=-1, keepdims=True)
    inverse = lax.rsqrt(jnp.mean(centred * centred, axis=-1, keepdims=True) + 1e-06)
    return centred * inverse, inverse


def normal_cdf(values):
    return 0.5 * (1.0 + lax.erf(values * math.sqrt(0.5)))


def loop(count, body, events=None):
    def step(i, carry):
        body(i)
        for at, calls in (events or {}).items():

            @pl.when(i == at)
            def _(calls=calls):
                for call in calls:
                    call()

        return carry

    lax.fori_loop(0, count, step, 0)


def fused_kernel(
    sharp_ref,
    offset_ref,
    x_hbm,
    caprow_ref,
    described_ref,
    qkv_hbm,
    out_hbm,
    up_hbm,
    down_hbm,
    small_hbm,
    patches_ref,
    pqkv_hbm,
    pout_hbm,
    pup_hbm,
    pdown_hbm,
    psmall_ref,
    units_out,
    down_out,
    input_out,
    small_out,
    loss_out,
    wts,
    wdn,
    h1,
    qkv,
    att,
    x1,
    h2,
    act,
    dg,
    gm,
    sdn,
    lc,
    lcd,
    lx,
    lxd,
    ly,
    lyd,
    lz,
    lzd,
    work,
    faces,
    small_in,
    params,
    member,
    pooled,
    caption_hi,
    caption_lo,
    partial,
    small_sum,
    small_land,
    face_rows,
    ag_send,
    ag_recv,
    core_send,
    core_recv,
    xy_send,
    xy_recv,
    z_send,
    z_recv,
    side_send,
    side_recv,
    local_sem,
):
    fs = lax.axis_index("fsdp")
    dp = lax.axis_index("dp")
    core = fs % 2
    xb = (fs // 2) % 2
    yb = fs // 4
    fs_core = fs + 1 - 2 * core
    fs_x = fs + 2 - 4 * xb
    fs_y = fs + 4 - 8 * yb
    fs_diag = fs_x + 4 - 8 * yb
    flip = 1 - 2 * core
    peer_core = (fs_core, dp)
    peer_x = (fs_x, dp)
    peer_y = (fs_y, dp)
    half_z = dp // 2
    is_end = (dp == 0) | (dp == 3)
    is_mid = (dp == 1) | (dp == 2)
    near = half_z
    far = 1 - half_z
    dp_inner = 1 + half_z
    dp_end = 3 * half_z
    dp_mid = 2 - half_z
    dp_pair = dp + 1 - 2 * (dp % 2)
    dp_far = dp + 2 - 4 * half_z

    barrier = pltpu.get_barrier_semaphore()
    greet = [peer_core, peer_x, peer_y, (fs, dp_pair), (fs, dp_far)]
    for peer in greet:
        pl.semaphore_signal(barrier, inc=1, device_id=peer, device_id_type=MESH_ID)

    local = []

    def fetch(src, dst):
        copy = pltpu.make_async_copy(src, dst, local_sem.at[len(local)])
        copy.start()
        local.append(copy)
        return copy

    own_rows = span(96 * fs, 96)
    own_copies = [fetch(qkv_hbm.at[:, pl.ds(768 * j, 768)], wts.at[j, own_rows, :]) for j in range(3)]
    own_copies.append(fetch(out_hbm, wts.at[3, own_rows, :]))
    own_copies += [fetch(up_hbm.at[:, pl.ds(768 * j, 768)], wts.at[4 + j, own_rows, :]) for j in range(4)]
    own_copies.append(fetch(down_hbm, wdn.at[span(384 * fs, 384), :]))
    small_copy = fetch(small_hbm, small_in.at[fs])
    pqkv_copy = fetch(pqkv_hbm, act.at[pl.ds(0, 768), pl.ds(0, 2304)])
    x_copy = fetch(x_hbm, h2)
    pout_copy = fetch(pout_hbm, act.at[pl.ds(0, 768), pl.ds(2304, 768)])
    pup_copy = fetch(pup_hbm, dg.at[pl.ds(0, 768), :])
    pdown_copy = fetch(pdown_hbm, sdn)

    pl.semaphore_wait(barrier, len(greet))

    def weight(unit, shard, part=None):
        if unit < 8:
            rows = span(96 * shard, 96) if part is None else span(96 * shard + 48 * part, 48)
            return wts.at[unit, rows, :]
        rows = span(384 * shard, 384) if part is None else span(384 * shard + 192 * part, 192)
        return wdn.at[rows, pl.ds(256 * (unit - 8), 256)]

    def ag(unit, kind, ref, peer):
        return pltpu.make_async_remote_copy(
            src_ref=ref,
            dst_ref=ref,
            send_sem=ag_send.at[unit, kind],
            recv_sem=ag_recv.at[unit, kind],
            device_id=peer,
            device_id_type=MESH_ID,
        )

    def ag_out(unit, kind):
        shard, part, peer = (
            (fs, None, peer_core),
            (fs, None, peer_x),
            (fs, None, peer_y),
            (fs_x, 0, peer_y),
            (fs_y, 1, peer_x),
            (fs_x, None, peer_core),
            (fs_y, None, peer_core),
            (fs_diag, 0, peer_core),
            (fs_diag, 1, peer_core),
        )[kind]
        return ag(unit, kind, weight(unit, shard, part), peer)

    def ag_in(unit, kind):
        shard, part = (
            (fs_core, None),
            (fs_x, None),
            (fs_y, None),
            (fs_diag, 0),
            (fs_diag, 1),
            (fs_x + flip, None),
            (fs_y + flip, None),
            (fs_diag + flip, 0),
            (fs_diag + flip, 1),
        )[kind]
        return ag(unit, kind, weight(unit, shard, part), peer_core)

    def ag_own(unit):
        if unit < N_AG:
            for kind in (1, 2, 0):
                ag_out(unit, kind).start()

    def ag_relay(unit):
        if 0 <= unit < N_AG:
            ag_in(unit, 1).wait_recv()
            ag_out(unit, 3).start()
            ag_in(unit, 2).wait_recv()
            ag_out(unit, 4).start()
            ag_out(unit, 5).start()
            ag_out(unit, 6).start()

    def ag_last(unit):
        if 0 <= unit < N_AG:
            ag_in(unit, 3).wait_recv()
            ag_out(unit, 7).start()
            ag_in(unit, 4).wait_recv()
            ag_out(unit, 8).start()

    def pump(unit):
        ag_relay(unit)
        ag_last(unit - 1)
        ag_own(unit + 3)

    def ready(unit):
        for kind in (0, 5, 6, 7, 8):
            ag_in(unit, kind).wait_recv()

    def side(index, src, dst, peer):
        return pltpu.make_async_remote_copy(
            src_ref=src,
            dst_ref=dst,
            send_sem=side_send.at[index],
            recv_sem=side_recv.at[index],
            device_id=peer,
            device_id_type=MESH_ID,
        )

    chip_slot = fs - core
    row_slot = 4 * yb

    def param_copy(step, start, count, peer):
        ref = small_in.at[pl.ds(start, count)]
        return side(step, ref, ref, peer)

    param_steps = (
        (fs, 1, peer_core, fs_core),
        (chip_slot, 2, peer_x, chip_slot + 2 - 4 * xb),
        (row_slot, 4, peer_y, 4 - row_slot),
    )

    def param_start(step):
        start, count, peer, _ = param_steps[step]
        param_copy(step, start, count, peer).start()

    def param_wait(step):
        _, count, peer, land = param_steps[step]
        param_copy(step, land, count, peer).wait_recv()

    face_steps = (
        (dp, 1, fs, 1, peer_core, dp, fs_core),
        (dp, 1, chip_slot, 2, peer_x, dp, chip_slot + 2 - 4 * xb),
        (dp, 1, row_slot, 4, peer_y, dp, 4 - row_slot),
        (dp, 1, 0, 8, (fs, dp_pair), dp_pair, 0),
        (2 * half_z, 2, 0, 8, (fs, dp_far), 2 - 2 * half_z, 0),
    )

    def face_copy(step, landing):
        d0, dn, f0, fn, peer, ld, lf = face_steps[step]
        if landing:
            d0, f0 = ld, lf
        ref = faces.at[span(64 * d0 + 8 * f0, 8 * dn * fn, 8), :]
        return side(3 + step, ref, ref, peer)

    def face_start(step):
        face_copy(step, False).start()

    def face_wait(step):
        face_copy(step, True).wait_recv()

    sum_peers = (peer_core, peer_x, peer_y, (fs, dp_pair), (fs, dp_far))

    def sum_copy(step):
        return side(8 + step, small_sum.at[step], small_land.at[step], sum_peers[step])

    def sum_start(step):
        sum_copy(step).start()

    def sum_wait(step):
        sum_copy(step).wait_recv()
        small_sum[step + 1] = small_sum[step] + small_land[step]

    def grad(unit, rows):
        if unit == D_UNIT:
            return sdn.at[rows, :]
        if unit >= 4:
            return act.at[rows, pl.ds(768 * (unit - 4), 768)]
        return wts.at[4 + unit, rows, :]

    def shape_of(unit):
        return 384 if unit == D_UNIT else 96

    def piece_shard(delta, which):
        chip_x = (xb + delta % 2) - 2 * xb * (delta % 2)
        chip_y = (yb + delta // 2) - 2 * yb * (delta // 2)
        return (chip_y * 2 + chip_x) * 2 + which

    def piece(unit, delta, which, part=None):
        size = shape_of(unit)
        shard = piece_shard(delta, which)
        if part is None:
            return grad(unit, span(size * shard, size))
        return grad(unit, span(size * shard + (size // 2) * part, size // 2))

    def lands(pair, unit, slot):
        wide, down_only = pair
        return down_only.at[slot] if unit == D_UNIT else wide.at[unit, slot]

    def accumulate(dst, *sources):
        rows = dst.shape[0]

        def body(i, carry):
            r = span(i * 48, 48)
            value = dst[r, :].astype(F32)
            for source in sources:
                value = value + source[r, :].astype(F32)
            dst[r, :] = value.astype(BF)
            return carry

        lax.fori_loop(0, rows // 48, body, 0)

    def core_copy(unit, delta):
        return pltpu.make_async_remote_copy(
            src_ref=piece(unit, delta, 1 - core),
            dst_ref=lands((lc, lcd), unit, delta),
            send_sem=core_send.at[unit, delta],
            recv_sem=core_recv.at[unit, delta],
            device_id=peer_core,
            device_id_type=MESH_ID,
        )

    def rs_core(unit):
        for delta in (3, 2, 1, 0):
            core_copy(unit, delta).start()

    xy_kinds = (
        (3, 0, (lx, lxd), 0, peer_x),
        (3, 1, (ly, lyd), 0, peer_y),
        (1, 0, (lx, lxd), 1, peer_x),
        (2, 1, (ly, lyd), 1, peer_y),
        (2, 0, (ly, lyd), 2, peer_y),
        (1, 1, (lx, lxd), 2, peer_x),
    )

    def xy_copy(unit, kind):
        delta, part, pair, slot, peer = xy_kinds[kind]
        return pltpu.make_async_remote_copy(
            src_ref=piece(unit, delta, core, part),
            dst_ref=lands(pair, unit, slot),
            send_sem=xy_send.at[unit, kind],
            recv_sem=xy_recv.at[unit, kind],
            device_id=peer,
            device_id_type=MESH_ID,
        )

    def rs_first_piece(unit, delta):
        core_copy(unit, delta).wait_recv()
        accumulate(piece(unit, delta, core), lands((lc, lcd), unit, delta))
        for kind in {3: (0, 1), 1: (2,), 2: (3,), 0: ()}[delta]:
            xy_copy(unit, kind).start()

    def rs_first(unit):
        for delta in (3, 2, 1, 0):
            rs_first_piece(unit, delta)

    def rs_second(unit):
        xy_copy(unit, 0).wait_recv()
        accumulate(piece(unit, 2, core, 0), lands((lx, lxd), unit, 0))
        xy_copy(unit, 4).start()
        xy_copy(unit, 1).wait_recv()
        accumulate(piece(unit, 1, core, 1), lands((ly, lyd), unit, 0))
        xy_copy(unit, 5).start()

    def z_copy(unit, index, src, slot, target):
        return pltpu.make_async_remote_copy(
            src_ref=src,
            dst_ref=lands((lz, lzd), unit, slot),
            send_sem=z_send.at[unit, index],
            recv_sem=z_recv.at[unit, slot],
            device_id=(fs, target),
            device_id_type=MESH_ID,
        )

    def z_land(unit, slot):
        return lands((lz, lzd), unit, slot)

    def z_wait(unit, slot):
        z_copy(unit, 0, z_land(unit, slot), slot, dp_pair).wait_recv()

    def z_out(unit, index):
        own_far = piece(unit, 0, core, far)
        own_near = piece(unit, 0, core, near)
        end = {
            0: (own_far, 1, dp_inner),
            1: (own_near, 0, dp_inner),
        }
        mid = {
            0: (own_far, 2, dp_mid),
            1: (z_land(unit, 2), 2, dp_end),
            2: (z_land(unit, 2), 3, dp_mid),
            3: (z_land(unit, 3), 3, dp_end),
        }
        return end.get(index), mid[index]

    def z_end(unit, index):
        return z_copy(unit, index, *z_out(unit, index)[0])

    def z_mid(unit, index):
        return z_copy(unit, index, *z_out(unit, index)[1])

    def rs_own(unit):
        for kind in (2, 3, 4, 5):
            xy_copy(unit, kind).wait_recv()
        accumulate(piece(unit, 0, core, 0), lands((lx, lxd), unit, 1), lands((ly, lyd), unit, 2))
        accumulate(piece(unit, 0, core, 1), lands((ly, lyd), unit, 1), lands((lx, lxd), unit, 2))

        @pl.when(is_end)
        def _():
            z_end(unit, 0).start()
            z_end(unit, 1).start()

    def rs_z2(unit):
        @pl.when(is_mid)
        def _():
            z_wait(unit, 1)
            accumulate(piece(unit, 0, core, far), z_land(unit, 1))
            z_mid(unit, 0).start()

    def rs_z3(unit):
        @pl.when(is_mid)
        def _():
            z_wait(unit, 0)
            z_wait(unit, 2)
            accumulate(z_land(unit, 2), z_land(unit, 0), piece(unit, 0, core, near))
            z_mid(unit, 1).start()
            z_mid(unit, 2).start()

    def rs_z4(unit):
        @pl.when(is_mid)
        def _():
            z_wait(unit, 3)
            z_mid(unit, 3).start()

    def result_copy(unit, slot):
        size = shape_of(unit) // 2
        rows = span(size * (near if slot == 2 else far), size)
        target = down_out.at[rows, :] if unit == D_UNIT else units_out.at[unit, rows, :]
        return pltpu.make_async_copy(z_land(unit, slot), target, local_sem.at[16 + 2 * unit + slot - 2])

    def rs_done(unit):
        @pl.when(is_end)
        def _():
            z_wait(unit, 2)
            z_wait(unit, 3)

        for slot in (2, 3):
            result_copy(unit, slot).start()

    for copy in own_copies:
        copy.wait()
    small_copy.wait()
    for unit in range(3):
        ag_own(unit)
    param_start(0)

    img_h = gm
    img_k = att
    img_v = h1
    img_gain = psmall_ref
    zero_tail = jnp.zeros((16, 768), BF)

    def image_norm(i):
        values = patches_ref[i].astype(F32)
        scaled, _ = norm_rows(values)
        normed = scaled * img_gain[0:1, :] + img_gain[6:7, :]
        img_h[span(64 * i + 48, 16), :] = zero_tail
        img_h[span(64 * i, 50), :] = normed.astype(BF)
        face_rows[0, pl.ds(i, 1), :] = values[0:1, :]
        face_rows[1, pl.ds(i, 1), :] = normed[0:1, :]

    loop(8, image_norm)
    pqkv_copy.wait()

    def image_kv(i):
        r = span(i * TILE, TILE)
        img_k[r, :] = nn(img_h[r, :], act[pl.ds(0, 768), pl.ds(768, 768)]).astype(BF)
        img_v[r, :] = (nn(img_h[r, :], act[pl.ds(0, 768), pl.ds(1536, 768)]) + img_gain[3:4, :]).astype(BF)

    loop(2, image_kv)
    param_wait(0)
    param_start(1)
    pump(0)

    lane_head = lax.broadcasted_iota(jnp.int32, (8, 768), 1) // 64
    img_q = (nn(face_rows[1].astype(BF), act[pl.ds(0, 768), pl.ds(0, 768)]) + img_gain[2:3, :]) * 0.125
    img_q = img_q.astype(BF).astype(F32)
    stacked = jnp.concatenate([jnp.where(lane_head == h, img_q, 0.0) for h in range(12)], axis=0).astype(BF)
    scores = nt(stacked, img_k[pl.ds(0, 512), :])
    token = lax.broadcasted_iota(jnp.int32, (96, 512), 1)
    image_of = lax.broadcasted_iota(jnp.int32, (96, 512), 0) % 8
    scores = jnp.where((token // 64 == image_of) & (token % 64 < 50), scores, -1e30)
    expd = jnp.exp(scores - jnp.max(scores, axis=-1, keepdims=True))
    probs = (expd / jnp.sum(expd, axis=-1, keepdims=True)).astype(BF)
    mixed = nn(probs, img_v[pl.ds(0, 512), :])
    joined = jnp.zeros((8, 768), F32)
    for h in range(12):
        joined = joined + jnp.where(lane_head == h, mixed[8 * h : 8 * h + 8, :], 0.0)
    param_wait(1)
    param_start(2)
    pump(1)
    pout_copy.wait()
    middle = face_rows[0] + (nn(joined.astype(BF), act[pl.ds(0, 768), pl.ds(2304, 768)]) + img_gain[4:5, :])
    scaled, _ = norm_rows(middle)
    normed = (scaled * img_gain[1:2, :] + img_gain[7:8, :]).astype(BF)
    face_rows[0] = middle
    pup_copy.wait()
    for j in range(4):
        hidden = nn(normed, dg[pl.ds(0, 768), pl.ds(768 * j, 768)]) + img_gain[8 + j : 9 + j, :]
        face_rows[2 + j] = hidden * normal_cdf(hidden)
    pump(2)
    pdown_copy.wait()
    total = face_rows[0] + img_gain[5:6, :]
    for j in range(4):
        total = total + nn(face_rows[2 + j].astype(BF), sdn[pl.ds(768 * j, 768), :])
    unit_norm = total * lax.rsqrt(jnp.mean(total * total, axis=-1, keepdims=True) + 1e-06)
    faces[span(64 * dp + 8 * fs, 8, 8), :] = unit_norm.astype(BF).astype(F32)
    face_start(0)
    param_wait(2)

    flat_small = small_in[...].reshape(128, 128)
    for r in range(4):
        lane = lax.broadcasted_iota(jnp.int32, (128, 384), 0)
        column = lax.broadcasted_iota(jnp.int32, (128, 384), 1)
        pick = jnp.where((column == lane + 96 * r) & (lane < 96), 1.0, 0.0).astype(BF)
        spread = nn(flat_small, pick)
        for block in range(2):
            shard = 4 * block + r
            value = spread[16 * shard : 16 * shard + 8, :]
            cols = slice(384 * block, 384 * block + 384)
            if r == 0:
                params[0:8, cols] = value
            else:
                params[0:8, cols] = params[0:8, cols] + value
        for shard in range(8):
            value = spread[16 * shard + 8 + r : 16 * shard + 9 + r, :]
            row = 8 + shard // 2
            cols = slice(384 * (shard % 2), 384 * (shard % 2) + 384)
            if r == 0:
                params[row : row + 1, cols] = value
            else:
                params[row : row + 1, cols] = params[row : row + 1, cols] + value

    x_copy.wait()

    def first_norm(i):
        r = span(32 * i, 32)
        scaled, _ = norm_rows(h2[r, :].astype(F32))
        h1[r, :] = (scaled * params[0:1, :] + params[6:7, :]).astype(BF)

    loop(32, first_norm)
    for group in range(8):
        same = lax.broadcasted_iota(jnp.int32, (64, 128), 0) == caprow_ref[group : group + 1, :]
        member[:, 128 * group : 128 * group + 128] = jnp.where(same, 1.0, 0.0).astype(BF)
    face_wait(0)
    face_start(1)
    pump(3)

    def project(j):
        def body(i):
            r = span(TILE * i, TILE)
            value = nn(h1[r, :], wts[j])
            if j == 0:
                value = (value + params[2:3, :]) * 0.125
            if j == 2:
                value = value + params[3:4, :]
            qkv[r, pl.ds(768 * j, 768)] = value.astype(BF)

        loop(4, body)

    ready(0)
    project(0)
    ready(1)
    project(1)
    pump(4)
    ready(2)
    project(2)
    face_wait(1)
    face_start(2)

    low_lane = lax.broadcasted_iota(jnp.int32, (128, 128), 1) < 64
    zero_block = jnp.zeros((128, 128), BF)

    def split_heads(block):
        return jnp.concatenate(
            [jnp.where(low_lane, block, zero_block), jnp.where(low_lane, zero_block, block)], axis=0
        )

    def join_heads(value):
        return jnp.where(low_lane, value[0:128, :], value[128:256, :])

    def same_caption(group):
        part = member[:, span(128 * group, 128, 128)]
        same = tn(part, part)
        return jnp.concatenate([same, same], axis=0) > 0.5

    def attention_probs(same, queries, keys):
        value = jnp.where(same, nt(queries, keys), -1e30)
        expd = jnp.exp(value - jnp.max(value, axis=-1, keepdims=True))
        return expd * (1.0 / jnp.sum(expd, axis=-1, keepdims=True))

    def attend(group):
        r = span(128 * group, 128)
        same = same_caption(group)
        for hp in range(6):
            queries = split_heads(qkv[r, pl.ds(128 * hp, 128)])
            probs = attention_probs(same, queries, qkv[r, pl.ds(768 + 128 * hp, 128)])
            mixed = nn(probs.astype(BF), qkv[r, pl.ds(1536 + 128 * hp, 128)])
            att[r, pl.ds(128 * hp, 128)] = join_heads(mixed).astype(BF)

    loop(8, attend, {1: [lambda: pump(5)], 4: [lambda: pump(6)], 7: [lambda: pump(7)]})
    face_wait(2)
    face_start(3)
    ready(3)

    def out_project(i):
        r = span(TILE * i, TILE)
        x1[r, :] = h2[r, :].astype(F32) + (nn(att[r, :], wts[3]) + params[4:5, :])

    loop(4, out_project)

    def second_norm(i):
        r = span(32 * i, 32)
        scaled, _ = norm_rows(x1[r, :])
        h2[r, :] = (scaled * params[1:2, :] + params[7:8, :]).astype(BF)

    loop(32, second_norm)
    face_wait(3)
    face_start(4)
    pump(8)

    def widen(j):
        def body(i):
            r = span(TILE * i, TILE)
            work[...] = nn(h2[r, :], wts[4 + j]) + params[8 + j : 9 + j, :]

            def gelu(k):
                inner = span(16 * k, 16)
                hidden = work[inner, :]
                cdf = normal_cdf(hidden)
                outer = span(TILE * i + 16 * k, 16)
                act[outer, pl.ds(768 * j, 768)] = (hidden * cdf).astype(BF)
                slope = cdf + hidden * (jnp.exp(-0.5 * hidden * hidden) * (1.0 / math.sqrt(2.0 * math.pi)))
                dg[outer, pl.ds(768 * j, 768)] = slope.astype(BF)

            loop(16, gelu)

        loop(4, body)

    for j in range(4):
        ready(4 + j)
        widen(j)
        if j < 2:
            pump(9 + j)
        elif j == 2:
            ag_last(10)
    face_wait(4)

    for jd in range(3):
        ready(8 + jd)
        cols = pl.ds(256 * jd, 256)

        def narrow(i, cols=cols, jd=jd):
            r = span(TILE * i, TILE)
            value = nn(act[r, :], wdn[:, cols]) + params[5:6, 256 * jd : 256 * jd + 256]
            value = x1[r, cols] + value
            top = value.astype(BF)
            rest = (value - top.astype(F32)).astype(BF)
            lanes = span(TILE * i, TILE, 128)
            piece_sum = nn(member[:, lanes], top) + nn(member[:, lanes], rest)

            @pl.when(i == 0)
            def _():
                pooled[:, cols] = piece_sum

            @pl.when(i > 0)
            def _():
                pooled[:, cols] = pooled[:, cols] + piece_sum

        loop(4, narrow)

    count = jnp.sum(member[...].astype(F32), axis=-1, keepdims=True)
    mean_rows = pooled[...] / count
    inverse = lax.rsqrt(jnp.mean(mean_rows * mean_rows, axis=-1, keepdims=True) + 1e-06)
    embed = mean_rows * inverse
    face_all = faces[...].astype(BF)
    amount = sharp_ref[0] * (1.0 / math.sqrt(768.0))
    match = amount * nt(embed.astype(BF), face_all) + offset_ref[0]
    slot = lax.broadcasted_iota(jnp.int32, (64, 256), 1)
    image_id = ((slot // 8) % 8) * 32 + (slot // 64) * 8 + slot % 8
    positive = described_ref[...] == image_id
    signed = jnp.where(positive, -match, match)
    terms = jnp.maximum(signed, 0.0) + jnp.log1p(jnp.exp(-jnp.abs(signed)))
    row_loss = jnp.sum(terms, axis=-1, keepdims=True) * (1.0 / 256.0)
    loss_out[...] = jnp.broadcast_to(row_loss, (64, 128))
    slope = ((jax.nn.sigmoid(match) - jnp.where(positive, 1.0, 0.0)) * amount).astype(BF)
    grad_embed = nn(slope, face_all)
    grad_pooled = inverse * (grad_embed - embed * jnp.mean(grad_embed * embed, axis=-1, keepdims=True))
    per_caption = grad_pooled / count
    caption_hi[...] = per_caption.astype(BF)
    caption_lo[...] = (per_caption - caption_hi[...].astype(F32)).astype(BF)

    def spread_down(i):
        gm[span(TILE * i, TILE), :] = tn(member[:, span(TILE * i, TILE, 128)], caption_hi[...]).astype(BF)

    loop(4, spread_down)

    for unit in range(N_AG):
        for kind in range(9):
            ag_out(unit, kind).wait_send()
    for step in range(3):
        start, sent, peer, _ = param_steps[step]
        param_copy(step, start, sent, peer).wait_send()
    for step in range(5):
        face_copy(step, False).wait_send()

    ones = jnp.ones((16, 1024), BF)

    def column_sum(value):
        return nn(ones, value)[0:1, :]

    def down_piece(delta):
        def body(i):
            which = (1 - core) + i * (2 * core - 1)
            shard = piece_shard(delta, which)
            sdn[span(384 * shard, 384), :] = tn(act[:, span(384 * shard, 384, 128)], gm[...]).astype(BF)

            @pl.when(i == 0)
            def _():
                core_copy(D_UNIT, delta).start()

        loop(2, body)

    down_piece(3)
    down_piece(2)
    rs_first_piece(D_UNIT, 3)
    down_piece(1)
    rs_first_piece(D_UNIT, 2)
    down_piece(0)
    rs_first_piece(D_UNIT, 1)
    rs_first_piece(D_UNIT, 0)

    def hidden_back(i):
        r = span(TILE * i, TILE)
        for jj in range(3):
            cols = pl.ds(1024 * jj, 1024)
            value = nt(gm[r, :], wdn[pl.ds(1024 * jj, 1024), :])
            dg[r, cols] = (dg[r, cols].astype(F32) * value).astype(BF)

    loop(4, hidden_back, {1: [lambda: rs_second(D_UNIT)]})
    partial_rows = {}

    def up_unit(j):
        def body(i):
            act[span(TILE * i, TILE), pl.ds(768 * j, 768)] = tn(
                h2[:, span(TILE * i, TILE, 128)], dg[:, pl.ds(768 * j, 768)]
            ).astype(BF)

        loop(3, body)
        rs_core(4 + j)
        small_sum[0, 8 + j : 9 + j, :] = column_sum(dg[:, pl.ds(768 * j, 768)])

    up_unit(0)
    up_unit(1)
    rs_first(4)
    up_unit(2)
    rs_first(5)
    up_unit(3)
    rs_first(6)
    rs_own(D_UNIT)
    small_sum[0, 5:6, :] = column_sum(gm[...])
    partial[...] = jnp.zeros((4, 8, 768), F32)

    def fold(value):
        return value.reshape(value.shape[0] // 8, 8, 768).sum(axis=0)

    def middle_back(i):
        r = span(TILE * i, TILE)
        total = nt(dg[r, pl.ds(0, 768)], wts[4])
        for j in range(1, 4):
            total = total + nt(dg[r, pl.ds(768 * j, 768)], wts[4 + j])
        work[...] = total
        faces[...] = tn(member[:, span(TILE * i, TILE, 128)], caption_lo[...])

        def rows_back(k):
            inner = span(16 * k, 16)
            outer = span(TILE * i + 16 * k, 16)
            upstream = work[inner, :]
            scaled, inverse = norm_rows(x1[outer, :])
            partial[0] = partial[0] + fold(upstream * scaled)
            partial[1] = partial[1] + fold(upstream)
            weighted = upstream * params[1:2, :]
            first_mean = jnp.mean(weighted, axis=-1, keepdims=True)
            second_mean = jnp.mean(weighted * scaled, axis=-1, keepdims=True)
            value = gm[outer, :].astype(F32) + faces[inner, :]
            value = value + inverse * (weighted - first_mean - scaled * second_mean)
            x1[outer, :] = value
            gm[outer, :] = value.astype(BF)

        loop(16, rows_back)

    loop(
        4,
        middle_back,
        {
            0: [lambda: rs_first(7)],
            1: [lambda: rs_second(4)],
            2: [lambda: rs_z2(D_UNIT)],
            3: [lambda: rs_second(5)],
        },
    )
    x_again = pltpu.make_async_copy(x_hbm, h2, local_sem.at[15])
    x_again.start()

    def out_unit(i):
        wts[7, span(TILE * i, TILE), :] = tn(att[:, span(TILE * i, TILE, 128)], gm[...]).astype(BF)

    loop(3, out_unit)
    rs_core(3)
    small_sum[0, 4:5, :] = column_sum(gm[...])

    def attended_back(i):
        r = span(TILE * i, TILE)
        att[r, :] = nt(gm[r, :], wts[3]).astype(BF)

    loop(4, attended_back)
    rs_second(6)
    rs_first(3)
    rs_own(4)
    rs_z3(D_UNIT)

    def attend_back(group):
        r = span(128 * group, 128)
        same = same_caption(group)
        for hp in range(6):
            qs = pl.ds(128 * hp, 128)
            ks = pl.ds(768 + 128 * hp, 128)
            vs = pl.ds(1536 + 128 * hp, 128)
            queries = split_heads(qkv[r, qs])
            keys = qkv[r, ks]
            upstream = split_heads(att[r, qs])
            probs = attention_probs(same, queries, keys)
            probs_grad = nt(upstream, qkv[r, vs])
            inner = jnp.sum(probs * probs_grad, axis=-1, keepdims=True)
            score_grad = (probs * (probs_grad - inner)).astype(BF)
            qkv[r, vs] = tn(probs.astype(BF), upstream).astype(BF)
            qkv[r, ks] = tn(score_grad, queries).astype(BF)
            qkv[r, qs] = (join_heads(nn(score_grad, keys)).astype(BF).astype(F32) * 0.125).astype(BF)

    loop(
        8,
        attend_back,
        {
            1: [lambda: rs_z2(4), lambda: rs_own(5), lambda: rs_second(7)],
            3: [lambda: rs_z2(5), lambda: rs_z3(4), lambda: rs_own(6), lambda: rs_second(3)],
            5: [lambda: rs_z4(D_UNIT), lambda: rs_z2(6), lambda: rs_z3(5), lambda: rs_own(7)],
            7: [lambda: rs_z2(7), lambda: rs_z3(6), lambda: rs_z4(4), lambda: rs_own(3)],
        },
    )

    def qkv_unit(j):
        def body(i):
            wts[4 + j, span(TILE * i, TILE), :] = tn(
                h1[:, span(TILE * i, TILE, 128)], qkv[:, pl.ds(768 * j, 768)]
            ).astype(BF)

        loop(3, body)
        rs_core(j)

    qkv_unit(0)
    rs_z2(3)
    rs_z3(7)
    rs_z4(5)
    qkv_unit(1)
    rs_first(0)
    rs_z3(3)
    rs_z4(6)
    qkv_unit(2)
    rs_first(1)
    rs_z4(7)
    small_sum[0, 2:3, :] = column_sum(qkv[:, pl.ds(0, 768)])
    small_sum[0, 3:4, :] = column_sum(qkv[:, pl.ds(1536, 768)])
    x_again.wait()

    def input_back(i):
        r = span(TILE * i, TILE)
        total = nt(qkv[r, pl.ds(0, 768)], wts[0])
        for j in range(1, 3):
            total = total + nt(qkv[r, pl.ds(768 * j, 768)], wts[j])
        work[...] = total

        def rows_back(k):
            inner = span(16 * k, 16)
            outer = span(TILE * i + 16 * k, 16)
            upstream = work[inner, :]
            scaled, inverse = norm_rows(h2[outer, :].astype(F32))
            partial[2] = partial[2] + fold(upstream * scaled)
            partial[3] = partial[3] + fold(upstream)
            weighted = upstream * params[0:1, :]
            first_mean = jnp.mean(weighted, axis=-1, keepdims=True)
            second_mean = jnp.mean(weighted * scaled, axis=-1, keepdims=True)
            value = x1[outer, :] + inverse * (weighted - first_mean - scaled * second_mean)
            att[outer, :] = value.astype(BF)

        loop(16, rows_back)

    loop(
        4,
        input_back,
        {
            0: [lambda: rs_first(2), lambda: rs_second(0)],
            1: [lambda: rs_second(1), lambda: rs_z4(3)],
            2: [lambda: rs_own(0)],
            3: [lambda: rs_second(2), lambda: rs_z2(0), lambda: rs_own(1)],
        },
    )
    input_copy = pltpu.make_async_copy(att, input_out, local_sem.at[34])
    input_copy.start()
    for row, index in ((0, 2), (1, 0), (6, 3), (7, 1)):
        small_sum[0, row : row + 1, :] = jnp.sum(partial[index], axis=0, keepdims=True)
    small_sum[0, 12:16, :] = jnp.zeros((4, 768), F32)
    sum_start(0)
    rs_z3(0)
    rs_z2(1)
    sum_wait(0)
    sum_start(1)
    for unit in (D_UNIT, 4, 5, 6, 7, 3):
        rs_done(unit)
    rs_own(2)
    sum_wait(1)
    sum_start(2)
    rs_z4(0)
    rs_z3(1)
    rs_z2(2)
    sum_wait(2)
    sum_start(3)
    rs_z4(1)
    rs_done(0)
    rs_z3(2)
    sum_wait(3)
    sum_start(4)
    rs_done(1)
    rs_z4(2)
    sum_wait(4)
    small_out[...] = small_sum[5]
    rs_done(2)

    input_copy.wait()
    for unit in range(9):
        for slot in (2, 3):
            result_copy(unit, slot).wait()
        for delta in range(4):
            core_copy(unit, delta).wait_send()
        for kind in range(6):
            xy_copy(unit, kind).wait_send()

        @pl.when(is_end)
        def _(unit=unit):
            for index in range(2):
                z_end(unit, index).wait_send()

        @pl.when(is_mid)
        def _(unit=unit):
            for index in range(4):
                z_mid(unit, index).wait_send()

    for step in range(5):
        sum_copy(step).wait_send()


def fused_step(
    incoming_word_states,
    sentence_number_per_word,
    described_picture,
    lookup_matrices,
    mixer_exit_matrix,
    widening_matrix,
    narrowing_matrix,
    normalizer_multipliers,
    word_offsets,
    widened_offset,
    picture_patches,
    picture_lookup_matrices,
    picture_mixer_exit_matrix,
    picture_widening_matrix,
    picture_narrowing_matrix,
    picture_normalizer_multipliers,
    picture_offsets,
    picture_widened_offset,
    sharpness_coefficient,
    objective_offset,
):
    rows, length, width = incoming_word_states.shape
    tokens = rows * length
    small = jnp.concatenate(
        [normalizer_multipliers, word_offsets, widened_offset.reshape(4, 96)], axis=0
    )
    small = jnp.pad(small, ((0, 4), (0, 32)))
    picture_small = jnp.concatenate(
        [picture_normalizer_multipliers, picture_offsets, picture_widened_offset.reshape(4, width)], axis=0
    )
    picture_small = jnp.pad(picture_small.astype(F32), ((0, 4), (0, 0)))
    caption = sentence_number_per_word + CAPS * jnp.arange(rows, dtype=jnp.int32)[:, None]
    vmem = pl.BlockSpec(memory_space=pltpu.VMEM)
    hbm = pl.BlockSpec(memory_space=pl.ANY)
    smem = pl.BlockSpec(memory_space=pltpu.SMEM)
    dma = pltpu.SemaphoreType.DMA
    outs = pl.pallas_call(
        fused_kernel,
        out_shape=(
            jax.ShapeDtypeStruct((8, 96, width), BF),
            jax.ShapeDtypeStruct((384, width), BF),
            jax.ShapeDtypeStruct((tokens, width), BF),
            jax.ShapeDtypeStruct((16, width), F32),
            jax.ShapeDtypeStruct((64, 128), F32),
        ),
        in_specs=[smem, smem, hbm, vmem, vmem, hbm, hbm, hbm, hbm, hbm, vmem, hbm, hbm, hbm, hbm, vmem],
        out_specs=(hbm, hbm, hbm, vmem, vmem),
        scratch_shapes=[
            pltpu.VMEM((8, 768, 768), BF),
            pltpu.VMEM((3072, 768), BF),
            pltpu.VMEM((1024, 768), BF),
            pltpu.VMEM((1024, 2304), BF),
            pltpu.VMEM((1024, 768), BF),
            pltpu.VMEM((1024, 768), F32),
            pltpu.VMEM((1024, 768), BF),
            pltpu.VMEM((1024, 3072), BF),
            pltpu.VMEM((1024, 3072), BF),
            pltpu.VMEM((1024, 768), BF),
            pltpu.VMEM((3072, 768), BF),
            pltpu.VMEM((8, 4, 96, 768), BF),
            pltpu.VMEM((4, 384, 768), BF),
            pltpu.VMEM((8, 3, 48, 768), BF),
            pltpu.VMEM((3, 192, 768), BF),
            pltpu.VMEM((8, 3, 48, 768), BF),
            pltpu.VMEM((3, 192, 768), BF),
            pltpu.VMEM((8, 4, 48, 768), BF),
            pltpu.VMEM((4, 192, 768), BF),
            pltpu.VMEM((TILE, 768), F32),
            pltpu.VMEM((TILE, 768), F32),
            pltpu.VMEM((8, 16, 128), BF),
            pltpu.VMEM((16, 768), F32),
            pltpu.VMEM((64, 1024), BF),
            pltpu.VMEM((64, 768), F32),
            pltpu.VMEM((64, 768), BF),
            pltpu.VMEM((64, 768), BF),
            pltpu.VMEM((4, 8, 768), F32),
            pltpu.VMEM((6, 16, 768), F32),
            pltpu.VMEM((5, 16, 768), F32),
            pltpu.VMEM((6, 8, 768), F32),
            dma((N_AG, 9)),
            dma((N_AG, 9)),
            dma((9, 4)),
            dma((9, 4)),
            dma((9, 6)),
            dma((9, 6)),
            dma((9, 4)),
            dma((9, 4)),
            dma((13,)),
            dma((13,)),
            dma((35,)),
        ],
        compiler_params=pltpu.CompilerParams(
            collective_id=0, has_side_effects=True, vmem_limit_bytes=67043328
        ),
        name="lit_step",
    )(
        sharpness_coefficient,
        objective_offset,
        incoming_word_states.reshape(tokens, width),
        caption.reshape(tokens // 128, 128),
        described_picture.reshape(-1, 1),
        lookup_matrices,
        mixer_exit_matrix,
        widening_matrix,
        narrowing_matrix,
        small,
        picture_patches,
        picture_lookup_matrices,
        picture_mixer_exit_matrix,
        picture_widening_matrix,
        picture_narrowing_matrix,
        picture_small,
    )
    units, down_part, input_part, small_part, loss_part = outs
    place = lax.axis_index("fsdp")
    columns = lax.dynamic_slice_in_dim(small_part[:8], place * 96, 96, axis=1)
    hidden_part = lax.dynamic_slice_in_dim(small_part[8:12].reshape(-1), place * 384, 384)
    wide = units.astype(F32)
    return (
        jnp.concatenate([wide[0], wide[1], wide[2]], axis=1),
        wide[3],
        jnp.concatenate([wide[4], wide[5], wide[6], wide[7]], axis=1),
        down_part.astype(F32),
        columns[:2],
        columns[2:8],
        hidden_part,
        input_part.reshape(rows, length, width),
        loss_part[:, 0],
    )


def solution(mesh):
    fits = mesh.shape["fsdp"] == 8 and mesh.shape["dp"] == 4
    return jax.shard_map(
        fused_step if fits else per_device,
        mesh=mesh,
        in_specs=(
            P(("fsdp", "dp"), None, None),
            P(("fsdp", "dp"), None),
            P(("fsdp", "dp")),
            P("fsdp", None),
            P("fsdp", None),
            P("fsdp", None),
            P("fsdp", None),
            P(None, "fsdp"),
            P(None, "fsdp"),
            P("fsdp"),
            P(("fsdp", "dp"), None, None),
            P(),
            P(),
            P(),
            P(),
            P(),
            P(),
            P(),
            P(),
            P(),
        ),
        out_specs=(
            P("fsdp", None),
            P("fsdp", None),
            P("fsdp", None),
            P("fsdp", None),
            P(None, "fsdp"),
            P(None, "fsdp"),
            P("fsdp"),
            P(("fsdp", "dp"), None, None),
            P(("fsdp", "dp")),
        ),
        check_vma=False,
    )
```

```python
import math

import jax
import jax.numpy as jnp
from jax import lax
from jax.experimental import pallas as pl
from jax.experimental.pallas import tpu as pltpu
from jax.sharding import PartitionSpec as P

HEAD_DIM = 64
CAPS = 4


def layer_norm(values, gain, shift):
    centred = values - jnp.mean(values, axis=-1, keepdims=True)
    inverse = lax.rsqrt(jnp.mean(centred * centred, axis=-1, keepdims=True) + 1e-06)
    scaled = centred * inverse
    return (scaled * gain + shift, scaled, inverse)


def norm_back(grad_scaled, scaled, inverse):
    first_mean = jnp.mean(grad_scaled, axis=-1, keepdims=True)
    second_mean = jnp.mean(grad_scaled * scaled, axis=-1, keepdims=True)
    return inverse * (grad_scaled - first_mean - scaled * second_mean)


def gelu_exact(values):
    return jax.nn.gelu(values, approximate=False)


def forward_block(flat, rows, length, mask, weights):
    qkv_w, out_w, up_w, down_w, gains_low, biases_low, up_b = weights
    gains = gains_low.astype(jnp.float32)
    biases = biases_low.astype(jnp.float32)
    channel_count = flat.shape[-1]
    heads = channel_count // HEAD_DIM
    scale = 1.0 / math.sqrt(HEAD_DIM)
    first, scaled_one, inverse_one = layer_norm(flat, gains[0], biases[4])
    first_low = first.astype(jnp.bfloat16)
    mixed = jnp.dot(first_low, qkv_w, preferred_element_type=jnp.float32)
    query = (
        ((mixed[:, :channel_count] + biases[0]) * scale)
        .astype(jnp.bfloat16)
        .reshape(rows, length, heads, HEAD_DIM)
    )
    key_low = (
        mixed[:, channel_count : 2 * channel_count]
        .astype(jnp.bfloat16)
        .reshape(rows, length, heads, HEAD_DIM)
    )
    value_low = (
        (mixed[:, 2 * channel_count :] + biases[1])
        .astype(jnp.bfloat16)
        .reshape(rows, length, heads, HEAD_DIM)
    )
    scores = jnp.einsum("rqhd,rkhd->rhqk", query, key_low, preferred_element_type=jnp.float32)
    if mask is not None:
        scores = jnp.where(mask[:, None], scores, -1e30)
    probs = jax.nn.softmax(scores, axis=-1)
    probs_low = probs.astype(jnp.bfloat16)
    attended = jnp.einsum(
        "rhqk,rkhd->rqhd", probs_low, value_low, preferred_element_type=jnp.float32
    )
    attended = attended.astype(jnp.bfloat16).reshape(rows * length, channel_count)
    middle = flat + (jnp.dot(attended, out_w, preferred_element_type=jnp.float32) + biases[2])
    second, scaled_two, inverse_two = layer_norm(middle, gains[1], biases[5])
    second_low = second.astype(jnp.bfloat16)
    hidden = jnp.dot(second_low, up_w, preferred_element_type=jnp.float32) + up_b.astype(
        jnp.float32
    )
    active = gelu_exact(hidden).astype(jnp.bfloat16)
    output = middle + (jnp.dot(active, down_w, preferred_element_type=jnp.float32) + biases[3])
    saved = (
        scaled_one,
        inverse_one,
        first_low,
        query,
        key_low,
        value_low,
        probs,
        probs_low,
        attended,
        scaled_two,
        inverse_two,
        second_low,
        hidden,
        active,
    )
    return (output, saved)


def backward_block(grad_output, saved, weights, rows, length):
    qkv_w, out_w, up_w, down_w, gains_low, biases_low, up_b = weights
    gains = gains_low.astype(jnp.float32)
    (
        scaled_one,
        inverse_one,
        first_low,
        query,
        key_low,
        value_low,
        probs,
        probs_low,
        attended,
        scaled_two,
        inverse_two,
        second_low,
        hidden,
        active,
    ) = saved
    channel_count = grad_output.shape[-1]
    heads = channel_count // HEAD_DIM
    scale = 1.0 / math.sqrt(HEAD_DIM)
    count = rows * length
    down_grad = grad_output.astype(jnp.bfloat16)
    grad_down_bias = jnp.sum(down_grad, axis=0, dtype=jnp.float32)
    grad_down_w = jnp.einsum("nf,nd->fd", active, down_grad, preferred_element_type=jnp.float32)
    active_grad = jnp.einsum("nd,fd->nf", down_grad, down_w, preferred_element_type=jnp.float32)
    gelu_back = jax.vjp(gelu_exact, hidden)[1]
    hidden_grad = gelu_back(active_grad)[0].astype(jnp.bfloat16)
    grad_up_bias = jnp.sum(hidden_grad, axis=0, dtype=jnp.float32)
    grad_up_w = jnp.einsum("nd,nf->df", second_low, hidden_grad, preferred_element_type=jnp.float32)
    second_grad = jnp.einsum("nf,df->nd", hidden_grad, up_w, preferred_element_type=jnp.float32)
    grad_gain_two = jnp.sum(second_grad * scaled_two, axis=0)
    grad_shift_two = jnp.sum(second_grad, axis=0)
    middle_grad = grad_output + norm_back(second_grad * gains[1], scaled_two, inverse_two)
    branch_grad = middle_grad.astype(jnp.bfloat16)
    grad_out_bias = jnp.sum(branch_grad, axis=0, dtype=jnp.float32)
    grad_out_w = jnp.einsum("nd,ne->de", attended, branch_grad, preferred_element_type=jnp.float32)
    attended_grad = jnp.einsum("ne,de->nd", branch_grad, out_w, preferred_element_type=jnp.float32)
    attended_grad = attended_grad.astype(jnp.bfloat16).reshape(rows, length, heads, HEAD_DIM)
    probs_grad = jnp.einsum(
        "rqhd,rkhd->rhqk", attended_grad, value_low, preferred_element_type=jnp.float32
    )
    value_grad = jnp.einsum(
        "rhqk,rqhd->rkhd", probs_low, attended_grad, preferred_element_type=jnp.float32
    ).astype(jnp.bfloat16)
    score_grad = probs * (probs_grad - jnp.sum(probs * probs_grad, axis=-1, keepdims=True))
    score_grad = score_grad.astype(jnp.bfloat16)
    query_grad = jnp.einsum(
        "rhqk,rkhd->rqhd", score_grad, key_low, preferred_element_type=jnp.float32
    ).astype(jnp.bfloat16)
    key_grad = jnp.einsum(
        "rhqk,rqhd->rkhd", score_grad, query, preferred_element_type=jnp.float32
    ).astype(jnp.bfloat16)
    query_flat = query_grad.reshape(count, channel_count) * scale
    value_flat = value_grad.reshape(count, channel_count)
    mixed_grad = jnp.concatenate(
        [query_flat, key_grad.reshape(count, channel_count), value_flat], axis=1
    )
    grad_query_bias = jnp.sum(query_flat, axis=0, dtype=jnp.float32)
    grad_value_bias = jnp.sum(value_flat, axis=0, dtype=jnp.float32)
    grad_qkv_w = jnp.einsum("nd,ne->de", first_low, mixed_grad, preferred_element_type=jnp.float32)
    first_grad = jnp.einsum("ne,de->nd", mixed_grad, qkv_w, preferred_element_type=jnp.float32)
    grad_gain_one = jnp.sum(first_grad * scaled_one, axis=0)
    grad_shift_one = jnp.sum(first_grad, axis=0)
    input_grad = middle_grad + norm_back(first_grad * gains[0], scaled_one, inverse_one)
    grad_gains = jnp.stack([grad_gain_one, grad_gain_two])
    grad_biases = jnp.stack(
        [
            grad_query_bias,
            grad_value_bias,
            grad_out_bias,
            grad_down_bias,
            grad_shift_one,
            grad_shift_two,
        ]
    )
    return (
        input_grad,
        (grad_qkv_w, grad_out_w, grad_up_w, grad_down_w, grad_gains, grad_biases, grad_up_bias),
    )


def image_first_token(patches, qkv_w, out_w, up_w, down_w, gains_low, biases_low, up_b):
    rows, length, channel_count = patches.shape
    gains = gains_low.astype(jnp.float32)
    biases = biases_low.astype(jnp.float32)
    heads = channel_count // HEAD_DIM
    scale = 1.0 / math.sqrt(HEAD_DIM)
    first_low = layer_norm(patches.astype(jnp.float32), gains[0], biases[4])[0].astype(jnp.bfloat16)
    flat_low = first_low.reshape(rows * length, channel_count)
    query = (
        (jnp.dot(first_low[:, 0], qkv_w[:, :channel_count], preferred_element_type=jnp.float32) + biases[0])
        * scale
    ).astype(jnp.bfloat16).reshape(rows, heads, HEAD_DIM)
    mixed = jnp.dot(flat_low, qkv_w[:, channel_count:], preferred_element_type=jnp.float32)
    key_low = mixed[:, :channel_count].astype(jnp.bfloat16).reshape(rows, length, heads, HEAD_DIM)
    value_low = (
        (mixed[:, channel_count:] + biases[1]).astype(jnp.bfloat16).reshape(rows, length, heads, HEAD_DIM)
    )
    scores = jnp.einsum("rhd,rkhd->rhk", query, key_low, preferred_element_type=jnp.float32)
    probs_low = jax.nn.softmax(scores, axis=-1).astype(jnp.bfloat16)
    attended = jnp.einsum("rhk,rkhd->rhd", probs_low, value_low, preferred_element_type=jnp.float32)
    attended = attended.astype(jnp.bfloat16).reshape(rows, channel_count)
    middle = patches[:, 0].astype(jnp.float32) + (
        jnp.dot(attended, out_w, preferred_element_type=jnp.float32) + biases[2]
    )
    second_low = layer_norm(middle, gains[1], biases[5])[0].astype(jnp.bfloat16)
    hidden = jnp.dot(second_low, up_w, preferred_element_type=jnp.float32) + up_b.astype(jnp.float32)
    active = gelu_exact(hidden).astype(jnp.bfloat16)
    return middle + (jnp.dot(active, down_w, preferred_element_type=jnp.float32) + biases[3])


def per_device(
    incoming_word_states,
    sentence_number_per_word,
    described_picture,
    lookup_matrices,
    mixer_exit_matrix,
    widening_matrix,
    narrowing_matrix,
    normalizer_multipliers,
    word_offsets,
    widened_offset,
    picture_patches,
    picture_lookup_matrices,
    picture_mixer_exit_matrix,
    picture_widening_matrix,
    picture_narrowing_matrix,
    picture_normalizer_multipliers,
    picture_offsets,
    picture_widened_offset,
    sharpness_coefficient,
    objective_offset,
):
    rows, length, channel_count = incoming_word_states.shape
    whole = (
        lax.all_gather(lookup_matrices, "fsdp", axis=0, tiled=True),
        lax.all_gather(mixer_exit_matrix, "fsdp", axis=0, tiled=True),
        lax.all_gather(widening_matrix, "fsdp", axis=0, tiled=True),
        lax.all_gather(narrowing_matrix, "fsdp", axis=0, tiled=True),
        lax.all_gather(normalizer_multipliers, "fsdp", axis=1, tiled=True),
        lax.all_gather(word_offsets, "fsdp", axis=1, tiled=True),
        lax.all_gather(widened_offset, "fsdp", axis=0, tiled=True),
    )
    image_rows, image_length = (picture_patches.shape[0], picture_patches.shape[1])
    image_token = image_first_token(
        picture_patches,
        picture_lookup_matrices,
        picture_mixer_exit_matrix,
        picture_widening_matrix,
        picture_narrowing_matrix,
        picture_normalizer_multipliers,
        picture_offsets,
        picture_widened_offset,
    )
    image_embed = (
        image_token * lax.rsqrt(jnp.mean(image_token * image_token, axis=-1, keepdims=True) + 1e-06)
    ).astype(jnp.bfloat16)
    mask = sentence_number_per_word[:, :, None] == sentence_number_per_word[:, None, :]
    flat = incoming_word_states.astype(jnp.float32).reshape(rows * length, channel_count)
    text_result, saved = forward_block(flat, rows, length, mask, whole)
    member = (sentence_number_per_word[:, :, None] == jnp.arange(CAPS, dtype=jnp.int32)).astype(
        jnp.float32
    )
    counts = jnp.sum(member, axis=1)[:, :, None]
    pooled = (
        jnp.einsum(
            "rsc,rsd->rcd",
            member,
            text_result.reshape(rows, length, channel_count),
            precision=lax.Precision.HIGHEST,
        )
        / counts
    )
    pooled = pooled.reshape(rows * CAPS, channel_count)
    inverse = lax.rsqrt(jnp.mean(pooled * pooled, axis=-1, keepdims=True) + 1e-06)
    embed = pooled * inverse
    embed_low = embed.astype(jnp.bfloat16)
    multiplier_amount = sharpness_coefficient[0] / math.sqrt(channel_count)
    piece = lax.all_gather(image_embed, ("fsdp", "dp"), axis=0, tiled=True)
    unscaled_similarity = jnp.einsum(
        "cd,nd->cn", embed_low, piece, preferred_element_type=jnp.float32
    )
    match_similarity = multiplier_amount * unscaled_similarity + objective_offset[0]
    positive = described_picture[:, None] == jnp.arange(piece.shape[0], dtype=jnp.int32)[None, :]
    labels = jnp.where(positive, 1.0, -1.0)
    total = jnp.sum(jax.nn.softplus(-labels * match_similarity), axis=1)
    slope = (
        (jax.nn.sigmoid(match_similarity) - positive.astype(jnp.float32)) * multiplier_amount
    ).astype(jnp.bfloat16)
    grad_embed = jnp.einsum("cn,nd->cd", slope, piece, preferred_element_type=jnp.float32)
    images_all = image_rows * lax.axis_size("fsdp") * lax.axis_size("dp")
    loss = total / images_all
    pooled_grad = inverse * (
        grad_embed - embed * jnp.mean(grad_embed * embed, axis=-1, keepdims=True)
    )
    per_caption = pooled_grad.reshape(rows, CAPS, channel_count) / counts
    token_grad = jnp.einsum(
        "rsc,rcd->rsd", member, per_caption, precision=lax.Precision.HIGHEST
    ).reshape(rows * length, channel_count)
    input_grad, grads = backward_block(token_grad, saved, whole, rows, length)
    owned = [
        lax.psum(
            lax.psum_scatter(piece_grad.astype(jnp.bfloat16), "fsdp", scatter_dimension=0, tiled=True), "dp"
        ).astype(jnp.float32)
        for piece_grad in grads[:4]
    ]
    small = jnp.concatenate([grads[4], grads[5], grads[6].reshape(-1, channel_count)], axis=0)
    small = lax.psum(small, ("fsdp", "dp"))
    place = lax.axis_index("fsdp")
    width = normalizer_multipliers.shape[1]
    columns = lax.dynamic_slice_in_dim(small[:8], place * width, width, axis=1)
    hidden_width = widened_offset.shape[0]
    hidden_part = lax.dynamic_slice_in_dim(small[8:].reshape(-1), place * hidden_width, hidden_width)
    summed = (*owned, columns[:2], columns[2:8], hidden_part)
    grad_input = input_grad.astype(jnp.bfloat16).reshape(rows, length, channel_count)
    return (
        summed[0],
        summed[1],
        summed[2],
        summed[3],
        summed[4],
        summed[5],
        summed[6],
        grad_input,
        loss,
    )


BF = jnp.bfloat16
F32 = jnp.float32
MESH_ID = pl.DeviceIdType.MESH
TILE = 256
ROWS = 128
GROUPS = 2
N_AG = 11
D_UNIT = 8


def nn(a, b):
    return jnp.dot(a, b, preferred_element_type=F32)


def nt(a, b):
    return lax.dot_general(a, b, (((1,), (1,)), ((), ())), preferred_element_type=F32)


def tn(a, b):
    return lax.dot_general(a, b, (((0,), (0,)), ((), ())), preferred_element_type=F32)


def span(start, size, unit=16):
    if isinstance(start, int):
        return pl.ds(start, size)
    return pl.ds(pl.multiple_of(start, unit), size)


def norm_rows(values):
    centred = values - jnp.mean(values, axis=-1, keepdims=True)
    inverse = lax.rsqrt(jnp.mean(centred * centred, axis=-1, keepdims=True) + 1e-06)
    return centred * inverse, inverse


def normal_cdf(values):
    return 0.5 * (1.0 + lax.erf(values * math.sqrt(0.5)))


def loop(count, body, events=None):
    def step(i, carry):
        body(i)
        for at, calls in (events or {}).items():

            @pl.when(i == at)
            def _(calls=calls):
                for call in calls:
                    call()

        return carry

    lax.fori_loop(0, count, step, 0)


def fused_kernel(
    sharp_ref,
    offset_ref,
    x_hbm,
    segment_ref,
    described_ref,
    qkv_hbm,
    out_hbm,
    up_hbm,
    down_hbm,
    gain_ref,
    shift_ref,
    hidden_ref,
    patches_hbm,
    pqkv_hbm,
    pout_hbm,
    pup_hbm,
    pdown_hbm,
    pgain_ref,
    pshift_ref,
    phidden_ref,
    units_out,
    down_out,
    input_out,
    small_out,
    loss_out,
    wts,
    wdn,
    h1,
    qkv,
    att,
    x1,
    h2,
    act,
    dg,
    gm,
    sdn,
    lc,
    lcd,
    lx,
    lxd,
    ly,
    lyd,
    lz,
    lzd,
    work,
    faces,
    small_in,
    params,
    img_gain,
    member,
    pooled,
    caption_hi,
    caption_lo,
    partial,
    small_sum,
    small_land,
    face_rows,
    ag_send,
    ag_recv,
    core_send,
    core_recv,
    xy_send,
    xy_recv,
    z_send,
    z_recv,
    side_send,
    side_recv,
    local_sem,
):
    fs = lax.axis_index("fsdp")
    dp = lax.axis_index("dp")
    core = fs % 2
    xb = (fs // 2) % 2
    yb = fs // 4
    fs_core = fs + 1 - 2 * core
    fs_x = fs + 2 - 4 * xb
    fs_y = fs + 4 - 8 * yb
    fs_diag = fs_x + 4 - 8 * yb
    flip = 1 - 2 * core
    peer_core = (fs_core, dp)
    peer_x = (fs_x, dp)
    peer_y = (fs_y, dp)
    half_z = dp // 2
    is_end = (dp == 0) | (dp == 3)
    is_mid = (dp == 1) | (dp == 2)
    near = half_z
    far = 1 - half_z
    dp_inner = 1 + half_z
    dp_end = 3 * half_z
    dp_mid = 2 - half_z
    dp_pair = dp + 1 - 2 * (dp % 2)
    dp_far = dp + 2 - 4 * half_z

    barrier = pltpu.get_barrier_semaphore()
    greet = [peer_core, peer_x, peer_y, (fs, dp_pair), (fs, dp_far)]
    for peer in greet:
        pl.semaphore_signal(barrier, inc=1, device_id=peer, device_id_type=MESH_ID)

    local = []

    def fetch(src, dst):
        copy = pltpu.make_async_copy(src, dst, local_sem.at[len(local)])
        copy.start()
        local.append(copy)
        return copy

    own_rows = span(96 * fs, 96)
    own_copies = [fetch(qkv_hbm.at[:, pl.ds(768 * j, 768)], wts.at[j, own_rows, :]) for j in range(3)]
    own_copies.append(fetch(out_hbm, wts.at[3, own_rows, :]))
    own_copies += [fetch(up_hbm.at[:, pl.ds(768 * j, 768)], wts.at[4 + j, own_rows, :]) for j in range(4)]
    own_copies.append(fetch(down_hbm, wdn.at[span(384 * fs, 384), :]))
    patches_copy = fetch(patches_hbm, gm.at[pl.ds(512, 400), :])
    pqkv_copy = fetch(pqkv_hbm, act.at[pl.ds(0, 768), pl.ds(0, 2304)])
    x_copy = fetch(x_hbm, h2)
    pout_copy = fetch(pout_hbm, act.at[pl.ds(0, 768), pl.ds(2304, 768)])
    pup_copy = fetch(pup_hbm, dg.at[pl.ds(0, 768), :])
    pdown_copy = fetch(pdown_hbm, sdn)

    small_in[fs] = jnp.zeros((16, 128), F32)
    small_in[fs, 0:2, 0:96] = gain_ref[...].astype(F32)
    small_in[fs, 2:8, 0:96] = shift_ref[...].astype(F32)
    small_in[fs, 8:11, :] = hidden_ref[...].astype(F32)
    pl.semaphore_wait(barrier, len(greet))

    def weight(unit, shard, part=None):
        if unit < 8:
            rows = span(96 * shard, 96) if part is None else span(96 * shard + 48 * part, 48)
            return wts.at[unit, rows, :]
        rows = span(384 * shard, 384) if part is None else span(384 * shard + 192 * part, 192)
        return wdn.at[rows, pl.ds(256 * (unit - 8), 256)]

    def own_weight(unit):
        if unit < 3:
            return qkv_hbm.at[:, pl.ds(768 * unit, 768)]
        if unit == 3:
            return out_hbm
        if unit < 8:
            return up_hbm.at[:, pl.ds(768 * (unit - 4), 768)]
        return down_hbm.at[:, pl.ds(256 * (unit - 8), 256)]

    def ag(unit, kind, ref, peer, source=None):
        return pltpu.make_async_remote_copy(
            src_ref=ref if source is None else source,
            dst_ref=ref,
            send_sem=ag_send.at[unit, kind],
            recv_sem=ag_recv.at[unit, kind],
            device_id=peer,
            device_id_type=MESH_ID,
        )

    def ag_out(unit, kind):
        shard, part, peer = (
            (fs, None, peer_core),
            (fs, None, peer_x),
            (fs, None, peer_y),
            (fs_x, 0, peer_y),
            (fs_y, 1, peer_x),
            (fs_x, None, peer_core),
            (fs_y, None, peer_core),
            (fs_diag, 0, peer_core),
            (fs_diag, 1, peer_core),
        )[kind]
        return ag(unit, kind, weight(unit, shard, part), peer, own_weight(unit) if kind < 3 else None)

    def ag_in(unit, kind):
        shard, part = (
            (fs_core, None),
            (fs_x, None),
            (fs_y, None),
            (fs_diag, 0),
            (fs_diag, 1),
            (fs_x + flip, None),
            (fs_y + flip, None),
            (fs_diag + flip, 0),
            (fs_diag + flip, 1),
        )[kind]
        return ag(unit, kind, weight(unit, shard, part), peer_core)

    def ag_own(unit):
        if unit < N_AG:
            for kind in (1, 2, 0):
                ag_out(unit, kind).start()

    def ag_relay(unit):
        if 0 <= unit < N_AG:
            ag_in(unit, 1).wait_recv()
            ag_out(unit, 3).start()
            ag_in(unit, 2).wait_recv()
            ag_out(unit, 4).start()
            ag_out(unit, 5).start()
            ag_out(unit, 6).start()

    def ag_last(unit):
        if 0 <= unit < N_AG:
            ag_in(unit, 3).wait_recv()
            ag_out(unit, 7).start()
            ag_in(unit, 4).wait_recv()
            ag_out(unit, 8).start()

    def pump(unit):
        ag_relay(unit)
        ag_last(unit - 1)
        ag_own(unit + 3)

    def ready(unit):
        for kind in (0, 5, 6, 7, 8):
            ag_in(unit, kind).wait_recv()

    def side(index, src, dst, peer):
        return pltpu.make_async_remote_copy(
            src_ref=src,
            dst_ref=dst,
            send_sem=side_send.at[index],
            recv_sem=side_recv.at[index],
            device_id=peer,
            device_id_type=MESH_ID,
        )

    chip_slot = fs - core
    row_slot = 4 * yb

    def param_copy(step, start, count, peer):
        ref = small_in.at[pl.ds(start, count)]
        return side(step, ref, ref, peer)

    param_steps = (
        (fs, 1, peer_core, fs_core),
        (chip_slot, 2, peer_x, chip_slot + 2 - 4 * xb),
        (row_slot, 4, peer_y, 4 - row_slot),
    )

    def param_start(step):
        start, count, peer, _ = param_steps[step]
        param_copy(step, start, count, peer).start()

    def param_wait(step):
        _, count, peer, land = param_steps[step]
        param_copy(step, land, count, peer).wait_recv()

    face_steps = (
        (dp, 1, fs, 1, peer_core, dp, fs_core),
        (dp, 1, chip_slot, 2, peer_x, dp, chip_slot + 2 - 4 * xb),
        (dp, 1, row_slot, 4, peer_y, dp, 4 - row_slot),
        (dp, 1, 0, 8, (fs, dp_pair), dp_pair, 0),
        (2 * half_z, 2, 0, 8, (fs, dp_far), 2 - 2 * half_z, 0),
    )

    def face_copy(step, landing):
        d0, dn, f0, fn, peer, ld, lf = face_steps[step]
        if landing:
            d0, f0 = ld, lf
        ref = faces.at[span(64 * d0 + 8 * f0, 8 * dn * fn, 8), :]
        return side(3 + step, ref, ref, peer)

    def face_start(step):
        face_copy(step, False).start()

    def face_wait(step):
        face_copy(step, True).wait_recv()

    sum_peers = (peer_core, peer_x, peer_y, (fs, dp_pair), (fs, dp_far))

    def sum_copy(step):
        return side(8 + step, small_sum.at[step], small_land.at[step], sum_peers[step])

    def sum_start(step):
        sum_copy(step).start()

    def sum_wait(step):
        sum_copy(step).wait_recv()
        small_sum[step + 1] = small_sum[step] + small_land[step]

    def grad(unit, rows):
        if unit == D_UNIT:
            return sdn.at[rows, :]
        if unit >= 4:
            return act.at[rows, pl.ds(768 * (unit - 4), 768)]
        return wts.at[4 + unit, rows, :]

    def shape_of(unit):
        return 384 if unit == D_UNIT else 96

    def piece_shard(delta, which):
        chip_x = (xb + delta % 2) - 2 * xb * (delta % 2)
        chip_y = (yb + delta // 2) - 2 * yb * (delta // 2)
        return (chip_y * 2 + chip_x) * 2 + which

    def piece(unit, delta, which, part=None):
        size = shape_of(unit)
        shard = piece_shard(delta, which)
        if part is None:
            return grad(unit, span(size * shard, size))
        return grad(unit, span(size * shard + (size // 2) * part, size // 2))

    def lands(pair, unit, slot):
        wide, down_only = pair
        return down_only.at[slot] if unit == D_UNIT else wide.at[unit, slot]

    def accumulate(dst, *sources):
        rows = dst.shape[0]

        def body(i, carry):
            r = span(i * 48, 48)
            value = dst[r, :].astype(F32)
            for source in sources:
                value = value + source[r, :].astype(F32)
            dst[r, :] = value.astype(BF)
            return carry

        lax.fori_loop(0, rows // 48, body, 0)

    def core_copy(unit, delta):
        return pltpu.make_async_remote_copy(
            src_ref=piece(unit, delta, 1 - core),
            dst_ref=lands((lc, lcd), unit, delta),
            send_sem=core_send.at[unit, delta],
            recv_sem=core_recv.at[unit, delta],
            device_id=peer_core,
            device_id_type=MESH_ID,
        )

    def rs_core(unit):
        for delta in (3, 2, 1, 0):
            core_copy(unit, delta).start()

    xy_kinds = (
        (3, 0, (lx, lxd), 0, peer_x),
        (3, 1, (ly, lyd), 0, peer_y),
        (1, 0, (lx, lxd), 1, peer_x),
        (2, 1, (ly, lyd), 1, peer_y),
        (2, 0, (ly, lyd), 2, peer_y),
        (1, 1, (lx, lxd), 2, peer_x),
    )

    def xy_copy(unit, kind):
        delta, part, pair, slot, peer = xy_kinds[kind]
        return pltpu.make_async_remote_copy(
            src_ref=piece(unit, delta, core, part),
            dst_ref=lands(pair, unit, slot),
            send_sem=xy_send.at[unit, kind],
            recv_sem=xy_recv.at[unit, kind],
            device_id=peer,
            device_id_type=MESH_ID,
        )

    def rs_first_piece(unit, delta):
        core_copy(unit, delta).wait_recv()
        accumulate(piece(unit, delta, core), lands((lc, lcd), unit, delta))
        for kind in {3: (0, 1), 1: (2,), 2: (3,), 0: ()}[delta]:
            xy_copy(unit, kind).start()

    def rs_first(unit):
        for delta in (3, 2, 1, 0):
            rs_first_piece(unit, delta)

    def rs_second(unit):
        xy_copy(unit, 0).wait_recv()
        accumulate(piece(unit, 2, core, 0), lands((lx, lxd), unit, 0))
        xy_copy(unit, 4).start()
        xy_copy(unit, 1).wait_recv()
        accumulate(piece(unit, 1, core, 1), lands((ly, lyd), unit, 0))
        xy_copy(unit, 5).start()

    def z_copy(unit, index, src, slot, target):
        return pltpu.make_async_remote_copy(
            src_ref=src,
            dst_ref=lands((lz, lzd), unit, slot),
            send_sem=z_send.at[unit, index],
            recv_sem=z_recv.at[unit, slot],
            device_id=(fs, target),
            device_id_type=MESH_ID,
        )

    def z_land(unit, slot):
        return lands((lz, lzd), unit, slot)

    def z_wait(unit, slot):
        z_copy(unit, 0, z_land(unit, slot), slot, dp_pair).wait_recv()

    def z_out(unit, index):
        own_far = piece(unit, 0, core, far)
        own_near = piece(unit, 0, core, near)
        end = {
            0: (own_far, 1, dp_inner),
            1: (own_near, 0, dp_inner),
        }
        mid = {
            0: (own_far, 2, dp_mid),
            1: (z_land(unit, 2), 2, dp_end),
            2: (z_land(unit, 2), 3, dp_mid),
            3: (z_land(unit, 3), 3, dp_end),
        }
        return end.get(index), mid[index]

    def z_end(unit, index):
        return z_copy(unit, index, *z_out(unit, index)[0])

    def z_mid(unit, index):
        return z_copy(unit, index, *z_out(unit, index)[1])

    def rs_own(unit):
        for kind in (2, 3, 4, 5):
            xy_copy(unit, kind).wait_recv()
        accumulate(piece(unit, 0, core, 0), lands((lx, lxd), unit, 1), lands((ly, lyd), unit, 2))
        accumulate(piece(unit, 0, core, 1), lands((ly, lyd), unit, 1), lands((lx, lxd), unit, 2))

        @pl.when(is_end)
        def _():
            z_end(unit, 0).start()
            z_end(unit, 1).start()

    def rs_z2(unit):
        @pl.when(is_mid)
        def _():
            z_wait(unit, 1)
            accumulate(piece(unit, 0, core, far), z_land(unit, 1))
            z_mid(unit, 0).start()

    def rs_z3(unit):
        @pl.when(is_mid)
        def _():
            z_wait(unit, 0)
            z_wait(unit, 2)
            accumulate(z_land(unit, 2), z_land(unit, 0), piece(unit, 0, core, near))
            z_mid(unit, 1).start()
            z_mid(unit, 2).start()

    def rs_z4(unit):
        @pl.when(is_mid)
        def _():
            z_wait(unit, 3)
            z_mid(unit, 3).start()

    def result_copy(unit, slot):
        size = shape_of(unit) // 2
        rows = span(size * (near if slot == 2 else far), size)
        target = down_out.at[rows, :] if unit == D_UNIT else units_out.at[unit, rows, :]
        return pltpu.make_async_copy(z_land(unit, slot), target, local_sem.at[16 + 2 * unit + slot - 2])

    def rs_done(unit):
        @pl.when(is_end)
        def _():
            z_wait(unit, 2)
            z_wait(unit, 3)

        for slot in (2, 3):
            result_copy(unit, slot).start()

    for unit in range(3):
        ag_own(unit)
    param_start(0)

    img_h = gm
    img_k = att
    img_v = h1
    img_gain[0:2, :] = pgain_ref[...].astype(F32)
    img_gain[2:8, :] = pshift_ref[...].astype(F32)
    phidden = phidden_ref[...].astype(F32)
    for q in range(24):
        img_gain[8 + q // 6 : 9 + q // 6, 128 * (q % 6) : 128 * (q % 6) + 128] = phidden[q : q + 1, :]
    img_h[pl.ds(400, 112), :] = jnp.zeros((112, 768), BF)
    patches_copy.wait()

    def image_normed(values):
        return norm_rows(values)[0] * img_gain[0:1, :] + img_gain[6:7, :]

    first_rows = img_h[pl.ds(512, 16), :].astype(F32)[0:8, :]
    face_rows[0] = first_rows
    face_rows[1] = image_normed(first_rows)

    def image_norm(i):
        img_h[span(80 * i, 80), :] = image_normed(img_h[span(512 + 80 * i, 80), :].astype(F32)).astype(BF)

    loop(5, image_norm)
    pqkv_copy.wait()

    def image_kv(i):
        r = span(i * TILE, TILE)
        img_k[r, :] = nn(img_h[r, :], act[pl.ds(0, 768), pl.ds(768, 768)]).astype(BF)
        img_v[r, :] = (nn(img_h[r, :], act[pl.ds(0, 768), pl.ds(1536, 768)]) + img_gain[3:4, :]).astype(BF)

    loop(2, image_kv)
    param_wait(0)
    param_start(1)
    pump(0)

    lane_head = lax.broadcasted_iota(jnp.int32, (8, 768), 1) // 64
    img_q = (nn(face_rows[1].astype(BF), act[pl.ds(0, 768), pl.ds(0, 768)]) + img_gain[2:3, :]) * 0.125
    img_q = img_q.astype(BF).astype(F32)
    stacked = jnp.concatenate([jnp.where(lane_head == h, img_q, 0.0) for h in range(12)], axis=0).astype(BF)
    scores = nt(stacked, img_k[pl.ds(0, 512), :])
    token = lax.broadcasted_iota(jnp.int32, (96, 512), 1)
    image_of = lax.broadcasted_iota(jnp.int32, (96, 512), 0) % 8
    scores = jnp.where((token % 8 == image_of) & (token < 400), scores, -1e30)
    expd = jnp.exp(scores - jnp.max(scores, axis=-1, keepdims=True))
    probs = (expd / jnp.sum(expd, axis=-1, keepdims=True)).astype(BF)
    mixed = nn(probs, img_v[pl.ds(0, 512), :])
    joined = jnp.zeros((8, 768), F32)
    for h in range(12):
        joined = joined + jnp.where(lane_head == h, mixed[8 * h : 8 * h + 8, :], 0.0)
    param_wait(1)
    param_start(2)
    pump(1)
    pout_copy.wait()
    middle = face_rows[0] + (nn(joined.astype(BF), act[pl.ds(0, 768), pl.ds(2304, 768)]) + img_gain[4:5, :])
    scaled, _ = norm_rows(middle)
    normed = (scaled * img_gain[1:2, :] + img_gain[7:8, :]).astype(BF)
    face_rows[0] = middle
    pup_copy.wait()
    for j in range(4):
        hidden = nn(normed, dg[pl.ds(0, 768), pl.ds(768 * j, 768)]) + img_gain[8 + j : 9 + j, :]
        face_rows[2 + j] = hidden * normal_cdf(hidden)
    pump(2)
    pdown_copy.wait()
    total = face_rows[0] + img_gain[5:6, :]
    for j in range(4):
        total = total + nn(face_rows[2 + j].astype(BF), sdn[pl.ds(768 * j, 768), :])
    unit_norm = total * lax.rsqrt(jnp.mean(total * total, axis=-1, keepdims=True) + 1e-06)
    faces[span(64 * dp + 8 * fs, 8, 8), :] = unit_norm.astype(BF).astype(F32)
    face_start(0)
    param_wait(2)

    flat_small = small_in[...].reshape(128, 128).astype(BF)
    for r in range(4):
        lane = lax.broadcasted_iota(jnp.int32, (128, 384), 0)
        column = lax.broadcasted_iota(jnp.int32, (128, 384), 1)
        pick = jnp.where((column == lane + 96 * r) & (lane < 96), 1.0, 0.0).astype(BF)
        spread = nn(flat_small, pick)
        for block in range(2):
            shard = 4 * block + r
            value = spread[16 * shard : 16 * shard + 8, :]
            cols = slice(384 * block, 384 * block + 384)
            if r == 0:
                params[0:8, cols] = value
            else:
                params[0:8, cols] = params[0:8, cols] + value
    for shard in range(8):
        for q in range(3):
            at = 384 * (shard % 2) + 128 * q
            params[8 + shard // 2 : 9 + shard // 2, at : at + 128] = small_in[shard, 8 + q : 9 + q, :]

    x_copy.wait()
    for copy in own_copies:
        copy.wait()

    def first_norm(i):
        r = span(32 * i, 32)
        scaled, _ = norm_rows(h2[r, :].astype(F32))
        h1[r, :] = (scaled * params[0:1, :] + params[6:7, :]).astype(BF)

    loop(32, first_norm)
    for group in range(8):
        rows = [segment_ref[2 * group + k : 2 * group + k + 1, :] + CAPS * (2 * group + k) for k in range(2)]
        same = lax.broadcasted_iota(jnp.int32, (64, 128), 0) == jnp.concatenate(rows, axis=1)
        member[:, 128 * group : 128 * group + 128] = jnp.where(same, 1.0, 0.0).astype(BF)
    face_wait(0)
    face_start(1)
    pump(3)

    def project(j):
        def body(i):
            r = span(TILE * i, TILE)
            value = nn(h1[r, :], wts[j])
            if j == 0:
                value = (value + params[2:3, :]) * 0.125
            if j == 2:
                value = value + params[3:4, :]
            qkv[r, pl.ds(768 * j, 768)] = value.astype(BF)

        loop(4, body)

    ready(0)
    project(0)
    ready(1)
    project(1)
    pump(4)
    ready(2)
    project(2)
    face_wait(1)
    face_start(2)

    low_lane = lax.broadcasted_iota(jnp.int32, (128, 128), 1) < 64
    zero_block = jnp.zeros((128, 128), BF)

    def split_heads(block):
        return jnp.concatenate(
            [jnp.where(low_lane, block, zero_block), jnp.where(low_lane, zero_block, block)], axis=0
        )

    def join_heads(value):
        return jnp.where(low_lane, value[0:128, :], value[128:256, :])

    def same_caption(group):
        part = member[:, span(128 * group, 128, 128)]
        same = tn(part, part)
        return jnp.concatenate([same, same], axis=0) > 0.5

    def attention_probs(same, queries, keys):
        value = jnp.where(same, nt(queries, keys), -1e30)
        expd = jnp.exp(value - jnp.max(value, axis=-1, keepdims=True))
        return expd * (1.0 / jnp.sum(expd, axis=-1, keepdims=True))

    def attend(group):
        r = span(128 * group, 128)
        same = same_caption(group)
        for hp in range(6):
            queries = split_heads(qkv[r, pl.ds(128 * hp, 128)])
            probs = attention_probs(same, queries, qkv[r, pl.ds(768 + 128 * hp, 128)])
            mixed = nn(probs.astype(BF), qkv[r, pl.ds(1536 + 128 * hp, 128)])
            att[r, pl.ds(128 * hp, 128)] = join_heads(mixed).astype(BF)

    loop(8, attend, {1: [lambda: pump(5)], 4: [lambda: pump(6)], 7: [lambda: pump(7)]})
    face_wait(2)
    face_start(3)
    ready(3)

    def out_project(i):
        r = span(TILE * i, TILE)
        x1[r, :] = h2[r, :].astype(F32) + (nn(att[r, :], wts[3]) + params[4:5, :])

    loop(4, out_project)

    def second_norm(i):
        r = span(32 * i, 32)
        scaled, _ = norm_rows(x1[r, :])
        h2[r, :] = (scaled * params[1:2, :] + params[7:8, :]).astype(BF)

    loop(32, second_norm)
    face_wait(3)
    face_start(4)
    pump(8)

    def widen(j):
        def body(i):
            r = span(TILE * i, TILE)
            work[...] = nn(h2[r, :], wts[4 + j]) + params[8 + j : 9 + j, :]

            def gelu(k):
                inner = span(16 * k, 16)
                hidden = work[inner, :]
                cdf = normal_cdf(hidden)
                outer = span(TILE * i + 16 * k, 16)
                act[outer, pl.ds(768 * j, 768)] = (hidden * cdf).astype(BF)
                slope = cdf + hidden * (jnp.exp(-0.5 * hidden * hidden) * (1.0 / math.sqrt(2.0 * math.pi)))
                dg[outer, pl.ds(768 * j, 768)] = slope.astype(BF)

            loop(16, gelu)

        loop(4, body)

    for j in range(4):
        ready(4 + j)
        widen(j)
        if j < 2:
            pump(9 + j)
        elif j == 2:
            ag_last(10)
    face_wait(4)

    for jd in range(3):
        ready(8 + jd)
        cols = pl.ds(256 * jd, 256)

        def narrow(i, cols=cols, jd=jd):
            r = span(TILE * i, TILE)
            value = nn(act[r, :], wdn[:, cols]) + params[5:6, 256 * jd : 256 * jd + 256]
            value = x1[r, cols] + value
            top = value.astype(BF)
            rest = (value - top.astype(F32)).astype(BF)
            lanes = span(TILE * i, TILE, 128)
            piece_sum = nn(member[:, lanes], top) + nn(member[:, lanes], rest)

            @pl.when(i == 0)
            def _():
                pooled[:, cols] = piece_sum

            @pl.when(i > 0)
            def _():
                pooled[:, cols] = pooled[:, cols] + piece_sum

        loop(4, narrow)

    count = jnp.sum(member[...].astype(F32), axis=-1, keepdims=True)
    mean_rows = pooled[...] / count
    inverse = lax.rsqrt(jnp.mean(mean_rows * mean_rows, axis=-1, keepdims=True) + 1e-06)
    embed = mean_rows * inverse
    face_all = faces[...].astype(BF)
    amount = sharp_ref[0] * (1.0 / math.sqrt(768.0))
    match = amount * nt(embed.astype(BF), face_all) + offset_ref[0]
    slot = lax.broadcasted_iota(jnp.int32, (64, 256), 1)
    image_id = ((slot // 8) % 8) * 32 + (slot // 64) * 8 + slot % 8
    diagonal = lax.broadcasted_iota(jnp.int32, (64, 64), 0) == lax.broadcasted_iota(jnp.int32, (64, 64), 1)
    described = jnp.where(diagonal, described_ref[...].astype(F32), 0.0)
    positive = jnp.sum(described, axis=-1, keepdims=True) == image_id.astype(F32)
    signed = jnp.where(positive, -match, match)
    terms = jnp.maximum(signed, 0.0) + jnp.log1p(jnp.exp(-jnp.abs(signed)))
    row_loss = jnp.sum(terms, axis=-1, keepdims=True) * (1.0 / 256.0)
    loss_out[...] = jnp.sum(jnp.where(diagonal, row_loss, 0.0), axis=0, keepdims=True)
    slope = ((jax.nn.sigmoid(match) - jnp.where(positive, 1.0, 0.0)) * amount).astype(BF)
    grad_embed = nn(slope, face_all)
    grad_pooled = inverse * (grad_embed - embed * jnp.mean(grad_embed * embed, axis=-1, keepdims=True))
    per_caption = grad_pooled / count
    caption_hi[...] = per_caption.astype(BF)
    caption_lo[...] = (per_caption - caption_hi[...].astype(F32)).astype(BF)

    def spread_down(i):
        gm[span(TILE * i, TILE), :] = tn(member[:, span(TILE * i, TILE, 128)], caption_hi[...]).astype(BF)

    loop(4, spread_down)

    for unit in range(N_AG):
        for kind in range(9):
            ag_out(unit, kind).wait_send()
    for step in range(3):
        start, sent, peer, _ = param_steps[step]
        param_copy(step, start, sent, peer).wait_send()
    for step in range(5):
        face_copy(step, False).wait_send()

    ones = jnp.ones((16, 1024), BF)

    def column_sum(value):
        return nn(ones, value)[0:1, :]

    def down_piece(delta):
        def body(i):
            which = (1 - core) + i * (2 * core - 1)
            shard = piece_shard(delta, which)
            sdn[span(384 * shard, 384), :] = tn(act[:, span(384 * shard, 384, 128)], gm[...]).astype(BF)

            @pl.when(i == 0)
            def _():
                core_copy(D_UNIT, delta).start()

        loop(2, body)

    down_piece(3)
    down_piece(2)
    rs_first_piece(D_UNIT, 3)
    down_piece(1)
    rs_first_piece(D_UNIT, 2)
    down_piece(0)
    rs_first_piece(D_UNIT, 1)
    rs_first_piece(D_UNIT, 0)

    def hidden_back(i):
        r = span(TILE * i, TILE)
        for jj in range(3):
            cols = pl.ds(1024 * jj, 1024)
            value = nt(gm[r, :], wdn[pl.ds(1024 * jj, 1024), :])
            dg[r, cols] = (dg[r, cols].astype(F32) * value).astype(BF)

    loop(4, hidden_back, {1: [lambda: rs_second(D_UNIT)]})
    partial_rows = {}

    def up_unit(j):
        def body(i):
            act[span(TILE * i, TILE), pl.ds(768 * j, 768)] = tn(
                h2[:, span(TILE * i, TILE, 128)], dg[:, pl.ds(768 * j, 768)]
            ).astype(BF)

        loop(3, body)
        rs_core(4 + j)
        small_sum[0, 8 + j : 9 + j, :] = column_sum(dg[:, pl.ds(768 * j, 768)])

    up_unit(0)
    up_unit(1)
    rs_first(4)
    up_unit(2)
    rs_first(5)
    up_unit(3)
    rs_first(6)
    rs_own(D_UNIT)
    small_sum[0, 5:6, :] = column_sum(gm[...])
    partial[...] = jnp.zeros((4, 8, 768), F32)

    def fold(value):
        return value.reshape(value.shape[0] // 8, 8, 768).sum(axis=0)

    def middle_back(i):
        r = span(TILE * i, TILE)
        total = nt(dg[r, pl.ds(0, 768)], wts[4])
        for j in range(1, 4):
            total = total + nt(dg[r, pl.ds(768 * j, 768)], wts[4 + j])
        work[...] = total
        faces[...] = tn(member[:, span(TILE * i, TILE, 128)], caption_lo[...])

        def rows_back(k):
            inner = span(ROWS * k, ROWS)
            outer = span(TILE * i + ROWS * k, ROWS)
            upstream = work[inner, :]
            scaled, inverse = norm_rows(x1[outer, :])
            partial[0] = partial[0] + fold(upstream * scaled)
            partial[1] = partial[1] + fold(upstream)
            weighted = upstream * params[1:2, :]
            first_mean = jnp.mean(weighted, axis=-1, keepdims=True)
            second_mean = jnp.mean(weighted * scaled, axis=-1, keepdims=True)
            value = gm[outer, :].astype(F32) + faces[inner, :]
            value = value + inverse * (weighted - first_mean - scaled * second_mean)
            x1[outer, :] = value
            gm[outer, :] = value.astype(BF)

        loop(TILE // ROWS, rows_back)

    loop(
        4,
        middle_back,
        {
            0: [lambda: rs_first(7)],
            1: [lambda: rs_second(4)],
            2: [lambda: rs_z2(D_UNIT)],
            3: [lambda: rs_second(5)],
        },
    )
    x_again = pltpu.make_async_copy(x_hbm, h2, local_sem.at[15])
    x_again.start()

    def out_unit(i):
        wts[7, span(TILE * i, TILE), :] = tn(att[:, span(TILE * i, TILE, 128)], gm[...]).astype(BF)

    loop(3, out_unit)
    rs_core(3)
    small_sum[0, 4:5, :] = column_sum(gm[...])

    def attended_back(i):
        r = span(TILE * i, TILE)
        att[r, :] = nt(gm[r, :], wts[3]).astype(BF)

    loop(4, attended_back)
    rs_second(6)
    rs_first(3)
    rs_own(4)
    rs_z3(D_UNIT)

    def attend_back(quad):
        def chain(group, same, half):
            r = span(128 * group, 128)
            at = 256 * quad + 128 * half
            qs = pl.ds(at, 128)
            queries = split_heads(qkv[r, qs])
            keys = qkv[r, pl.ds(768 + at, 128)]
            upstream = split_heads(att[r, qs])
            probs = attention_probs(same, queries, keys)
            probs_grad = nt(upstream, qkv[r, pl.ds(1536 + at, 128)])
            inner = jnp.sum(probs * probs_grad, axis=-1, keepdims=True)
            score_grad = (probs * (probs_grad - inner)).astype(BF)
            to = 768 * quad + 128 * half
            dg[r, pl.ds(to + 512, 128)] = tn(probs.astype(BF), upstream).astype(BF)
            dg[r, pl.ds(to + 256, 128)] = tn(score_grad, queries).astype(BF)
            query_grad = join_heads(nn(score_grad, keys)).astype(BF).astype(F32)
            dg[r, pl.ds(to, 128)] = (query_grad * 0.125).astype(BF)

        def body(i):
            for group in range(GROUPS):
                same = same_caption(GROUPS * i + group)
                for half in range(2):
                    chain(GROUPS * i + group, same, half)

        return body

    def qkv_unit(quad):
        def body(i):
            wts[4 + quad, span(TILE * i, TILE), :] = tn(
                h1[:, span(TILE * i, TILE, 128)], dg[:, pl.ds(768 * quad, 768)]
            ).astype(BF)

        loop(3, body)
        rs_core(quad)

    loop(
        8 // GROUPS,
        attend_back(0),
        {
            1: [lambda: rs_z2(4), lambda: rs_own(5), lambda: rs_second(7)],
            3: [lambda: rs_z2(5), lambda: rs_z3(4), lambda: rs_own(6), lambda: rs_second(3)],
        },
    )
    qkv_unit(0)
    loop(
        8 // GROUPS,
        attend_back(1),
        {
            0: [lambda: rs_first(0)],
            1: [lambda: rs_z4(D_UNIT), lambda: rs_z2(6), lambda: rs_z3(5), lambda: rs_own(7)],
            3: [lambda: rs_second(0), lambda: rs_z2(7), lambda: rs_z3(6), lambda: rs_z4(4), lambda: rs_own(3)],
        },
    )
    qkv_unit(1)
    loop(
        8 // GROUPS,
        attend_back(2),
        {
            0: [lambda: rs_first(1), lambda: rs_z2(3)],
            1: [lambda: rs_own(0), lambda: rs_z3(7), lambda: rs_z4(5)],
            3: [lambda: rs_second(1), lambda: rs_z2(0), lambda: rs_z3(3), lambda: rs_z4(6)],
        },
    )
    qkv_unit(2)
    rs_own(1)
    rs_z3(0)
    rs_z4(7)
    rs_first(2)
    for quad in range(3):
        to = slice(256 * quad, 256 * quad + 256)
        small_sum[0, 2:3, to] = column_sum(dg[:, pl.ds(768 * quad, 256)])
        small_sum[0, 3:4, to] = column_sum(dg[:, pl.ds(768 * quad + 512, 256)])
    x_again.wait()

    def input_back(i):
        r = span(TILE * i, TILE)
        total = jnp.zeros((TILE, 768), F32)
        for quad in range(3):
            for j in range(3):
                part = dg[r, pl.ds(768 * quad + 256 * j, 256)]
                total = total + nt(part, wts[j, :, pl.ds(256 * quad, 256)])
        work[...] = total

        def rows_back(k):
            inner = span(ROWS * k, ROWS)
            outer = span(TILE * i + ROWS * k, ROWS)
            upstream = work[inner, :]
            scaled, inverse = norm_rows(h2[outer, :].astype(F32))
            partial[2] = partial[2] + fold(upstream * scaled)
            partial[3] = partial[3] + fold(upstream)
            weighted = upstream * params[0:1, :]
            first_mean = jnp.mean(weighted, axis=-1, keepdims=True)
            second_mean = jnp.mean(weighted * scaled, axis=-1, keepdims=True)
            value = x1[outer, :] + inverse * (weighted - first_mean - scaled * second_mean)
            att[outer, :] = value.astype(BF)

        loop(TILE // ROWS, rows_back)

    loop(
        4,
        input_back,
        {
            0: [lambda: rs_second(2), lambda: rs_z2(1), lambda: rs_z4(3)],
            1: [lambda: rs_own(2), lambda: rs_z4(0)],
            2: [lambda: rs_z3(1)],
            3: [lambda: rs_z2(2)],
        },
    )
    input_copy = pltpu.make_async_copy(att, input_out, local_sem.at[34])
    input_copy.start()
    for row, index in ((0, 2), (1, 0), (6, 3), (7, 1)):
        small_sum[0, row : row + 1, :] = jnp.sum(partial[index], axis=0, keepdims=True)
    small_sum[0, 12:16, :] = jnp.zeros((4, 768), F32)
    sum_start(0)
    rs_z4(1)
    rs_z3(2)
    sum_wait(0)
    sum_start(1)
    for unit in (D_UNIT, 4, 5, 6, 7, 3, 0):
        rs_done(unit)
    sum_wait(1)
    sum_start(2)
    rs_z4(2)
    sum_wait(2)
    sum_start(3)
    rs_done(1)
    sum_wait(3)
    sum_start(4)
    rs_done(2)
    sum_wait(4)
    small_out[...] = small_sum[5]

    input_copy.wait()
    for unit in range(9):
        for slot in (2, 3):
            result_copy(unit, slot).wait()
        for delta in range(4):
            core_copy(unit, delta).wait_send()
        for kind in range(6):
            xy_copy(unit, kind).wait_send()

        @pl.when(is_end)
        def _(unit=unit):
            for index in range(2):
                z_end(unit, index).wait_send()

        @pl.when(is_mid)
        def _(unit=unit):
            for index in range(4):
                z_mid(unit, index).wait_send()

    for step in range(5):
        sum_copy(step).wait_send()


def finish_kernel(
    units_hbm,
    down_hbm,
    input_hbm,
    small_ref,
    loss_ref,
    qkv_out,
    out_out,
    up_out,
    down_out,
    gain_out,
    shift_out,
    hidden_out,
    input_out,
    loss_out,
    units,
    down,
    tokens,
    qkv,
    out,
    up,
    down_wide,
    sem,
):
    fs = lax.axis_index("fsdp")

    def move(src, dst, index):
        copy = pltpu.make_async_copy(src, dst, sem.at[index])
        copy.start()
        return copy

    units_in = move(units_hbm, units, 0)
    down_in = move(down_hbm, down, 1)
    tokens_in = move(input_hbm, tokens, 2)
    for shard in range(8):

        @pl.when(fs == shard)
        def _(shard=shard):
            gain_out[...] = small_ref[0:2, 96 * shard : 96 * shard + 96]
            shift_out[...] = small_ref[2:8, 96 * shard : 96 * shard + 96]
            for q in range(3):
                at = 384 * (shard % 2) + 128 * q
                hidden_out[q : q + 1, :] = small_ref[8 + shard // 2 : 9 + shard // 2, at : at + 128]

    loss_out[...] = loss_ref[...]
    units_in.wait()
    for quad in range(3):
        for j in range(3):
            at = 768 * j + 256 * quad
            qkv[:, at : at + 256] = units[quad, :, 256 * j : 256 * j + 256].astype(F32)
    moves = [move(qkv, qkv_out, 3)]
    out[...] = units[3].astype(F32)
    moves.append(move(out, out_out, 4))
    for j in range(4):
        up[:, 768 * j : 768 * j + 768] = units[4 + j].astype(F32)
    moves.append(move(up, up_out, 5))
    down_in.wait()
    down_wide[...] = down[...].astype(F32)
    moves.append(move(down_wide, down_out, 6))
    tokens_in.wait()
    moves.append(move(tokens, input_out, 7))
    for copy in moves:
        copy.wait()


def fused_step(
    incoming_word_states,
    sentence_number_per_word,
    described_picture,
    lookup_matrices,
    mixer_exit_matrix,
    widening_matrix,
    narrowing_matrix,
    normalizer_multipliers,
    word_offsets,
    widened_offset,
    picture_patches,
    picture_lookup_matrices,
    picture_mixer_exit_matrix,
    picture_widening_matrix,
    picture_narrowing_matrix,
    picture_normalizer_multipliers,
    picture_offsets,
    picture_widened_offset,
    sharpness_coefficient,
    objective_offset,
):
    rows, length, width = incoming_word_states.shape
    tokens = rows * length
    vmem = pl.BlockSpec(memory_space=pltpu.VMEM)
    hbm = pl.BlockSpec(memory_space=pl.ANY)
    smem = pl.BlockSpec(memory_space=pltpu.SMEM)
    dma = pltpu.SemaphoreType.DMA
    outs = pl.pallas_call(
        fused_kernel,
        out_shape=(
            jax.ShapeDtypeStruct((8, 96, width), BF),
            jax.ShapeDtypeStruct((384, width), BF),
            jax.ShapeDtypeStruct((tokens, width), BF),
            jax.ShapeDtypeStruct((16, width), F32),
            jax.ShapeDtypeStruct((1, 64), F32),
        ),
        in_specs=[smem, smem, hbm, vmem, vmem, *[hbm] * 4, *[vmem] * 3, *[hbm] * 5, *[vmem] * 3],
        out_specs=(hbm, hbm, hbm, vmem, vmem),
        scratch_shapes=[
            pltpu.VMEM((8, 768, 768), BF),
            pltpu.VMEM((3072, 768), BF),
            pltpu.VMEM((1024, 768), BF),
            pltpu.VMEM((1024, 2304), BF),
            pltpu.VMEM((1024, 768), BF),
            pltpu.VMEM((1024, 768), F32),
            pltpu.VMEM((1024, 768), BF),
            pltpu.VMEM((1024, 3072), BF),
            pltpu.VMEM((1024, 3072), BF),
            pltpu.VMEM((1024, 768), BF),
            pltpu.VMEM((3072, 768), BF),
            pltpu.VMEM((8, 4, 96, 768), BF),
            pltpu.VMEM((4, 384, 768), BF),
            pltpu.VMEM((8, 3, 48, 768), BF),
            pltpu.VMEM((3, 192, 768), BF),
            pltpu.VMEM((8, 3, 48, 768), BF),
            pltpu.VMEM((3, 192, 768), BF),
            pltpu.VMEM((8, 4, 48, 768), BF),
            pltpu.VMEM((4, 192, 768), BF),
            pltpu.VMEM((TILE, 768), F32),
            pltpu.VMEM((TILE, 768), F32),
            pltpu.VMEM((8, 16, 128), F32),
            pltpu.VMEM((16, 768), F32),
            pltpu.VMEM((16, 768), F32),
            pltpu.VMEM((64, 1024), BF),
            pltpu.VMEM((64, 768), F32),
            pltpu.VMEM((64, 768), BF),
            pltpu.VMEM((64, 768), BF),
            pltpu.VMEM((4, 8, 768), F32),
            pltpu.VMEM((6, 16, 768), F32),
            pltpu.VMEM((5, 16, 768), F32),
            pltpu.VMEM((6, 8, 768), F32),
            dma((N_AG, 9)),
            dma((N_AG, 9)),
            dma((9, 4)),
            dma((9, 4)),
            dma((9, 6)),
            dma((9, 6)),
            dma((9, 4)),
            dma((9, 4)),
            dma((13,)),
            dma((13,)),
            dma((35,)),
        ],
        compiler_params=pltpu.CompilerParams(
            collective_id=0, has_side_effects=True, vmem_limit_bytes=67043328
        ),
        name="lit_step",
    )(
        sharpness_coefficient,
        objective_offset,
        incoming_word_states.reshape(tokens, width),
        sentence_number_per_word,
        described_picture.reshape(1, -1),
        lookup_matrices,
        mixer_exit_matrix,
        widening_matrix,
        narrowing_matrix,
        normalizer_multipliers,
        word_offsets,
        widened_offset.reshape(3, 128),
        picture_patches.transpose(1, 0, 2).reshape(-1, width),
        picture_lookup_matrices,
        picture_mixer_exit_matrix,
        picture_widening_matrix,
        picture_narrowing_matrix,
        picture_normalizer_multipliers,
        picture_offsets,
        picture_widened_offset.reshape(24, 128),
    )
    finished = pl.pallas_call(
        finish_kernel,
        out_shape=(
            jax.ShapeDtypeStruct((96, 2304), F32),
            jax.ShapeDtypeStruct((96, width), F32),
            jax.ShapeDtypeStruct((96, 3072), F32),
            jax.ShapeDtypeStruct((384, width), F32),
            jax.ShapeDtypeStruct((2, 96), F32),
            jax.ShapeDtypeStruct((6, 96), F32),
            jax.ShapeDtypeStruct((3, 128), F32),
            jax.ShapeDtypeStruct((tokens, width), BF),
            jax.ShapeDtypeStruct((1, 64), F32),
        ),
        in_specs=[hbm, hbm, hbm, vmem, vmem],
        out_specs=(hbm, hbm, hbm, hbm, vmem, vmem, vmem, hbm, vmem),
        scratch_shapes=[
            pltpu.VMEM((8, 96, width), BF),
            pltpu.VMEM((384, width), BF),
            pltpu.VMEM((tokens, width), BF),
            pltpu.VMEM((96, 2304), F32),
            pltpu.VMEM((96, width), F32),
            pltpu.VMEM((96, 3072), F32),
            pltpu.VMEM((384, width), F32),
            dma((8,)),
        ],
        compiler_params=pltpu.CompilerParams(vmem_limit_bytes=60 * 2**20),
        name="lit_finish",
    )(*outs)
    finished = list(finished)
    finished[6] = finished[6].reshape(-1)
    finished[7] = finished[7].reshape(rows, length, width)
    finished[8] = finished[8].reshape(-1)
    return tuple(finished)


def solution(mesh):
    fits = mesh.shape["fsdp"] == 8 and mesh.shape["dp"] == 4
    return jax.shard_map(
        fused_step if fits else per_device,
        mesh=mesh,
        in_specs=(
            P(("fsdp", "dp"), None, None),
            P(("fsdp", "dp"), None),
            P(("fsdp", "dp")),
            P("fsdp", None),
            P("fsdp", None),
            P("fsdp", None),
            P("fsdp", None),
            P(None, "fsdp"),
            P(None, "fsdp"),
            P("fsdp"),
            P(("fsdp", "dp"), None, None),
            P(),
            P(),
            P(),
            P(),
            P(),
            P(),
            P(),
            P(),
            P(),
        ),
        out_specs=(
            P("fsdp", None),
            P("fsdp", None),
            P("fsdp", None),
            P("fsdp", None),
            P(None, "fsdp"),
            P(None, "fsdp"),
            P("fsdp"),
            P(("fsdp", "dp"), None, None),
            P(("fsdp", "dp")),
        ),
        check_vma=False,
    )
```

```python
import math

import jax
import jax.numpy as jnp
from jax import lax
from jax.experimental import pallas as pl
from jax.experimental.pallas import tpu as pltpu
from jax.sharding import PartitionSpec as P

HEAD_DIM = 64
CAPS = 4


def layer_norm(values, gain, shift):
    centred = values - jnp.mean(values, axis=-1, keepdims=True)
    inverse = lax.rsqrt(jnp.mean(centred * centred, axis=-1, keepdims=True) + 1e-06)
    scaled = centred * inverse
    return (scaled * gain + shift, scaled, inverse)


def norm_back(grad_scaled, scaled, inverse):
    first_mean = jnp.mean(grad_scaled, axis=-1, keepdims=True)
    second_mean = jnp.mean(grad_scaled * scaled, axis=-1, keepdims=True)
    return inverse * (grad_scaled - first_mean - scaled * second_mean)


def gelu_exact(values):
    return jax.nn.gelu(values, approximate=False)


def forward_block(flat, rows, length, mask, weights):
    qkv_w, out_w, up_w, down_w, gains_low, biases_low, up_b = weights
    gains = gains_low.astype(jnp.float32)
    biases = biases_low.astype(jnp.float32)
    channel_count = flat.shape[-1]
    heads = channel_count // HEAD_DIM
    scale = 1.0 / math.sqrt(HEAD_DIM)
    first, scaled_one, inverse_one = layer_norm(flat, gains[0], biases[4])
    first_low = first.astype(jnp.bfloat16)
    mixed = jnp.dot(first_low, qkv_w, preferred_element_type=jnp.float32)
    query = (
        ((mixed[:, :channel_count] + biases[0]) * scale)
        .astype(jnp.bfloat16)
        .reshape(rows, length, heads, HEAD_DIM)
    )
    key_low = (
        mixed[:, channel_count : 2 * channel_count]
        .astype(jnp.bfloat16)
        .reshape(rows, length, heads, HEAD_DIM)
    )
    value_low = (
        (mixed[:, 2 * channel_count :] + biases[1])
        .astype(jnp.bfloat16)
        .reshape(rows, length, heads, HEAD_DIM)
    )
    scores = jnp.einsum("rqhd,rkhd->rhqk", query, key_low, preferred_element_type=jnp.float32)
    if mask is not None:
        scores = jnp.where(mask[:, None], scores, -1e30)
    probs = jax.nn.softmax(scores, axis=-1)
    probs_low = probs.astype(jnp.bfloat16)
    attended = jnp.einsum(
        "rhqk,rkhd->rqhd", probs_low, value_low, preferred_element_type=jnp.float32
    )
    attended = attended.astype(jnp.bfloat16).reshape(rows * length, channel_count)
    middle = flat + (jnp.dot(attended, out_w, preferred_element_type=jnp.float32) + biases[2])
    second, scaled_two, inverse_two = layer_norm(middle, gains[1], biases[5])
    second_low = second.astype(jnp.bfloat16)
    hidden = jnp.dot(second_low, up_w, preferred_element_type=jnp.float32) + up_b.astype(
        jnp.float32
    )
    active = gelu_exact(hidden).astype(jnp.bfloat16)
    output = middle + (jnp.dot(active, down_w, preferred_element_type=jnp.float32) + biases[3])
    saved = (
        scaled_one,
        inverse_one,
        first_low,
        query,
        key_low,
        value_low,
        probs,
        probs_low,
        attended,
        scaled_two,
        inverse_two,
        second_low,
        hidden,
        active,
    )
    return (output, saved)


def backward_block(grad_output, saved, weights, rows, length):
    qkv_w, out_w, up_w, down_w, gains_low, biases_low, up_b = weights
    gains = gains_low.astype(jnp.float32)
    (
        scaled_one,
        inverse_one,
        first_low,
        query,
        key_low,
        value_low,
        probs,
        probs_low,
        attended,
        scaled_two,
        inverse_two,
        second_low,
        hidden,
        active,
    ) = saved
    channel_count = grad_output.shape[-1]
    heads = channel_count // HEAD_DIM
    scale = 1.0 / math.sqrt(HEAD_DIM)
    count = rows * length
    down_grad = grad_output.astype(jnp.bfloat16)
    grad_down_bias = jnp.sum(down_grad, axis=0, dtype=jnp.float32)
    grad_down_w = jnp.einsum("nf,nd->fd", active, down_grad, preferred_element_type=jnp.float32)
    active_grad = jnp.einsum("nd,fd->nf", down_grad, down_w, preferred_element_type=jnp.float32)
    gelu_back = jax.vjp(gelu_exact, hidden)[1]
    hidden_grad = gelu_back(active_grad)[0].astype(jnp.bfloat16)
    grad_up_bias = jnp.sum(hidden_grad, axis=0, dtype=jnp.float32)
    grad_up_w = jnp.einsum("nd,nf->df", second_low, hidden_grad, preferred_element_type=jnp.float32)
    second_grad = jnp.einsum("nf,df->nd", hidden_grad, up_w, preferred_element_type=jnp.float32)
    grad_gain_two = jnp.sum(second_grad * scaled_two, axis=0)
    grad_shift_two = jnp.sum(second_grad, axis=0)
    middle_grad = grad_output + norm_back(second_grad * gains[1], scaled_two, inverse_two)
    branch_grad = middle_grad.astype(jnp.bfloat16)
    grad_out_bias = jnp.sum(branch_grad, axis=0, dtype=jnp.float32)
    grad_out_w = jnp.einsum("nd,ne->de", attended, branch_grad, preferred_element_type=jnp.float32)
    attended_grad = jnp.einsum("ne,de->nd", branch_grad, out_w, preferred_element_type=jnp.float32)
    attended_grad = attended_grad.astype(jnp.bfloat16).reshape(rows, length, heads, HEAD_DIM)
    probs_grad = jnp.einsum(
        "rqhd,rkhd->rhqk", attended_grad, value_low, preferred_element_type=jnp.float32
    )
    value_grad = jnp.einsum(
        "rhqk,rqhd->rkhd", probs_low, attended_grad, preferred_element_type=jnp.float32
    ).astype(jnp.bfloat16)
    score_grad = probs * (probs_grad - jnp.sum(probs * probs_grad, axis=-1, keepdims=True))
    score_grad = score_grad.astype(jnp.bfloat16)
    query_grad = jnp.einsum(
        "rhqk,rkhd->rqhd", score_grad, key_low, preferred_element_type=jnp.float32
    ).astype(jnp.bfloat16)
    key_grad = jnp.einsum(
        "rhqk,rqhd->rkhd", score_grad, query, preferred_element_type=jnp.float32
    ).astype(jnp.bfloat16)
    query_flat = query_grad.reshape(count, channel_count) * scale
    value_flat = value_grad.reshape(count, channel_count)
    mixed_grad = jnp.concatenate(
        [query_flat, key_grad.reshape(count, channel_count), value_flat], axis=1
    )
    grad_query_bias = jnp.sum(query_flat, axis=0, dtype=jnp.float32)
    grad_value_bias = jnp.sum(value_flat, axis=0, dtype=jnp.float32)
    grad_qkv_w = jnp.einsum("nd,ne->de", first_low, mixed_grad, preferred_element_type=jnp.float32)
    first_grad = jnp.einsum("ne,de->nd", mixed_grad, qkv_w, preferred_element_type=jnp.float32)
    grad_gain_one = jnp.sum(first_grad * scaled_one, axis=0)
    grad_shift_one = jnp.sum(first_grad, axis=0)
    input_grad = middle_grad + norm_back(first_grad * gains[0], scaled_one, inverse_one)
    grad_gains = jnp.stack([grad_gain_one, grad_gain_two])
    grad_biases = jnp.stack(
        [
            grad_query_bias,
            grad_value_bias,
            grad_out_bias,
            grad_down_bias,
            grad_shift_one,
            grad_shift_two,
        ]
    )
    return (
        input_grad,
        (grad_qkv_w, grad_out_w, grad_up_w, grad_down_w, grad_gains, grad_biases, grad_up_bias),
    )


def image_first_token(patches, qkv_w, out_w, up_w, down_w, gains_low, biases_low, up_b):
    rows, length, channel_count = patches.shape
    gains = gains_low.astype(jnp.float32)
    biases = biases_low.astype(jnp.float32)
    heads = channel_count // HEAD_DIM
    scale = 1.0 / math.sqrt(HEAD_DIM)
    first_low = layer_norm(patches.astype(jnp.float32), gains[0], biases[4])[0].astype(jnp.bfloat16)
    flat_low = first_low.reshape(rows * length, channel_count)
    query = (
        (jnp.dot(first_low[:, 0], qkv_w[:, :channel_count], preferred_element_type=jnp.float32) + biases[0])
        * scale
    ).astype(jnp.bfloat16).reshape(rows, heads, HEAD_DIM)
    mixed = jnp.dot(flat_low, qkv_w[:, channel_count:], preferred_element_type=jnp.float32)
    key_low = mixed[:, :channel_count].astype(jnp.bfloat16).reshape(rows, length, heads, HEAD_DIM)
    value_low = (
        (mixed[:, channel_count:] + biases[1]).astype(jnp.bfloat16).reshape(rows, length, heads, HEAD_DIM)
    )
    scores = jnp.einsum("rhd,rkhd->rhk", query, key_low, preferred_element_type=jnp.float32)
    probs_low = jax.nn.softmax(scores, axis=-1).astype(jnp.bfloat16)
    attended = jnp.einsum("rhk,rkhd->rhd", probs_low, value_low, preferred_element_type=jnp.float32)
    attended = attended.astype(jnp.bfloat16).reshape(rows, channel_count)
    middle = patches[:, 0].astype(jnp.float32) + (
        jnp.dot(attended, out_w, preferred_element_type=jnp.float32) + biases[2]
    )
    second_low = layer_norm(middle, gains[1], biases[5])[0].astype(jnp.bfloat16)
    hidden = jnp.dot(second_low, up_w, preferred_element_type=jnp.float32) + up_b.astype(jnp.float32)
    active = gelu_exact(hidden).astype(jnp.bfloat16)
    return middle + (jnp.dot(active, down_w, preferred_element_type=jnp.float32) + biases[3])


def per_device(
    incoming_word_states,
    sentence_number_per_word,
    described_picture,
    lookup_matrices,
    mixer_exit_matrix,
    widening_matrix,
    narrowing_matrix,
    normalizer_multipliers,
    word_offsets,
    widened_offset,
    picture_patches,
    picture_lookup_matrices,
    picture_mixer_exit_matrix,
    picture_widening_matrix,
    picture_narrowing_matrix,
    picture_normalizer_multipliers,
    picture_offsets,
    picture_widened_offset,
    sharpness_coefficient,
    objective_offset,
):
    rows, length, channel_count = incoming_word_states.shape
    whole = (
        lax.all_gather(lookup_matrices, "fsdp", axis=0, tiled=True),
        lax.all_gather(mixer_exit_matrix, "fsdp", axis=0, tiled=True),
        lax.all_gather(widening_matrix, "fsdp", axis=0, tiled=True),
        lax.all_gather(narrowing_matrix, "fsdp", axis=0, tiled=True),
        lax.all_gather(normalizer_multipliers, "fsdp", axis=1, tiled=True),
        lax.all_gather(word_offsets, "fsdp", axis=1, tiled=True),
        lax.all_gather(widened_offset, "fsdp", axis=0, tiled=True),
    )
    image_rows, image_length = (picture_patches.shape[0], picture_patches.shape[1])
    image_token = image_first_token(
        picture_patches,
        picture_lookup_matrices,
        picture_mixer_exit_matrix,
        picture_widening_matrix,
        picture_narrowing_matrix,
        picture_normalizer_multipliers,
        picture_offsets,
        picture_widened_offset,
    )
    image_embed = (
        image_token * lax.rsqrt(jnp.mean(image_token * image_token, axis=-1, keepdims=True) + 1e-06)
    ).astype(jnp.bfloat16)
    mask = sentence_number_per_word[:, :, None] == sentence_number_per_word[:, None, :]
    flat = incoming_word_states.astype(jnp.float32).reshape(rows * length, channel_count)
    text_result, saved = forward_block(flat, rows, length, mask, whole)
    member = (sentence_number_per_word[:, :, None] == jnp.arange(CAPS, dtype=jnp.int32)).astype(
        jnp.float32
    )
    counts = jnp.sum(member, axis=1)[:, :, None]
    pooled = (
        jnp.einsum(
            "rsc,rsd->rcd",
            member,
            text_result.reshape(rows, length, channel_count),
            precision=lax.Precision.HIGHEST,
        )
        / counts
    )
    pooled = pooled.reshape(rows * CAPS, channel_count)
    inverse = lax.rsqrt(jnp.mean(pooled * pooled, axis=-1, keepdims=True) + 1e-06)
    embed = pooled * inverse
    embed_low = embed.astype(jnp.bfloat16)
    multiplier_amount = sharpness_coefficient[0] / math.sqrt(channel_count)
    piece = lax.all_gather(image_embed, ("fsdp", "dp"), axis=0, tiled=True)
    unscaled_similarity = jnp.einsum(
        "cd,nd->cn", embed_low, piece, preferred_element_type=jnp.float32
    )
    match_similarity = multiplier_amount * unscaled_similarity + objective_offset[0]
    positive = described_picture[:, None] == jnp.arange(piece.shape[0], dtype=jnp.int32)[None, :]
    labels = jnp.where(positive, 1.0, -1.0)
    total = jnp.sum(jax.nn.softplus(-labels * match_similarity), axis=1)
    slope = (
        (jax.nn.sigmoid(match_similarity) - positive.astype(jnp.float32)) * multiplier_amount
    ).astype(jnp.bfloat16)
    grad_embed = jnp.einsum("cn,nd->cd", slope, piece, preferred_element_type=jnp.float32)
    images_all = image_rows * lax.axis_size("fsdp") * lax.axis_size("dp")
    loss = total / images_all
    pooled_grad = inverse * (
        grad_embed - embed * jnp.mean(grad_embed * embed, axis=-1, keepdims=True)
    )
    per_caption = pooled_grad.reshape(rows, CAPS, channel_count) / counts
    token_grad = jnp.einsum(
        "rsc,rcd->rsd", member, per_caption, precision=lax.Precision.HIGHEST
    ).reshape(rows * length, channel_count)
    input_grad, grads = backward_block(token_grad, saved, whole, rows, length)
    owned = [
        lax.psum(
            lax.psum_scatter(piece_grad.astype(jnp.bfloat16), "fsdp", scatter_dimension=0, tiled=True), "dp"
        ).astype(jnp.float32)
        for piece_grad in grads[:4]
    ]
    small = jnp.concatenate([grads[4], grads[5], grads[6].reshape(-1, channel_count)], axis=0)
    small = lax.psum(small, ("fsdp", "dp"))
    place = lax.axis_index("fsdp")
    width = normalizer_multipliers.shape[1]
    columns = lax.dynamic_slice_in_dim(small[:8], place * width, width, axis=1)
    hidden_width = widened_offset.shape[0]
    hidden_part = lax.dynamic_slice_in_dim(small[8:].reshape(-1), place * hidden_width, hidden_width)
    summed = (*owned, columns[:2], columns[2:8], hidden_part)
    grad_input = input_grad.astype(jnp.bfloat16).reshape(rows, length, channel_count)
    return (
        summed[0],
        summed[1],
        summed[2],
        summed[3],
        summed[4],
        summed[5],
        summed[6],
        grad_input,
        loss,
    )


BF = jnp.bfloat16
F32 = jnp.float32
MESH_ID = pl.DeviceIdType.MESH
TILE = 256
ROWS = 128
GROUPS = 2
N_AG = 11
Z_PAIRS = ((0, 1), (3, 4), (6, 7), (9, 10))
GATHER = {
    "start": ("o0", "o1", "o7", "o3",),
    "keys": ("r0", "r1", "o2",),
    "mixed": ("l0", "r3", "o4",),
    "image": ("l1", "o6", "r7", "z0", "r2", "l3", "o5",),
    "norm": ("y0", "r4", "l2",),
    "project1": ("o10", "r5", "r6",),
    "project2": ("o9", "l4",),
    "attend2": ("o8",),
    "attend4": ("l6", "l7", "z1",),
    "attend6": ("y1",),
    "attend7": ("l5",),
    "out": ("r9", "r10", "z2",),
    "norm2": ("r8", "y2",),
    "widen1": ("l8", "l10", "l9",),
    "widen2": ("z3",),
    "widen3": ("y3",),
}
D_UNIT = 8


def nn(a, b):
    return jnp.dot(a, b, preferred_element_type=F32)


def nt(a, b):
    return lax.dot_general(a, b, (((1,), (1,)), ((), ())), preferred_element_type=F32)


def tn(a, b):
    return lax.dot_general(a, b, (((0,), (0,)), ((), ())), preferred_element_type=F32)


def span(start, size, unit=16):
    if isinstance(start, int):
        return pl.ds(start, size)
    return pl.ds(pl.multiple_of(start, unit), size)


def norm_rows(values):
    centred = values - jnp.mean(values, axis=-1, keepdims=True)
    inverse = lax.rsqrt(jnp.mean(centred * centred, axis=-1, keepdims=True) + 1e-06)
    return centred * inverse, inverse


def normal_cdf(values):
    return 0.5 * (1.0 + lax.erf(values * math.sqrt(0.5)))


def loop(count, body, events=None):
    def step(i, carry):
        body(i)
        for at, calls in (events or {}).items():

            @pl.when(i == at)
            def _(calls=calls):
                for call in calls:
                    call()

        return carry

    lax.fori_loop(0, count, step, 0)


def fused_kernel(
    sharp_ref,
    offset_ref,
    x_hbm,
    segment_ref,
    described_ref,
    qkv_hbm,
    out_hbm,
    up_hbm,
    down_hbm,
    gain_ref,
    shift_ref,
    hidden_ref,
    patches_hbm,
    pqkv_hbm,
    pout_hbm,
    pup_hbm,
    pdown_hbm,
    pgain_ref,
    pshift_ref,
    phidden_ref,
    units_out,
    down_out,
    input_out,
    small_out,
    loss_out,
    wts,
    wdn,
    h1,
    qkv,
    att,
    x1,
    h2,
    act,
    dg,
    gm,
    sdn,
    lc,
    lcd,
    lx,
    lxd,
    ly,
    lyd,
    lz,
    lzd,
    work,
    low,
    faces,
    small_in,
    params,
    img_gain,
    member,
    pooled,
    caption_hi,
    caption_lo,
    partial,
    small_sum,
    small_land,
    face_rows,
    ag_send,
    ag_recv,
    core_send,
    core_recv,
    xy_send,
    xy_recv,
    z_send,
    z_recv,
    side_send,
    side_recv,
    local_sem,
):
    fs = lax.axis_index("fsdp")
    dp = lax.axis_index("dp")
    core = fs % 2
    xb = (fs // 2) % 2
    yb = fs // 4
    fs_core = fs + 1 - 2 * core
    fs_x = fs + 2 - 4 * xb
    fs_y = fs + 4 - 8 * yb
    fs_diag = fs_x + 4 - 8 * yb
    flip = 1 - 2 * core
    peer_core = (fs_core, dp)
    peer_x = (fs_x, dp)
    peer_y = (fs_y, dp)
    half_z = dp // 2
    is_end = (dp == 0) | (dp == 3)
    is_mid = (dp == 1) | (dp == 2)
    near = half_z
    far = 1 - half_z
    dp_inner = 1 + half_z
    dp_end = 3 * half_z
    dp_mid = 2 - half_z
    dp_pair = dp + 1 - 2 * (dp % 2)
    dp_far = dp + 2 - 4 * half_z

    barrier = pltpu.get_barrier_semaphore()
    others = (fs_core, fs_x, fs_y, fs_diag, fs_x + flip, fs_y + flip, fs_diag + flip)
    greet = [(other, dp) for other in others] + [(fs, dp_pair), (fs, dp_far)]
    for peer in greet:
        pl.semaphore_signal(barrier, inc=1, device_id=peer, device_id_type=MESH_ID)

    local = []

    def fetch(src, dst):
        copy = pltpu.make_async_copy(src, dst, local_sem.at[len(local)])
        copy.start()
        local.append(copy)
        return copy

    own_rows = span(96 * fs, 96)
    own_copies = [fetch(qkv_hbm.at[:, pl.ds(768 * j, 768)], wts.at[j, own_rows, :]) for j in range(3)]
    own_copies.append(fetch(out_hbm, wts.at[3, own_rows, :]))
    own_copies += [fetch(up_hbm.at[:, pl.ds(768 * j, 768)], wts.at[4 + j, own_rows, :]) for j in range(4)]
    own_copies.append(fetch(down_hbm, wdn.at[span(384 * fs, 384), :]))
    patches_copy = fetch(patches_hbm, gm.at[pl.ds(512, 400), :])
    pqkv_copy = fetch(pqkv_hbm, act.at[pl.ds(0, 768), pl.ds(0, 2304)])
    x_copy = fetch(x_hbm, h2)
    pout_copy = fetch(pout_hbm, act.at[pl.ds(0, 768), pl.ds(2304, 768)])
    pup_copy = fetch(pup_hbm, dg.at[pl.ds(0, 768), :])
    pdown_copy = fetch(pdown_hbm, sdn)

    small_in[fs] = jnp.zeros((16, 128), F32)
    small_in[fs, 0:2, 0:96] = gain_ref[...].astype(F32)
    small_in[fs, 2:8, 0:96] = shift_ref[...].astype(F32)
    small_in[fs, 8:11, :] = hidden_ref[...].astype(F32)
    pl.semaphore_wait(barrier, len(greet))

    def weight(unit, shard, part=None):
        if unit < 8:
            rows = span(96 * shard, 96) if part is None else span(96 * shard + 48 * part, 48)
            return wts.at[unit, rows, :]
        rows = span(384 * shard, 384) if part is None else span(384 * shard + 192 * part, 192)
        return wdn.at[rows, pl.ds(256 * (unit - 8), 256)]

    def own_weight(unit):
        if unit < 3:
            return qkv_hbm.at[:, pl.ds(768 * unit, 768)]
        if unit == 3:
            return out_hbm
        if unit < 8:
            return up_hbm.at[:, pl.ds(768 * (unit - 4), 768)]
        return down_hbm.at[:, pl.ds(256 * (unit - 8), 256)]

    def ag(unit, kind, ref, peer, source=None):
        return pltpu.make_async_remote_copy(
            src_ref=ref if source is None else source,
            dst_ref=ref,
            send_sem=ag_send.at[unit, kind],
            recv_sem=ag_recv.at[unit, kind],
            device_id=peer,
            device_id_type=MESH_ID,
        )

    def ag_out(unit, kind):
        shard, part, peer = (
            (fs, None, peer_core),
            (fs, None, peer_x),
            (fs, None, peer_y),
            (fs_x, 0, peer_y),
            (fs_y, 1, peer_x),
            (fs_x, None, peer_core),
            (fs_y, None, peer_core),
            (fs_diag, 0, peer_core),
            (fs_diag, 1, peer_core),
            (fs_x, None, (fs, dp_pair)),
            (fs_y, None, (fs, dp_pair)),
            (fs_diag, 0, (fs, dp_pair)),
            (fs_diag, 1, (fs, dp_pair)),
        )[kind]
        return ag(unit, kind, weight(unit, shard, part), peer, own_weight(unit) if kind < 3 else None)

    def ag_in(unit, kind):
        shard, part = (
            (fs_core, None),
            (fs_x, None),
            (fs_y, None),
            (fs_diag, 0),
            (fs_diag, 1),
            (fs_x + flip, None),
            (fs_y + flip, None),
            (fs_diag + flip, 0),
            (fs_diag + flip, 1),
            (fs_x, None),
            (fs_y, None),
            (fs_diag, 0),
            (fs_diag, 1),
        )[kind]
        return ag(unit, kind, weight(unit, shard, part), peer_core)

    def fetching(unit, body):
        for pair in Z_PAIRS:
            if unit in pair:
                pl.when(dp % 2 == pair.index(unit))(body)
                return
        body()

    def ag_own(*units):
        for unit in units:

            def body(unit=unit):
                for kind in (1, 2):
                    ag_out(unit, kind).start()

            fetching(unit, body)
            ag_out(unit, 0).start()

    def handed(unit):
        return any(unit in pair for pair in Z_PAIRS)

    def ag_relay(*units):
        for unit in units:

            def body(unit=unit):
                for arrived, onward, inner, across in ((1, 3, 5, 9), (2, 4, 6, 10)):
                    ag_in(unit, arrived).wait_recv()
                    ag_out(unit, onward).start()
                    ag_out(unit, inner).start()
                    if handed(unit):
                        ag_out(unit, across).start()

            fetching(unit, body)

    def ag_last(*units):
        for unit in units:

            def body(unit=unit):
                for arrived, inner, across in ((3, 7, 11), (4, 8, 12)):
                    ag_in(unit, arrived).wait_recv()
                    ag_out(unit, inner).start()
                    if handed(unit):
                        ag_out(unit, across).start()

            fetching(unit, body)

    def ag_across(pair, kinds):
        for index in range(2):

            @pl.when(dp % 2 != index)
            def _(unit=pair[index]):
                for arrived, inner in kinds:
                    ag_in(unit, arrived).wait_recv()
                    ag_out(unit, inner).start()

    def z_relay(pair):
        ag_across(pair, ((9, 5), (10, 6)))

    def z_last(pair):
        ag_across(pair, ((11, 7), (12, 8)))

    def ag_drain():
        for unit in range(N_AG):

            def body(unit=unit):
                for kind in (1, 2, 3, 4) + ((9, 10, 11, 12) if handed(unit) else ()):
                    ag_out(unit, kind).wait_send()

            fetching(unit, body)
            for kind in (0, 5, 6, 7, 8):
                ag_out(unit, kind).wait_send()

    def hook(point):
        for step in GATHER.get(point, ()):
            number = int(step[1:])
            if step[0] == "o":
                ag_own(number)
            elif step[0] == "r":
                ag_relay(number)
            elif step[0] == "l":
                ag_last(number)
            elif step[0] == "z":
                z_relay(Z_PAIRS[number])
            else:
                z_last(Z_PAIRS[number])

    def ready(unit):
        for kind in (0, 5, 6, 7, 8):
            ag_in(unit, kind).wait_recv()

    def side(index, src, dst, peer):
        return pltpu.make_async_remote_copy(
            src_ref=src,
            dst_ref=dst,
            send_sem=side_send.at[index],
            recv_sem=side_recv.at[index],
            device_id=peer,
            device_id_type=MESH_ID,
        )

    chip_slot = fs - core
    row_slot = 4 * yb

    def param_copy(index, slot):
        ref = small_in.at[slot]
        return side(index, ref, ref, (others[index], dp))

    far_plane = 2 - 2 * half_z
    face_steps = (
        (dp, 1, fs, 1, peer_core, dp, fs_core),
        (dp, 1, chip_slot, 2, peer_x, dp, chip_slot + 2 - 4 * xb),
        (dp, 1, row_slot, 4, peer_y, dp, 4 - row_slot),
        (dp, 1, 4 * core, 4, (fs, dp_pair), dp_pair, 4 * core),
        (2 * half_z, 2, 4 * core, 4, (fs, dp_far), far_plane, 4 * core),
        (dp_pair, 1, 4 * core, 4, peer_core, dp_pair, 4 - 4 * core),
        (far_plane, 2, 4 * core, 4, peer_core, far_plane, 4 - 4 * core),
    )

    def face_copy(step, landing):
        d0, dn, f0, fn, peer, ld, lf = face_steps[step]
        if landing:
            d0, f0 = ld, lf
        ref = faces.at[pl.ds(d0, dn), pl.ds(f0, fn)]
        return side(7 + step, ref, ref, peer)

    def face_start(step):
        face_copy(step, False).start()

    def face_wait(step):
        face_copy(step, True).wait_recv()

    sum_peers = (peer_core, peer_x, peer_y, (fs, dp_pair), (fs, dp_far))

    def sum_copy(step):
        return side(14 + step, small_sum.at[step], small_land.at[step], sum_peers[step])

    def sum_start(step):
        sum_copy(step).start()

    def sum_wait(step):
        sum_copy(step).wait_recv()
        small_sum[step + 1] = small_sum[step] + small_land[step]

    def grad(unit, rows):
        if unit == D_UNIT:
            return sdn.at[rows, :]
        if unit >= 4:
            return act.at[rows, pl.ds(768 * (unit - 4), 768)]
        return wts.at[4 + unit, rows, :]

    def shape_of(unit):
        return 384 if unit == D_UNIT else 96

    def piece_shard(delta, which):
        chip_x = (xb + delta % 2) - 2 * xb * (delta % 2)
        chip_y = (yb + delta // 2) - 2 * yb * (delta // 2)
        return (chip_y * 2 + chip_x) * 2 + which

    def piece(unit, delta, which, part=None):
        size = shape_of(unit)
        shard = piece_shard(delta, which)
        if part is None:
            return grad(unit, span(size * shard, size))
        return grad(unit, span(size * shard + (size // 2) * part, size // 2))

    def lands(pair, unit, slot):
        wide, down_only = pair
        return down_only.at[slot] if unit == D_UNIT else wide.at[unit, slot]

    def accumulate(dst, *sources):
        rows = dst.shape[0]

        def body(i, carry):
            r = span(i * 48, 48)
            value = dst[r, :].astype(F32)
            for source in sources:
                value = value + source[r, :].astype(F32)
            dst[r, :] = value.astype(BF)
            return carry

        lax.fori_loop(0, rows // 48, body, 0)

    def core_copy(unit, delta):
        return pltpu.make_async_remote_copy(
            src_ref=piece(unit, delta, 1 - core),
            dst_ref=lands((lc, lcd), unit, delta),
            send_sem=core_send.at[unit, delta],
            recv_sem=core_recv.at[unit, delta],
            device_id=peer_core,
            device_id_type=MESH_ID,
        )

    def rs_core(unit):
        for delta in (3, 2, 1, 0):
            core_copy(unit, delta).start()

    xy_kinds = (
        (3, 0, (lx, lxd), 0, peer_x),
        (3, 1, (ly, lyd), 0, peer_y),
        (1, 0, (lx, lxd), 1, peer_x),
        (2, 1, (ly, lyd), 1, peer_y),
        (2, 0, (ly, lyd), 2, peer_y),
        (1, 1, (lx, lxd), 2, peer_x),
    )

    def xy_copy(unit, kind):
        delta, part, pair, slot, peer = xy_kinds[kind]
        return pltpu.make_async_remote_copy(
            src_ref=piece(unit, delta, core, part),
            dst_ref=lands(pair, unit, slot),
            send_sem=xy_send.at[unit, kind],
            recv_sem=xy_recv.at[unit, kind],
            device_id=peer,
            device_id_type=MESH_ID,
        )

    def rs_first_piece(unit, delta):
        core_copy(unit, delta).wait_recv()
        accumulate(piece(unit, delta, core), lands((lc, lcd), unit, delta))
        for kind in {3: (0, 1), 1: (2,), 2: (3,), 0: ()}[delta]:
            xy_copy(unit, kind).start()

    def rs_first(unit):
        for delta in (3, 2, 1, 0):
            rs_first_piece(unit, delta)

    def rs_second(unit):
        xy_copy(unit, 0).wait_recv()
        accumulate(piece(unit, 2, core, 0), lands((lx, lxd), unit, 0))
        xy_copy(unit, 4).start()
        xy_copy(unit, 1).wait_recv()
        accumulate(piece(unit, 1, core, 1), lands((ly, lyd), unit, 0))
        xy_copy(unit, 5).start()

    def z_copy(unit, index, src, slot, target):
        return pltpu.make_async_remote_copy(
            src_ref=src,
            dst_ref=lands((lz, lzd), unit, slot),
            send_sem=z_send.at[unit, index],
            recv_sem=z_recv.at[unit, slot],
            device_id=(fs, target),
            device_id_type=MESH_ID,
        )

    def z_land(unit, slot):
        return lands((lz, lzd), unit, slot)

    def z_wait(unit, slot):
        z_copy(unit, 0, z_land(unit, slot), slot, dp_pair).wait_recv()

    def z_out(unit, index):
        own_far = piece(unit, 0, core, far)
        own_near = piece(unit, 0, core, near)
        end = {
            0: (own_far, 1, dp_inner),
            1: (own_near, 0, dp_inner),
        }
        mid = {
            0: (own_far, 2, dp_mid),
            1: (z_land(unit, 2), 2, dp_end),
            2: (z_land(unit, 2), 3, dp_mid),
            3: (z_land(unit, 3), 3, dp_end),
        }
        return end.get(index), mid[index]

    def z_end(unit, index):
        return z_copy(unit, index, *z_out(unit, index)[0])

    def z_mid(unit, index):
        return z_copy(unit, index, *z_out(unit, index)[1])

    def rs_own(unit):
        for kind in (2, 3, 4, 5):
            xy_copy(unit, kind).wait_recv()
        accumulate(piece(unit, 0, core, 0), lands((lx, lxd), unit, 1), lands((ly, lyd), unit, 2))
        accumulate(piece(unit, 0, core, 1), lands((ly, lyd), unit, 1), lands((lx, lxd), unit, 2))

        @pl.when(is_end)
        def _():
            z_end(unit, 0).start()
            z_end(unit, 1).start()

    def rs_z2(unit):
        @pl.when(is_mid)
        def _():
            z_wait(unit, 1)
            accumulate(piece(unit, 0, core, far), z_land(unit, 1))
            z_mid(unit, 0).start()

    def rs_z3(unit):
        @pl.when(is_mid)
        def _():
            z_wait(unit, 0)
            z_wait(unit, 2)
            accumulate(z_land(unit, 2), z_land(unit, 0), piece(unit, 0, core, near))
            z_mid(unit, 1).start()
            z_mid(unit, 2).start()

    def rs_z4(unit):
        @pl.when(is_mid)
        def _():
            z_wait(unit, 3)
            z_mid(unit, 3).start()

    def result_copy(unit, slot):
        size = shape_of(unit) // 2
        rows = span(size * (near if slot == 2 else far), size)
        target = down_out.at[rows, :] if unit == D_UNIT else units_out.at[unit, rows, :]
        return pltpu.make_async_copy(z_land(unit, slot), target, local_sem.at[16 + 2 * unit + slot - 2])

    def rs_done(unit):
        @pl.when(is_end)
        def _():
            z_wait(unit, 2)
            z_wait(unit, 3)

        for slot in (2, 3):
            result_copy(unit, slot).start()

    for index in range(7):
        param_copy(index, fs).start()
    hook("start")

    img_h = gm
    img_k = att
    img_v = h1
    img_gain[0:2, :] = pgain_ref[...].astype(F32)
    img_gain[2:8, :] = pshift_ref[...].astype(F32)
    phidden = phidden_ref[...].astype(F32)
    for q in range(24):
        img_gain[8 + q // 6 : 9 + q // 6, 128 * (q % 6) : 128 * (q % 6) + 128] = phidden[q : q + 1, :]
    img_h[pl.ds(400, 112), :] = jnp.zeros((112, 768), BF)
    patches_copy.wait()

    def image_normed(values):
        return norm_rows(values)[0] * img_gain[0:1, :] + img_gain[6:7, :]

    first_rows = img_h[pl.ds(512, 16), :].astype(F32)[0:8, :]
    face_rows[0] = first_rows
    face_rows[1] = image_normed(first_rows)

    def image_norm(i):
        img_h[span(80 * i, 80), :] = image_normed(img_h[span(512 + 80 * i, 80), :].astype(F32)).astype(BF)

    loop(5, image_norm)
    pqkv_copy.wait()

    def image_kv(i):
        r = span(i * TILE, TILE)
        img_k[r, :] = nn(img_h[r, :], act[pl.ds(0, 768), pl.ds(768, 768)]).astype(BF)
        img_v[r, :] = (nn(img_h[r, :], act[pl.ds(0, 768), pl.ds(1536, 768)]) + img_gain[3:4, :]).astype(BF)

    loop(2, image_kv)
    hook("keys")

    lane_head = lax.broadcasted_iota(jnp.int32, (8, 768), 1) // 64
    img_q = (nn(face_rows[1].astype(BF), act[pl.ds(0, 768), pl.ds(0, 768)]) + img_gain[2:3, :]) * 0.125
    img_q = img_q.astype(BF).astype(F32)
    stacked = jnp.concatenate([jnp.where(lane_head == h, img_q, 0.0) for h in range(12)], axis=0).astype(BF)
    scores = nt(stacked, img_k[pl.ds(0, 512), :])
    token = lax.broadcasted_iota(jnp.int32, (96, 512), 1)
    image_of = lax.broadcasted_iota(jnp.int32, (96, 512), 0) % 8
    scores = jnp.where((token % 8 == image_of) & (token < 400), scores, -1e30)
    expd = jnp.exp(scores - jnp.max(scores, axis=-1, keepdims=True))
    probs = (expd / jnp.sum(expd, axis=-1, keepdims=True)).astype(BF)
    mixed = nn(probs, img_v[pl.ds(0, 512), :])
    joined = jnp.zeros((8, 768), F32)
    for h in range(12):
        joined = joined + jnp.where(lane_head == h, mixed[8 * h : 8 * h + 8, :], 0.0)
    hook("mixed")
    pout_copy.wait()
    middle = face_rows[0] + (nn(joined.astype(BF), act[pl.ds(0, 768), pl.ds(2304, 768)]) + img_gain[4:5, :])
    scaled, _ = norm_rows(middle)
    normed = (scaled * img_gain[1:2, :] + img_gain[7:8, :]).astype(BF)
    face_rows[0] = middle
    pup_copy.wait()
    for j in range(4):
        hidden = nn(normed, dg[pl.ds(0, 768), pl.ds(768 * j, 768)]) + img_gain[8 + j : 9 + j, :]
        face_rows[2 + j] = hidden * normal_cdf(hidden)
    hook("image")
    pdown_copy.wait()
    total = face_rows[0] + img_gain[5:6, :]
    for j in range(4):
        total = total + nn(face_rows[2 + j].astype(BF), sdn[pl.ds(768 * j, 768), :])
    unit_norm = total * lax.rsqrt(jnp.mean(total * total, axis=-1, keepdims=True) + 1e-06)
    faces[dp, fs] = unit_norm.astype(BF)
    face_start(0)
    for index in range(7):
        param_copy(index, others[index]).wait_recv()

    flat_small = small_in[...].reshape(128, 128).astype(BF)
    for r in range(4):
        lane = lax.broadcasted_iota(jnp.int32, (128, 384), 0)
        column = lax.broadcasted_iota(jnp.int32, (128, 384), 1)
        pick = jnp.where((column == lane + 96 * r) & (lane < 96), 1.0, 0.0).astype(BF)
        spread = nn(flat_small, pick)
        for block in range(2):
            shard = 4 * block + r
            value = spread[16 * shard : 16 * shard + 8, :]
            cols = slice(384 * block, 384 * block + 384)
            if r == 0:
                params[0:8, cols] = value
            else:
                params[0:8, cols] = params[0:8, cols] + value
    for shard in range(8):
        for q in range(3):
            at = 384 * (shard % 2) + 128 * q
            params[8 + shard // 2 : 9 + shard // 2, at : at + 128] = small_in[shard, 8 + q : 9 + q, :]

    x_copy.wait()
    for copy in own_copies:
        copy.wait()

    def first_norm(i):
        r = span(32 * i, 32)
        scaled, _ = norm_rows(h2[r, :].astype(F32))
        h1[r, :] = (scaled * params[0:1, :] + params[6:7, :]).astype(BF)

    loop(32, first_norm)
    for group in range(8):
        rows = [segment_ref[2 * group + k : 2 * group + k + 1, :] + CAPS * (2 * group + k) for k in range(2)]
        same = lax.broadcasted_iota(jnp.int32, (64, 128), 0) == jnp.concatenate(rows, axis=1)
        member[:, 128 * group : 128 * group + 128] = jnp.where(same, 1.0, 0.0).astype(BF)
    face_wait(0)
    face_start(1)
    hook("norm")

    def project(j):
        def body(i):
            r = span(TILE * i, TILE)
            value = nn(h1[r, :], wts[j])
            if j == 0:
                value = (value + params[2:3, :]) * 0.125
            if j == 2:
                value = value + params[3:4, :]
            qkv[r, pl.ds(768 * j, 768)] = value.astype(BF)

        loop(4, body)

    ready(0)
    project(0)
    hook("project0")
    ready(1)
    project(1)
    hook("project1")
    ready(2)
    project(2)
    face_wait(1)
    face_start(2)

    low_lane = lax.broadcasted_iota(jnp.int32, (128, 128), 1) < 64
    zero_block = jnp.zeros((128, 128), BF)

    def split_heads(block):
        return jnp.concatenate(
            [jnp.where(low_lane, block, zero_block), jnp.where(low_lane, zero_block, block)], axis=0
        )

    def join_heads(value):
        return jnp.where(low_lane, value[0:128, :], value[128:256, :])

    def same_caption(group):
        part = member[:, span(128 * group, 128, 128)]
        same = tn(part, part)
        return jnp.concatenate([same, same], axis=0) > 0.5

    def attention_probs(same, queries, keys):
        value = jnp.where(same, nt(queries, keys), -1e30)
        expd = jnp.exp(value - jnp.max(value, axis=-1, keepdims=True))
        return expd * (1.0 / jnp.sum(expd, axis=-1, keepdims=True))

    def attend(group):
        r = span(128 * group, 128)
        same = same_caption(group)
        for hp in range(6):
            queries = split_heads(qkv[r, pl.ds(128 * hp, 128)])
            probs = attention_probs(same, queries, qkv[r, pl.ds(768 + 128 * hp, 128)])
            mixed = nn(probs.astype(BF), qkv[r, pl.ds(1536 + 128 * hp, 128)])
            att[r, pl.ds(128 * hp, 128)] = join_heads(mixed).astype(BF)

    hook("project2")
    loop(8, attend, {i: [lambda i=i: hook(f"attend{i}")] for i in range(8)})
    face_wait(2)
    face_start(3)
    ready(3)

    def out_project(i):
        r = span(TILE * i, TILE)
        x1[r, :] = h2[r, :].astype(F32) + (nn(att[r, :], wts[3]) + params[4:5, :])

    loop(4, out_project)
    hook("out")

    def second_norm(i):
        r = span(32 * i, 32)
        scaled, _ = norm_rows(x1[r, :])
        h2[r, :] = (scaled * params[1:2, :] + params[7:8, :]).astype(BF)

    loop(32, second_norm)
    hook("norm2")
    face_wait(3)
    face_start(4)
    face_start(5)

    def widen(j):
        def body(i):
            r = span(TILE * i, TILE)
            work[...] = nn(h2[r, :], wts[4 + j]) + params[8 + j : 9 + j, :]

            def gelu(k):
                inner = span(16 * k, 16)
                hidden = work[inner, :]
                cdf = normal_cdf(hidden)
                outer = span(TILE * i + 16 * k, 16)
                act[outer, pl.ds(768 * j, 768)] = (hidden * cdf).astype(BF)
                slope = cdf + hidden * (jnp.exp(-0.5 * hidden * hidden) * (1.0 / math.sqrt(2.0 * math.pi)))
                dg[outer, pl.ds(768 * j, 768)] = slope.astype(BF)

            loop(16, gelu)

        loop(4, body)

    for j in range(4):
        ready(4 + j)
        widen(j)
        hook(f"widen{j}")
    face_wait(4)
    face_start(6)

    for jd in range(3):
        ready(8 + jd)
        cols = pl.ds(256 * jd, 256)

        def narrow(i, cols=cols, jd=jd):
            r = span(TILE * i, TILE)
            value = nn(act[r, :], wdn[:, cols]) + params[5:6, 256 * jd : 256 * jd + 256]
            value = x1[r, cols] + value
            top = value.astype(BF)
            rest = (value - top.astype(F32)).astype(BF)
            lanes = span(TILE * i, TILE, 128)
            piece_sum = nn(member[:, lanes], top) + nn(member[:, lanes], rest)

            @pl.when(i == 0)
            def _():
                pooled[:, cols] = piece_sum

            @pl.when(i > 0)
            def _():
                pooled[:, cols] = pooled[:, cols] + piece_sum

        loop(4, narrow)

    face_wait(5)
    face_wait(6)

    count = jnp.sum(member[...].astype(F32), axis=-1, keepdims=True)
    mean_rows = pooled[...] / count
    inverse = lax.rsqrt(jnp.mean(mean_rows * mean_rows, axis=-1, keepdims=True) + 1e-06)
    embed = mean_rows * inverse
    face_all = faces[...].astype(F32).reshape(256, 768).astype(BF)
    amount = sharp_ref[0] * (1.0 / math.sqrt(768.0))
    match = amount * nt(embed.astype(BF), face_all) + offset_ref[0]
    slot = lax.broadcasted_iota(jnp.int32, (64, 256), 1)
    image_id = ((slot // 8) % 8) * 32 + (slot // 64) * 8 + slot % 8
    diagonal = lax.broadcasted_iota(jnp.int32, (64, 64), 0) == lax.broadcasted_iota(jnp.int32, (64, 64), 1)
    described = jnp.where(diagonal, described_ref[...].astype(F32), 0.0)
    positive = jnp.sum(described, axis=-1, keepdims=True) == image_id.astype(F32)
    signed = jnp.where(positive, -match, match)
    terms = jnp.maximum(signed, 0.0) + jnp.log1p(jnp.exp(-jnp.abs(signed)))
    row_loss = jnp.sum(terms, axis=-1, keepdims=True) * (1.0 / 256.0)
    loss_out[...] = jnp.sum(jnp.where(diagonal, row_loss, 0.0), axis=0, keepdims=True)
    slope = ((jax.nn.sigmoid(match) - jnp.where(positive, 1.0, 0.0)) * amount).astype(BF)
    grad_embed = nn(slope, face_all)
    grad_pooled = inverse * (grad_embed - embed * jnp.mean(grad_embed * embed, axis=-1, keepdims=True))
    per_caption = grad_pooled / count
    caption_hi[...] = per_caption.astype(BF)
    caption_lo[...] = (per_caption - caption_hi[...].astype(F32)).astype(BF)

    def spread_down(i):
        gm[span(TILE * i, TILE), :] = tn(member[:, span(TILE * i, TILE, 128)], caption_hi[...]).astype(BF)

    loop(4, spread_down)

    ag_drain()
    for index in range(7):
        param_copy(index, fs).wait_send()
    for step in range(7):
        face_copy(step, False).wait_send()

    ones = jnp.ones((16, 1024), BF)

    def column_sum(value):
        return nn(ones, value)[0:1, :]

    def down_piece(delta):
        def body(i):
            which = (1 - core) + i * (2 * core - 1)
            shard = piece_shard(delta, which)
            sdn[span(384 * shard, 384), :] = tn(act[:, span(384 * shard, 384, 128)], gm[...]).astype(BF)

            @pl.when(i == 0)
            def _():
                core_copy(D_UNIT, delta).start()

        loop(2, body)

    down_piece(3)
    down_piece(2)
    rs_first_piece(D_UNIT, 3)
    down_piece(1)
    rs_first_piece(D_UNIT, 2)
    down_piece(0)
    rs_first_piece(D_UNIT, 1)
    rs_first_piece(D_UNIT, 0)

    def hidden_back(i):
        r = span(TILE * i, TILE)
        for jj in range(3):
            cols = pl.ds(1024 * jj, 1024)
            value = nt(gm[r, :], wdn[pl.ds(1024 * jj, 1024), :])
            dg[r, cols] = (dg[r, cols].astype(F32) * value).astype(BF)

    loop(4, hidden_back, {1: [lambda: rs_second(D_UNIT)]})
    partial_rows = {}

    def up_unit(j):
        def body(i):
            act[span(TILE * i, TILE), pl.ds(768 * j, 768)] = tn(
                h2[:, span(TILE * i, TILE, 128)], dg[:, pl.ds(768 * j, 768)]
            ).astype(BF)

        loop(3, body)
        rs_core(4 + j)
        small_sum[0, 8 + j : 9 + j, :] = column_sum(dg[:, pl.ds(768 * j, 768)])

    up_unit(0)
    up_unit(1)
    rs_first(4)
    up_unit(2)
    rs_first(5)
    up_unit(3)
    rs_first(6)
    rs_own(D_UNIT)
    small_sum[0, 5:6, :] = column_sum(gm[...])
    partial[...] = jnp.zeros((4, 8, 768), F32)

    def fold(value):
        return value.reshape(value.shape[0] // 8, 8, 768).sum(axis=0)

    def middle_back(i):
        r = span(TILE * i, TILE)
        total = nt(dg[r, pl.ds(0, 768)], wts[4])
        for j in range(1, 4):
            total = total + nt(dg[r, pl.ds(768 * j, 768)], wts[4 + j])
        work[...] = total
        low[...] = tn(member[:, span(TILE * i, TILE, 128)], caption_lo[...]).astype(BF)

        def rows_back(k):
            inner = span(ROWS * k, ROWS)
            outer = span(TILE * i + ROWS * k, ROWS)
            upstream = work[inner, :]
            scaled, inverse = norm_rows(x1[outer, :])
            partial[0] = partial[0] + fold(upstream * scaled)
            partial[1] = partial[1] + fold(upstream)
            weighted = upstream * params[1:2, :]
            first_mean = jnp.mean(weighted, axis=-1, keepdims=True)
            second_mean = jnp.mean(weighted * scaled, axis=-1, keepdims=True)
            value = gm[outer, :].astype(F32) + low[inner, :].astype(F32)
            value = value + inverse * (weighted - first_mean - scaled * second_mean)
            x1[outer, :] = value
            gm[outer, :] = value.astype(BF)

        loop(TILE // ROWS, rows_back)

    loop(
        4,
        middle_back,
        {
            0: [lambda: rs_first(7)],
            1: [lambda: rs_second(4)],
            2: [lambda: rs_z2(D_UNIT)],
            3: [lambda: rs_second(5)],
        },
    )
    x_again = pltpu.make_async_copy(x_hbm, h2, local_sem.at[15])
    x_again.start()

    def out_unit(i):
        wts[7, span(TILE * i, TILE), :] = tn(att[:, span(TILE * i, TILE, 128)], gm[...]).astype(BF)

    loop(3, out_unit)
    rs_core(3)
    small_sum[0, 4:5, :] = column_sum(gm[...])

    def attended_back(i):
        r = span(TILE * i, TILE)
        att[r, :] = nt(gm[r, :], wts[3]).astype(BF)

    loop(4, attended_back)
    rs_second(6)
    rs_first(3)
    rs_own(4)
    rs_z3(D_UNIT)

    def attend_back(quad):
        def chain(group, same, half):
            r = span(128 * group, 128)
            at = 256 * quad + 128 * half
            qs = pl.ds(at, 128)
            queries = split_heads(qkv[r, qs])
            keys = qkv[r, pl.ds(768 + at, 128)]
            upstream = split_heads(att[r, qs])
            probs = attention_probs(same, queries, keys)
            probs_grad = nt(upstream, qkv[r, pl.ds(1536 + at, 128)])
            inner = jnp.sum(probs * probs_grad, axis=-1, keepdims=True)
            score_grad = (probs * (probs_grad - inner)).astype(BF)
            to = 768 * quad + 128 * half
            dg[r, pl.ds(to + 512, 128)] = tn(probs.astype(BF), upstream).astype(BF)
            dg[r, pl.ds(to + 256, 128)] = tn(score_grad, queries).astype(BF)
            query_grad = join_heads(nn(score_grad, keys)).astype(BF).astype(F32)
            dg[r, pl.ds(to, 128)] = (query_grad * 0.125).astype(BF)

        def body(i):
            for group in range(GROUPS):
                same = same_caption(GROUPS * i + group)
                for half in range(2):
                    chain(GROUPS * i + group, same, half)

        return body

    def qkv_unit(quad):
        def body(i):
            wts[4 + quad, span(TILE * i, TILE), :] = tn(
                h1[:, span(TILE * i, TILE, 128)], dg[:, pl.ds(768 * quad, 768)]
            ).astype(BF)

        loop(3, body)
        rs_core(quad)

    loop(
        8 // GROUPS,
        attend_back(0),
        {
            1: [lambda: rs_z2(4), lambda: rs_own(5), lambda: rs_second(7)],
            3: [lambda: rs_z2(5), lambda: rs_z3(4), lambda: rs_own(6), lambda: rs_second(3)],
        },
    )
    qkv_unit(0)
    loop(
        8 // GROUPS,
        attend_back(1),
        {
            0: [lambda: rs_first(0)],
            1: [lambda: rs_z4(D_UNIT), lambda: rs_z2(6), lambda: rs_z3(5), lambda: rs_own(7)],
            3: [lambda: rs_second(0), lambda: rs_z2(7), lambda: rs_z3(6), lambda: rs_z4(4), lambda: rs_own(3)],
        },
    )
    qkv_unit(1)
    loop(
        8 // GROUPS,
        attend_back(2),
        {
            0: [lambda: rs_first(1), lambda: rs_z2(3)],
            1: [lambda: rs_own(0), lambda: rs_z3(7), lambda: rs_z4(5)],
            3: [lambda: rs_second(1), lambda: rs_z2(0), lambda: rs_z3(3), lambda: rs_z4(6)],
        },
    )
    qkv_unit(2)
    rs_own(1)
    rs_z3(0)
    rs_z4(7)
    rs_first(2)
    for quad in range(3):
        to = slice(256 * quad, 256 * quad + 256)
        small_sum[0, 2:3, to] = column_sum(dg[:, pl.ds(768 * quad, 256)])
        small_sum[0, 3:4, to] = column_sum(dg[:, pl.ds(768 * quad + 512, 256)])
    x_again.wait()

    def input_back(i):
        r = span(TILE * i, TILE)
        total = jnp.zeros((TILE, 768), F32)
        for quad in range(3):
            for j in range(3):
                part = dg[r, pl.ds(768 * quad + 256 * j, 256)]
                total = total + nt(part, wts[j, :, pl.ds(256 * quad, 256)])
        work[...] = total

        def rows_back(k):
            inner = span(ROWS * k, ROWS)
            outer = span(TILE * i + ROWS * k, ROWS)
            upstream = work[inner, :]
            scaled, inverse = norm_rows(h2[outer, :].astype(F32))
            partial[2] = partial[2] + fold(upstream * scaled)
            partial[3] = partial[3] + fold(upstream)
            weighted = upstream * params[0:1, :]
            first_mean = jnp.mean(weighted, axis=-1, keepdims=True)
            second_mean = jnp.mean(weighted * scaled, axis=-1, keepdims=True)
            value = x1[outer, :] + inverse * (weighted - first_mean - scaled * second_mean)
            att[outer, :] = value.astype(BF)

        loop(TILE // ROWS, rows_back)

    loop(
        4,
        input_back,
        {
            0: [lambda: rs_second(2), lambda: rs_z2(1), lambda: rs_z4(3)],
            1: [lambda: rs_own(2), lambda: rs_z4(0)],
            2: [lambda: rs_z3(1)],
            3: [lambda: rs_z2(2)],
        },
    )
    input_copy = pltpu.make_async_copy(att, input_out, local_sem.at[34])
    input_copy.start()
    for row, index in ((0, 2), (1, 0), (6, 3), (7, 1)):
        small_sum[0, row : row + 1, :] = jnp.sum(partial[index], axis=0, keepdims=True)
    small_sum[0, 12:16, :] = jnp.zeros((4, 768), F32)
    sum_start(0)
    rs_z4(1)
    rs_z3(2)
    sum_wait(0)
    sum_start(1)
    for unit in (D_UNIT, 4, 5, 6, 7, 3, 0):
        rs_done(unit)
    sum_wait(1)
    sum_start(2)
    rs_z4(2)
    sum_wait(2)
    sum_start(3)
    rs_done(1)
    sum_wait(3)
    sum_start(4)
    rs_done(2)
    sum_wait(4)
    small_out[...] = small_sum[5]

    input_copy.wait()
    for unit in range(9):
        for slot in (2, 3):
            result_copy(unit, slot).wait()
        for delta in range(4):
            core_copy(unit, delta).wait_send()
        for kind in range(6):
            xy_copy(unit, kind).wait_send()

        @pl.when(is_end)
        def _(unit=unit):
            for index in range(2):
                z_end(unit, index).wait_send()

        @pl.when(is_mid)
        def _(unit=unit):
            for index in range(4):
                z_mid(unit, index).wait_send()

    for step in range(5):
        sum_copy(step).wait_send()


def finish_kernel(
    units_hbm,
    down_hbm,
    input_hbm,
    small_ref,
    loss_ref,
    qkv_out,
    out_out,
    up_out,
    down_out,
    gain_out,
    shift_out,
    hidden_out,
    input_out,
    loss_out,
    units,
    down,
    tokens,
    qkv,
    out,
    up,
    down_wide,
    sem,
):
    fs = lax.axis_index("fsdp")

    def move(src, dst, index):
        copy = pltpu.make_async_copy(src, dst, sem.at[index])
        copy.start()
        return copy

    units_in = move(units_hbm, units, 0)
    down_in = move(down_hbm, down, 1)
    tokens_in = move(input_hbm, tokens, 2)
    for shard in range(8):

        @pl.when(fs == shard)
        def _(shard=shard):
            gain_out[...] = small_ref[0:2, 96 * shard : 96 * shard + 96]
            shift_out[...] = small_ref[2:8, 96 * shard : 96 * shard + 96]
            for q in range(3):
                at = 384 * (shard % 2) + 128 * q
                hidden_out[q : q + 1, :] = small_ref[8 + shard // 2 : 9 + shard // 2, at : at + 128]

    loss_out[...] = loss_ref[...]
    units_in.wait()
    for quad in range(3):
        for j in range(3):
            at = 768 * j + 256 * quad
            qkv[:, at : at + 256] = units[quad, :, 256 * j : 256 * j + 256].astype(F32)
    moves = [move(qkv, qkv_out, 3)]
    out[...] = units[3].astype(F32)
    moves.append(move(out, out_out, 4))
    for j in range(4):
        up[:, 768 * j : 768 * j + 768] = units[4 + j].astype(F32)
    moves.append(move(up, up_out, 5))
    down_in.wait()
    down_wide[...] = down[...].astype(F32)
    moves.append(move(down_wide, down_out, 6))
    tokens_in.wait()
    moves.append(move(tokens, input_out, 7))
    for copy in moves:
        copy.wait()


def fused_step(
    incoming_word_states,
    sentence_number_per_word,
    described_picture,
    lookup_matrices,
    mixer_exit_matrix,
    widening_matrix,
    narrowing_matrix,
    normalizer_multipliers,
    word_offsets,
    widened_offset,
    picture_patches,
    picture_lookup_matrices,
    picture_mixer_exit_matrix,
    picture_widening_matrix,
    picture_narrowing_matrix,
    picture_normalizer_multipliers,
    picture_offsets,
    picture_widened_offset,
    sharpness_coefficient,
    objective_offset,
):
    rows, length, width = incoming_word_states.shape
    tokens = rows * length
    vmem = pl.BlockSpec(memory_space=pltpu.VMEM)
    hbm = pl.BlockSpec(memory_space=pl.ANY)
    smem = pl.BlockSpec(memory_space=pltpu.SMEM)
    dma = pltpu.SemaphoreType.DMA
    outs = pl.pallas_call(
        fused_kernel,
        out_shape=(
            jax.ShapeDtypeStruct((8, 96, width), BF),
            jax.ShapeDtypeStruct((384, width), BF),
            jax.ShapeDtypeStruct((tokens, width), BF),
            jax.ShapeDtypeStruct((16, width), F32),
            jax.ShapeDtypeStruct((1, 64), F32),
        ),
        in_specs=[smem, smem, hbm, vmem, vmem, *[hbm] * 4, *[vmem] * 3, *[hbm] * 5, *[vmem] * 3],
        out_specs=(hbm, hbm, hbm, vmem, vmem),
        scratch_shapes=[
            pltpu.VMEM((8, 768, 768), BF),
            pltpu.VMEM((3072, 768), BF),
            pltpu.VMEM((1024, 768), BF),
            pltpu.VMEM((1024, 2304), BF),
            pltpu.VMEM((1024, 768), BF),
            pltpu.VMEM((1024, 768), F32),
            pltpu.VMEM((1024, 768), BF),
            pltpu.VMEM((1024, 3072), BF),
            pltpu.VMEM((1024, 3072), BF),
            pltpu.VMEM((1024, 768), BF),
            pltpu.VMEM((3072, 768), BF),
            pltpu.VMEM((8, 4, 96, 768), BF),
            pltpu.VMEM((4, 384, 768), BF),
            pltpu.VMEM((8, 3, 48, 768), BF),
            pltpu.VMEM((3, 192, 768), BF),
            pltpu.VMEM((8, 3, 48, 768), BF),
            pltpu.VMEM((3, 192, 768), BF),
            pltpu.VMEM((8, 4, 48, 768), BF),
            pltpu.VMEM((4, 192, 768), BF),
            pltpu.VMEM((TILE, 768), F32),
            pltpu.VMEM((TILE, 768), BF),
            pltpu.VMEM((4, 8, 8, 768), BF),
            pltpu.VMEM((8, 16, 128), F32),
            pltpu.VMEM((16, 768), F32),
            pltpu.VMEM((16, 768), F32),
            pltpu.VMEM((64, 1024), BF),
            pltpu.VMEM((64, 768), F32),
            pltpu.VMEM((64, 768), BF),
            pltpu.VMEM((64, 768), BF),
            pltpu.VMEM((4, 8, 768), F32),
            pltpu.VMEM((6, 16, 768), F32),
            pltpu.VMEM((5, 16, 768), F32),
            pltpu.VMEM((6, 8, 768), F32),
            dma((N_AG, 13)),
            dma((N_AG, 13)),
            dma((9, 4)),
            dma((9, 4)),
            dma((9, 6)),
            dma((9, 6)),
            dma((9, 4)),
            dma((9, 4)),
            dma((21,)),
            dma((21,)),
            dma((35,)),
        ],
        compiler_params=pltpu.CompilerParams(
            collective_id=0, has_side_effects=True, vmem_limit_bytes=67043328
        ),
        name="lit_step",
    )(
        sharpness_coefficient,
        objective_offset,
        incoming_word_states.reshape(tokens, width),
        sentence_number_per_word,
        described_picture.reshape(1, -1),
        lookup_matrices,
        mixer_exit_matrix,
        widening_matrix,
        narrowing_matrix,
        normalizer_multipliers,
        word_offsets,
        widened_offset.reshape(3, 128),
        picture_patches.transpose(1, 0, 2).reshape(-1, width),
        picture_lookup_matrices,
        picture_mixer_exit_matrix,
        picture_widening_matrix,
        picture_narrowing_matrix,
        picture_normalizer_multipliers,
        picture_offsets,
        picture_widened_offset.reshape(24, 128),
    )
    finished = pl.pallas_call(
        finish_kernel,
        out_shape=(
            jax.ShapeDtypeStruct((96, 2304), F32),
            jax.ShapeDtypeStruct((96, width), F32),
            jax.ShapeDtypeStruct((96, 3072), F32),
            jax.ShapeDtypeStruct((384, width), F32),
            jax.ShapeDtypeStruct((2, 96), F32),
            jax.ShapeDtypeStruct((6, 96), F32),
            jax.ShapeDtypeStruct((3, 128), F32),
            jax.ShapeDtypeStruct((tokens, width), BF),
            jax.ShapeDtypeStruct((1, 64), F32),
        ),
        in_specs=[hbm, hbm, hbm, vmem, vmem],
        out_specs=(hbm, hbm, hbm, hbm, vmem, vmem, vmem, hbm, vmem),
        scratch_shapes=[
            pltpu.VMEM((8, 96, width), BF),
            pltpu.VMEM((384, width), BF),
            pltpu.VMEM((tokens, width), BF),
            pltpu.VMEM((96, 2304), F32),
            pltpu.VMEM((96, width), F32),
            pltpu.VMEM((96, 3072), F32),
            pltpu.VMEM((384, width), F32),
            dma((8,)),
        ],
        compiler_params=pltpu.CompilerParams(vmem_limit_bytes=60 * 2**20),
        name="lit_finish",
    )(*outs)
    finished = list(finished)
    finished[6] = finished[6].reshape(-1)
    finished[7] = finished[7].reshape(rows, length, width)
    finished[8] = finished[8].reshape(-1)
    return tuple(finished)


def solution(mesh):
    fits = mesh.shape["fsdp"] == 8 and mesh.shape["dp"] == 4
    return jax.shard_map(
        fused_step if fits else per_device,
        mesh=mesh,
        in_specs=(
            P(("fsdp", "dp"), None, None),
            P(("fsdp", "dp"), None),
            P(("fsdp", "dp")),
            P("fsdp", None),
            P("fsdp", None),
            P("fsdp", None),
            P("fsdp", None),
            P(None, "fsdp"),
            P(None, "fsdp"),
            P("fsdp"),
            P(("fsdp", "dp"), None, None),
            P(),
            P(),
            P(),
            P(),
            P(),
            P(),
            P(),
            P(),
            P(),
        ),
        out_specs=(
            P("fsdp", None),
            P("fsdp", None),
            P("fsdp", None),
            P("fsdp", None),
            P(None, "fsdp"),
            P(None, "fsdp"),
            P("fsdp"),
            P(("fsdp", "dp"), None, None),
            P(("fsdp", "dp")),
        ),
        check_vma=False,
    )
```

```python
import math

import jax
import jax.numpy as jnp
from jax import lax
from jax.experimental import pallas as pl
from jax.experimental.pallas import tpu as pltpu
from jax.sharding import PartitionSpec as P

HEAD_DIM = 64
CAPS = 4


def layer_norm(values, gain, shift):
    centred = values - jnp.mean(values, axis=-1, keepdims=True)
    inverse = lax.rsqrt(jnp.mean(centred * centred, axis=-1, keepdims=True) + 1e-06)
    scaled = centred * inverse
    return (scaled * gain + shift, scaled, inverse)


def norm_back(grad_scaled, scaled, inverse):
    first_mean = jnp.mean(grad_scaled, axis=-1, keepdims=True)
    second_mean = jnp.mean(grad_scaled * scaled, axis=-1, keepdims=True)
    return inverse * (grad_scaled - first_mean - scaled * second_mean)


def gelu_exact(values):
    return jax.nn.gelu(values, approximate=False)


def forward_block(flat, rows, length, mask, weights):
    qkv_w, out_w, up_w, down_w, gains_low, biases_low, up_b = weights
    gains = gains_low.astype(jnp.float32)
    biases = biases_low.astype(jnp.float32)
    channel_count = flat.shape[-1]
    heads = channel_count // HEAD_DIM
    scale = 1.0 / math.sqrt(HEAD_DIM)
    first, scaled_one, inverse_one = layer_norm(flat, gains[0], biases[4])
    first_low = first.astype(jnp.bfloat16)
    mixed = jnp.dot(first_low, qkv_w, preferred_element_type=jnp.float32)
    query = (
        ((mixed[:, :channel_count] + biases[0]) * scale)
        .astype(jnp.bfloat16)
        .reshape(rows, length, heads, HEAD_DIM)
    )
    key_low = (
        mixed[:, channel_count : 2 * channel_count]
        .astype(jnp.bfloat16)
        .reshape(rows, length, heads, HEAD_DIM)
    )
    value_low = (
        (mixed[:, 2 * channel_count :] + biases[1])
        .astype(jnp.bfloat16)
        .reshape(rows, length, heads, HEAD_DIM)
    )
    scores = jnp.einsum("rqhd,rkhd->rhqk", query, key_low, preferred_element_type=jnp.float32)
    if mask is not None:
        scores = jnp.where(mask[:, None], scores, -1e30)
    probs = jax.nn.softmax(scores, axis=-1)
    probs_low = probs.astype(jnp.bfloat16)
    attended = jnp.einsum(
        "rhqk,rkhd->rqhd", probs_low, value_low, preferred_element_type=jnp.float32
    )
    attended = attended.astype(jnp.bfloat16).reshape(rows * length, channel_count)
    middle = flat + (jnp.dot(attended, out_w, preferred_element_type=jnp.float32) + biases[2])
    second, scaled_two, inverse_two = layer_norm(middle, gains[1], biases[5])
    second_low = second.astype(jnp.bfloat16)
    hidden = jnp.dot(second_low, up_w, preferred_element_type=jnp.float32) + up_b.astype(
        jnp.float32
    )
    active = gelu_exact(hidden).astype(jnp.bfloat16)
    output = middle + (jnp.dot(active, down_w, preferred_element_type=jnp.float32) + biases[3])
    saved = (
        scaled_one,
        inverse_one,
        first_low,
        query,
        key_low,
        value_low,
        probs,
        probs_low,
        attended,
        scaled_two,
        inverse_two,
        second_low,
        hidden,
        active,
    )
    return (output, saved)


def backward_block(grad_output, saved, weights, rows, length):
    qkv_w, out_w, up_w, down_w, gains_low, biases_low, up_b = weights
    gains = gains_low.astype(jnp.float32)
    (
        scaled_one,
        inverse_one,
        first_low,
        query,
        key_low,
        value_low,
        probs,
        probs_low,
        attended,
        scaled_two,
        inverse_two,
        second_low,
        hidden,
        active,
    ) = saved
    channel_count = grad_output.shape[-1]
    heads = channel_count // HEAD_DIM
    scale = 1.0 / math.sqrt(HEAD_DIM)
    count = rows * length
    down_grad = grad_output.astype(jnp.bfloat16)
    grad_down_bias = jnp.sum(down_grad, axis=0, dtype=jnp.float32)
    grad_down_w = jnp.einsum("nf,nd->fd", active, down_grad, preferred_element_type=jnp.float32)
    active_grad = jnp.einsum("nd,fd->nf", down_grad, down_w, preferred_element_type=jnp.float32)
    gelu_back = jax.vjp(gelu_exact, hidden)[1]
    hidden_grad = gelu_back(active_grad)[0].astype(jnp.bfloat16)
    grad_up_bias = jnp.sum(hidden_grad, axis=0, dtype=jnp.float32)
    grad_up_w = jnp.einsum("nd,nf->df", second_low, hidden_grad, preferred_element_type=jnp.float32)
    second_grad = jnp.einsum("nf,df->nd", hidden_grad, up_w, preferred_element_type=jnp.float32)
    grad_gain_two = jnp.sum(second_grad * scaled_two, axis=0)
    grad_shift_two = jnp.sum(second_grad, axis=0)
    middle_grad = grad_output + norm_back(second_grad * gains[1], scaled_two, inverse_two)
    branch_grad = middle_grad.astype(jnp.bfloat16)
    grad_out_bias = jnp.sum(branch_grad, axis=0, dtype=jnp.float32)
    grad_out_w = jnp.einsum("nd,ne->de", attended, branch_grad, preferred_element_type=jnp.float32)
    attended_grad = jnp.einsum("ne,de->nd", branch_grad, out_w, preferred_element_type=jnp.float32)
    attended_grad = attended_grad.astype(jnp.bfloat16).reshape(rows, length, heads, HEAD_DIM)
    probs_grad = jnp.einsum(
        "rqhd,rkhd->rhqk", attended_grad, value_low, preferred_element_type=jnp.float32
    )
    value_grad = jnp.einsum(
        "rhqk,rqhd->rkhd", probs_low, attended_grad, preferred_element_type=jnp.float32
    ).astype(jnp.bfloat16)
    score_grad = probs * (probs_grad - jnp.sum(probs * probs_grad, axis=-1, keepdims=True))
    score_grad = score_grad.astype(jnp.bfloat16)
    query_grad = jnp.einsum(
        "rhqk,rkhd->rqhd", score_grad, key_low, preferred_element_type=jnp.float32
    ).astype(jnp.bfloat16)
    key_grad = jnp.einsum(
        "rhqk,rqhd->rkhd", score_grad, query, preferred_element_type=jnp.float32
    ).astype(jnp.bfloat16)
    query_flat = query_grad.reshape(count, channel_count) * scale
    value_flat = value_grad.reshape(count, channel_count)
    mixed_grad = jnp.concatenate(
        [query_flat, key_grad.reshape(count, channel_count), value_flat], axis=1
    )
    grad_query_bias = jnp.sum(query_flat, axis=0, dtype=jnp.float32)
    grad_value_bias = jnp.sum(value_flat, axis=0, dtype=jnp.float32)
    grad_qkv_w = jnp.einsum("nd,ne->de", first_low, mixed_grad, preferred_element_type=jnp.float32)
    first_grad = jnp.einsum("ne,de->nd", mixed_grad, qkv_w, preferred_element_type=jnp.float32)
    grad_gain_one = jnp.sum(first_grad * scaled_one, axis=0)
    grad_shift_one = jnp.sum(first_grad, axis=0)
    input_grad = middle_grad + norm_back(first_grad * gains[0], scaled_one, inverse_one)
    grad_gains = jnp.stack([grad_gain_one, grad_gain_two])
    grad_biases = jnp.stack(
        [
            grad_query_bias,
            grad_value_bias,
            grad_out_bias,
            grad_down_bias,
            grad_shift_one,
            grad_shift_two,
        ]
    )
    return (
        input_grad,
        (grad_qkv_w, grad_out_w, grad_up_w, grad_down_w, grad_gains, grad_biases, grad_up_bias),
    )


def image_first_token(patches, qkv_w, out_w, up_w, down_w, gains_low, biases_low, up_b):
    rows, length, channel_count = patches.shape
    gains = gains_low.astype(jnp.float32)
    biases = biases_low.astype(jnp.float32)
    heads = channel_count // HEAD_DIM
    scale = 1.0 / math.sqrt(HEAD_DIM)
    first_low = layer_norm(patches.astype(jnp.float32), gains[0], biases[4])[0].astype(jnp.bfloat16)
    flat_low = first_low.reshape(rows * length, channel_count)
    query = (
        (jnp.dot(first_low[:, 0], qkv_w[:, :channel_count], preferred_element_type=jnp.float32) + biases[0])
        * scale
    ).astype(jnp.bfloat16).reshape(rows, heads, HEAD_DIM)
    mixed = jnp.dot(flat_low, qkv_w[:, channel_count:], preferred_element_type=jnp.float32)
    key_low = mixed[:, :channel_count].astype(jnp.bfloat16).reshape(rows, length, heads, HEAD_DIM)
    value_low = (
        (mixed[:, channel_count:] + biases[1]).astype(jnp.bfloat16).reshape(rows, length, heads, HEAD_DIM)
    )
    scores = jnp.einsum("rhd,rkhd->rhk", query, key_low, preferred_element_type=jnp.float32)
    probs_low = jax.nn.softmax(scores, axis=-1).astype(jnp.bfloat16)
    attended = jnp.einsum("rhk,rkhd->rhd", probs_low, value_low, preferred_element_type=jnp.float32)
    attended = attended.astype(jnp.bfloat16).reshape(rows, channel_count)
    middle = patches[:, 0].astype(jnp.float32) + (
        jnp.dot(attended, out_w, preferred_element_type=jnp.float32) + biases[2]
    )
    second_low = layer_norm(middle, gains[1], biases[5])[0].astype(jnp.bfloat16)
    hidden = jnp.dot(second_low, up_w, preferred_element_type=jnp.float32) + up_b.astype(jnp.float32)
    active = gelu_exact(hidden).astype(jnp.bfloat16)
    return middle + (jnp.dot(active, down_w, preferred_element_type=jnp.float32) + biases[3])


def per_device(
    incoming_word_states,
    sentence_number_per_word,
    described_picture,
    lookup_matrices,
    mixer_exit_matrix,
    widening_matrix,
    narrowing_matrix,
    normalizer_multipliers,
    word_offsets,
    widened_offset,
    picture_patches,
    picture_lookup_matrices,
    picture_mixer_exit_matrix,
    picture_widening_matrix,
    picture_narrowing_matrix,
    picture_normalizer_multipliers,
    picture_offsets,
    picture_widened_offset,
    sharpness_coefficient,
    objective_offset,
):
    rows, length, channel_count = incoming_word_states.shape
    whole = (
        lax.all_gather(lookup_matrices, "fsdp", axis=0, tiled=True),
        lax.all_gather(mixer_exit_matrix, "fsdp", axis=0, tiled=True),
        lax.all_gather(widening_matrix, "fsdp", axis=0, tiled=True),
        lax.all_gather(narrowing_matrix, "fsdp", axis=0, tiled=True),
        lax.all_gather(normalizer_multipliers, "fsdp", axis=1, tiled=True),
        lax.all_gather(word_offsets, "fsdp", axis=1, tiled=True),
        lax.all_gather(widened_offset, "fsdp", axis=0, tiled=True),
    )
    image_rows, image_length = (picture_patches.shape[0], picture_patches.shape[1])
    image_token = image_first_token(
        picture_patches,
        picture_lookup_matrices,
        picture_mixer_exit_matrix,
        picture_widening_matrix,
        picture_narrowing_matrix,
        picture_normalizer_multipliers,
        picture_offsets,
        picture_widened_offset,
    )
    image_embed = (
        image_token * lax.rsqrt(jnp.mean(image_token * image_token, axis=-1, keepdims=True) + 1e-06)
    ).astype(jnp.bfloat16)
    mask = sentence_number_per_word[:, :, None] == sentence_number_per_word[:, None, :]
    flat = incoming_word_states.astype(jnp.float32).reshape(rows * length, channel_count)
    text_result, saved = forward_block(flat, rows, length, mask, whole)
    member = (sentence_number_per_word[:, :, None] == jnp.arange(CAPS, dtype=jnp.int32)).astype(
        jnp.float32
    )
    counts = jnp.sum(member, axis=1)[:, :, None]
    pooled = (
        jnp.einsum(
            "rsc,rsd->rcd",
            member,
            text_result.reshape(rows, length, channel_count),
            precision=lax.Precision.HIGHEST,
        )
        / counts
    )
    pooled = pooled.reshape(rows * CAPS, channel_count)
    inverse = lax.rsqrt(jnp.mean(pooled * pooled, axis=-1, keepdims=True) + 1e-06)
    embed = pooled * inverse
    embed_low = embed.astype(jnp.bfloat16)
    multiplier_amount = sharpness_coefficient[0] / math.sqrt(channel_count)
    piece = lax.all_gather(image_embed, ("fsdp", "dp"), axis=0, tiled=True)
    unscaled_similarity = jnp.einsum(
        "cd,nd->cn", embed_low, piece, preferred_element_type=jnp.float32
    )
    match_similarity = multiplier_amount * unscaled_similarity + objective_offset[0]
    positive = described_picture[:, None] == jnp.arange(piece.shape[0], dtype=jnp.int32)[None, :]
    labels = jnp.where(positive, 1.0, -1.0)
    total = jnp.sum(jax.nn.softplus(-labels * match_similarity), axis=1)
    slope = (
        (jax.nn.sigmoid(match_similarity) - positive.astype(jnp.float32)) * multiplier_amount
    ).astype(jnp.bfloat16)
    grad_embed = jnp.einsum("cn,nd->cd", slope, piece, preferred_element_type=jnp.float32)
    images_all = image_rows * lax.axis_size("fsdp") * lax.axis_size("dp")
    loss = total / images_all
    pooled_grad = inverse * (
        grad_embed - embed * jnp.mean(grad_embed * embed, axis=-1, keepdims=True)
    )
    per_caption = pooled_grad.reshape(rows, CAPS, channel_count) / counts
    token_grad = jnp.einsum(
        "rsc,rcd->rsd", member, per_caption, precision=lax.Precision.HIGHEST
    ).reshape(rows * length, channel_count)
    input_grad, grads = backward_block(token_grad, saved, whole, rows, length)
    owned = [
        lax.psum(
            lax.psum_scatter(piece_grad.astype(jnp.bfloat16), "fsdp", scatter_dimension=0, tiled=True), "dp"
        ).astype(jnp.float32)
        for piece_grad in grads[:4]
    ]
    small = jnp.concatenate([grads[4], grads[5], grads[6].reshape(-1, channel_count)], axis=0)
    small = lax.psum(small, ("fsdp", "dp"))
    place = lax.axis_index("fsdp")
    width = normalizer_multipliers.shape[1]
    columns = lax.dynamic_slice_in_dim(small[:8], place * width, width, axis=1)
    hidden_width = widened_offset.shape[0]
    hidden_part = lax.dynamic_slice_in_dim(small[8:].reshape(-1), place * hidden_width, hidden_width)
    summed = (*owned, columns[:2], columns[2:8], hidden_part)
    grad_input = input_grad.astype(jnp.bfloat16).reshape(rows, length, channel_count)
    return (
        summed[0],
        summed[1],
        summed[2],
        summed[3],
        summed[4],
        summed[5],
        summed[6],
        grad_input,
        loss,
    )


BF = jnp.bfloat16
F32 = jnp.float32
MESH_ID = pl.DeviceIdType.MESH
TILE = 256
ROWS = 128
GROUPS = 2
N_AG = 11
Z_PAIRS = ((0, 1), (3, 4), (6, 7))
GATHER = {
    "start": ("o1", "o0", "o2",),
    "mixed": ("r0", "o4", "o6", "r1", "o3",),
    "image": ("r2", "l1", "l0", "r4", "o7",),
    "norm": ("z0", "l4", "r3", "o5", "y0", "l2",),
    "project0": ("r7", "o8",),
    "project1": ("l3", "r6",),
    "attend2": ("o9", "r5",),
    "attend3": ("z1", "y1",),
    "attend7": ("o10", "l6", "r8", "l7",),
    "norm2": ("l5", "r9", "z2",),
    "widen0": ("y2",),
    "widen1": ("r10",),
    "widen2": ("l8",),
    "widen3": ("l10", "l9",),
}
D_UNIT = 8


def nn(a, b):
    return jnp.dot(a, b, preferred_element_type=F32)


def nt(a, b):
    return lax.dot_general(a, b, (((1,), (1,)), ((), ())), preferred_element_type=F32)


def tn(a, b):
    return lax.dot_general(a, b, (((0,), (0,)), ((), ())), preferred_element_type=F32)


def span(start, size, unit=16):
    if isinstance(start, int):
        return pl.ds(start, size)
    return pl.ds(pl.multiple_of(start, unit), size)


def norm_rows(values):
    centred = values - jnp.mean(values, axis=-1, keepdims=True)
    inverse = lax.rsqrt(jnp.mean(centred * centred, axis=-1, keepdims=True) + 1e-06)
    return centred * inverse, inverse


def normal_cdf(values):
    return 0.5 * (1.0 + lax.erf(values * math.sqrt(0.5)))


def loop(count, body, events=None):
    def step(i, carry):
        body(i)
        for at, calls in (events or {}).items():

            @pl.when(i == at)
            def _(calls=calls):
                for call in calls:
                    call()

        return carry

    lax.fori_loop(0, count, step, 0)


def fused_kernel(
    sharp_ref,
    offset_ref,
    x_hbm,
    segment_ref,
    described_ref,
    qkv_hbm,
    out_hbm,
    up_hbm,
    down_hbm,
    gain_ref,
    shift_ref,
    hidden_ref,
    patches_hbm,
    pqkv_hbm,
    pout_hbm,
    pup_hbm,
    pdown_hbm,
    pgain_ref,
    pshift_ref,
    phidden_ref,
    units_out,
    down_out,
    input_out,
    small_out,
    loss_out,
    wts,
    wdn,
    h1,
    qkv,
    att,
    x1,
    h2,
    act,
    dg,
    gm,
    sdn,
    lc,
    lcd,
    lx,
    lxd,
    ly,
    lyd,
    lz,
    lzd,
    work,
    low,
    faces,
    small_in,
    params,
    img_gain,
    member,
    pooled,
    caption_hi,
    caption_lo,
    partial,
    small_sum,
    small_land,
    face_rows,
    ag_send,
    ag_recv,
    core_send,
    core_recv,
    xy_send,
    xy_recv,
    z_send,
    z_recv,
    side_send,
    side_recv,
    local_sem,
):
    fs = lax.axis_index("fsdp")
    dp = lax.axis_index("dp")
    core = fs % 2
    xb = (fs // 2) % 2
    yb = fs // 4
    fs_core = fs + 1 - 2 * core
    fs_x = fs + 2 - 4 * xb
    fs_y = fs + 4 - 8 * yb
    fs_diag = fs_x + 4 - 8 * yb
    flip = 1 - 2 * core
    peer_core = (fs_core, dp)
    peer_x = (fs_x, dp)
    peer_y = (fs_y, dp)
    half_z = dp // 2
    is_end = (dp == 0) | (dp == 3)
    is_mid = (dp == 1) | (dp == 2)
    near = half_z
    far = 1 - half_z
    dp_inner = 1 + half_z
    dp_end = 3 * half_z
    dp_mid = 2 - half_z
    dp_pair = dp + 1 - 2 * (dp % 2)
    dp_far = dp + 2 - 4 * half_z

    barrier = pltpu.get_barrier_semaphore()
    others = (fs_core, fs_x, fs_y, fs_diag, fs_x + flip, fs_y + flip, fs_diag + flip)
    greet = [(other, dp) for other in others] + [(fs, dp_pair), (fs, dp_far)]
    for peer in greet:
        pl.semaphore_signal(barrier, inc=1, device_id=peer, device_id_type=MESH_ID)

    local = []

    def fetch(src, dst):
        copy = pltpu.make_async_copy(src, dst, local_sem.at[len(local)])
        copy.start()
        local.append(copy)
        return copy

    own_rows = span(96 * fs, 96)
    own_copies = [fetch(qkv_hbm.at[:, pl.ds(768 * j, 768)], wts.at[j, own_rows, :]) for j in range(3)]
    own_copies.append(fetch(out_hbm, wts.at[3, own_rows, :]))
    own_copies += [fetch(up_hbm.at[:, pl.ds(768 * j, 768)], wts.at[4 + j, own_rows, :]) for j in range(4)]
    own_copies.append(fetch(down_hbm, wdn.at[span(384 * fs, 384), :]))
    patches_copy = fetch(patches_hbm, gm.at[pl.ds(512, 400), :])
    pqkv_copy = fetch(pqkv_hbm, act.at[pl.ds(0, 768), pl.ds(0, 2304)])
    x_copy = fetch(x_hbm, h2)
    pout_copy = fetch(pout_hbm, act.at[pl.ds(0, 768), pl.ds(2304, 768)])
    pup_copy = fetch(pup_hbm, dg.at[pl.ds(0, 768), :])
    pdown_copy = fetch(pdown_hbm, sdn)

    small_in[fs] = jnp.zeros((16, 128), F32)
    small_in[fs, 0:2, 0:96] = gain_ref[...].astype(F32)
    small_in[fs, 2:8, 0:96] = shift_ref[...].astype(F32)
    small_in[fs, 8:11, :] = hidden_ref[...].astype(F32)
    pl.semaphore_wait(barrier, len(greet))

    def weight(unit, shard, part=None):
        if unit < 8:
            rows = span(96 * shard, 96) if part is None else span(96 * shard + 48 * part, 48)
            return wts.at[unit, rows, :]
        rows = span(384 * shard, 384) if part is None else span(384 * shard + 192 * part, 192)
        return wdn.at[rows, pl.ds(256 * (unit - 8), 256)]

    def own_weight(unit):
        if unit < 3:
            return qkv_hbm.at[:, pl.ds(768 * unit, 768)]
        if unit == 3:
            return out_hbm
        if unit < 8:
            return up_hbm.at[:, pl.ds(768 * (unit - 4), 768)]
        return down_hbm.at[:, pl.ds(256 * (unit - 8), 256)]

    def ag(unit, kind, ref, peer, source=None):
        return pltpu.make_async_remote_copy(
            src_ref=ref if source is None else source,
            dst_ref=ref,
            send_sem=ag_send.at[unit, kind],
            recv_sem=ag_recv.at[unit, kind],
            device_id=peer,
            device_id_type=MESH_ID,
        )

    def ag_out(unit, kind):
        shard, part, peer = (
            (fs, None, peer_core),
            (fs, None, peer_x),
            (fs, None, peer_y),
            (fs_x, 0, peer_y),
            (fs_y, 1, peer_x),
            (fs_x, None, peer_core),
            (fs_y, None, peer_core),
            (fs_diag, 0, peer_core),
            (fs_diag, 1, peer_core),
            (fs_x, None, (fs, dp_pair)),
            (fs_y, None, (fs, dp_pair)),
            (fs_diag, 0, (fs, dp_pair)),
            (fs_diag, 1, (fs, dp_pair)),
        )[kind]
        return ag(unit, kind, weight(unit, shard, part), peer, own_weight(unit) if kind < 3 else None)

    def ag_in(unit, kind):
        shard, part = (
            (fs_core, None),
            (fs_x, None),
            (fs_y, None),
            (fs_diag, 0),
            (fs_diag, 1),
            (fs_x + flip, None),
            (fs_y + flip, None),
            (fs_diag + flip, 0),
            (fs_diag + flip, 1),
            (fs_x, None),
            (fs_y, None),
            (fs_diag, 0),
            (fs_diag, 1),
        )[kind]
        return ag(unit, kind, weight(unit, shard, part), peer_core)

    def fetching(unit, body):
        for pair in Z_PAIRS:
            if unit in pair:
                pl.when(dp % 2 == pair.index(unit))(body)
                return
        body()

    def ag_own(*units):
        for unit in units:

            def body(unit=unit):
                for kind in (1, 2):
                    ag_out(unit, kind).start()

            fetching(unit, body)
            ag_out(unit, 0).start()

    def handed(unit):
        return any(unit in pair for pair in Z_PAIRS)

    def ag_relay(*units):
        for unit in units:

            def body(unit=unit):
                for arrived, onward, inner, across in ((1, 3, 5, 9), (2, 4, 6, 10)):
                    ag_in(unit, arrived).wait_recv()
                    ag_out(unit, onward).start()
                    ag_out(unit, inner).start()
                    if handed(unit):
                        ag_out(unit, across).start()

            fetching(unit, body)

    def ag_last(*units):
        for unit in units:

            def body(unit=unit):
                for arrived, inner, across in ((3, 7, 11), (4, 8, 12)):
                    ag_in(unit, arrived).wait_recv()
                    ag_out(unit, inner).start()
                    if handed(unit):
                        ag_out(unit, across).start()

            fetching(unit, body)

    def ag_across(pair, kinds):
        for index in range(2):

            @pl.when(dp % 2 != index)
            def _(unit=pair[index]):
                for arrived, inner in kinds:
                    ag_in(unit, arrived).wait_recv()
                    ag_out(unit, inner).start()

    def z_relay(pair):
        ag_across(pair, ((9, 5), (10, 6)))

    def z_last(pair):
        ag_across(pair, ((11, 7), (12, 8)))

    def ag_drain():
        for unit in range(N_AG):

            def body(unit=unit):
                for kind in (1, 2, 3, 4) + ((9, 10, 11, 12) if handed(unit) else ()):
                    ag_out(unit, kind).wait_send()

            fetching(unit, body)
            for kind in (0, 5, 6, 7, 8):
                ag_out(unit, kind).wait_send()

    def hook(point):
        for step in GATHER.get(point, ()):
            number = int(step[1:])
            if step[0] == "o":
                ag_own(number)
            elif step[0] == "r":
                ag_relay(number)
            elif step[0] == "l":
                ag_last(number)
            elif step[0] == "z":
                z_relay(Z_PAIRS[number])
            else:
                z_last(Z_PAIRS[number])

    def ready(unit):
        for kind in (0, 5, 6, 7, 8):
            ag_in(unit, kind).wait_recv()

    def side(index, src, dst, peer):
        return pltpu.make_async_remote_copy(
            src_ref=src,
            dst_ref=dst,
            send_sem=side_send.at[index],
            recv_sem=side_recv.at[index],
            device_id=peer,
            device_id_type=MESH_ID,
        )

    chip_slot = fs - core
    row_slot = 4 * yb

    def param_copy(index, slot):
        ref = small_in.at[slot]
        return side(index, ref, ref, (others[index], dp))

    far_plane = 2 - 2 * half_z
    face_steps = (
        (dp, 1, fs, 1, peer_core, dp, fs_core),
        (dp, 1, chip_slot, 2, peer_x, dp, chip_slot + 2 - 4 * xb),
        (dp, 1, row_slot, 4, peer_y, dp, 4 - row_slot),
        (dp, 1, 4 * core, 4, (fs, dp_pair), dp_pair, 4 * core),
        (2 * half_z, 2, 4 * core, 4, (fs, dp_far), far_plane, 4 * core),
        (dp_pair, 1, 4 * core, 4, peer_core, dp_pair, 4 - 4 * core),
        (far_plane, 2, 4 * core, 4, peer_core, far_plane, 4 - 4 * core),
    )

    def face_copy(step, landing):
        d0, dn, f0, fn, peer, ld, lf = face_steps[step]
        if landing:
            d0, f0 = ld, lf
        ref = faces.at[pl.ds(d0, dn), pl.ds(f0, fn)]
        return side(7 + step, ref, ref, peer)

    def face_start(step):
        face_copy(step, False).start()

    def face_wait(step):
        face_copy(step, True).wait_recv()

    sum_peers = (peer_core, peer_x, peer_y, (fs, dp_pair), (fs, dp_far))

    def sum_copy(step):
        return side(14 + step, small_sum.at[step], small_land.at[step], sum_peers[step])

    def sum_start(step):
        sum_copy(step).start()

    def sum_wait(step):
        sum_copy(step).wait_recv()
        small_sum[step + 1] = small_sum[step] + small_land[step]

    def grad(unit, rows):
        if unit == D_UNIT:
            return sdn.at[rows, :]
        if unit >= 4:
            return act.at[rows, pl.ds(768 * (unit - 4), 768)]
        return wts.at[4 + unit, rows, :]

    def shape_of(unit):
        return 384 if unit == D_UNIT else 96

    def piece_shard(delta, which):
        chip_x = (xb + delta % 2) - 2 * xb * (delta % 2)
        chip_y = (yb + delta // 2) - 2 * yb * (delta // 2)
        return (chip_y * 2 + chip_x) * 2 + which

    def piece(unit, delta, which, part=None):
        size = shape_of(unit)
        shard = piece_shard(delta, which)
        if part is None:
            return grad(unit, span(size * shard, size))
        return grad(unit, span(size * shard + (size // 2) * part, size // 2))

    def lands(pair, unit, slot):
        wide, down_only = pair
        return down_only.at[slot] if unit == D_UNIT else wide.at[unit, slot]

    def accumulate(dst, *sources):
        rows = dst.shape[0]

        def body(i, carry):
            r = span(i * 48, 48)
            value = dst[r, :].astype(F32)
            for source in sources:
                value = value + source[r, :].astype(F32)
            dst[r, :] = value.astype(BF)
            return carry

        lax.fori_loop(0, rows // 48, body, 0)

    def core_copy(unit, delta):
        return pltpu.make_async_remote_copy(
            src_ref=piece(unit, delta, 1 - core),
            dst_ref=lands((lc, lcd), unit, delta),
            send_sem=core_send.at[unit, delta],
            recv_sem=core_recv.at[unit, delta],
            device_id=peer_core,
            device_id_type=MESH_ID,
        )

    def rs_core(unit):
        for delta in (3, 2, 1, 0):
            core_copy(unit, delta).start()

    xy_kinds = (
        (3, 0, (lx, lxd), 0, peer_x),
        (3, 1, (ly, lyd), 0, peer_y),
        (1, 0, (lx, lxd), 1, peer_x),
        (2, 1, (ly, lyd), 1, peer_y),
        (2, 0, (ly, lyd), 2, peer_y),
        (1, 1, (lx, lxd), 2, peer_x),
    )

    def xy_copy(unit, kind):
        delta, part, pair, slot, peer = xy_kinds[kind]
        return pltpu.make_async_remote_copy(
            src_ref=piece(unit, delta, core, part),
            dst_ref=lands(pair, unit, slot),
            send_sem=xy_send.at[unit, kind],
            recv_sem=xy_recv.at[unit, kind],
            device_id=peer,
            device_id_type=MESH_ID,
        )

    def rs_first_piece(unit, delta):
        core_copy(unit, delta).wait_recv()
        accumulate(piece(unit, delta, core), lands((lc, lcd), unit, delta))
        for kind in {3: (0, 1), 1: (2,), 2: (3,), 0: ()}[delta]:
            xy_copy(unit, kind).start()

    def rs_first(unit):
        for delta in (3, 2, 1, 0):
            rs_first_piece(unit, delta)

    def rs_second(unit):
        xy_copy(unit, 0).wait_recv()
        accumulate(piece(unit, 2, core, 0), lands((lx, lxd), unit, 0))
        xy_copy(unit, 4).start()
        xy_copy(unit, 1).wait_recv()
        accumulate(piece(unit, 1, core, 1), lands((ly, lyd), unit, 0))
        xy_copy(unit, 5).start()

    def z_copy(unit, index, src, slot, target):
        return pltpu.make_async_remote_copy(
            src_ref=src,
            dst_ref=lands((lz, lzd), unit, slot),
            send_sem=z_send.at[unit, index],
            recv_sem=z_recv.at[unit, slot],
            device_id=(fs, target),
            device_id_type=MESH_ID,
        )

    def z_land(unit, slot):
        return lands((lz, lzd), unit, slot)

    def z_wait(unit, slot):
        z_copy(unit, 0, z_land(unit, slot), slot, dp_pair).wait_recv()

    def z_out(unit, index):
        own_far = piece(unit, 0, core, far)
        own_near = piece(unit, 0, core, near)
        end = {
            0: (own_far, 1, dp_inner),
            1: (own_near, 0, dp_inner),
        }
        mid = {
            0: (own_far, 2, dp_mid),
            1: (z_land(unit, 2), 2, dp_end),
            2: (z_land(unit, 2), 3, dp_mid),
            3: (z_land(unit, 3), 3, dp_end),
        }
        return end.get(index), mid[index]

    def z_end(unit, index):
        return z_copy(unit, index, *z_out(unit, index)[0])

    def z_mid(unit, index):
        return z_copy(unit, index, *z_out(unit, index)[1])

    def rs_own(unit):
        for kind in (2, 3, 4, 5):
            xy_copy(unit, kind).wait_recv()
        accumulate(piece(unit, 0, core, 0), lands((lx, lxd), unit, 1), lands((ly, lyd), unit, 2))
        accumulate(piece(unit, 0, core, 1), lands((ly, lyd), unit, 1), lands((lx, lxd), unit, 2))

        @pl.when(is_end)
        def _():
            z_end(unit, 0).start()
            z_end(unit, 1).start()

    def rs_z2(unit):
        @pl.when(is_mid)
        def _():
            z_wait(unit, 1)
            accumulate(piece(unit, 0, core, far), z_land(unit, 1))
            z_mid(unit, 0).start()

    def rs_z3(unit):
        @pl.when(is_mid)
        def _():
            z_wait(unit, 0)
            z_wait(unit, 2)
            accumulate(z_land(unit, 2), z_land(unit, 0), piece(unit, 0, core, near))
            z_mid(unit, 1).start()
            z_mid(unit, 2).start()

    def rs_z4(unit):
        @pl.when(is_mid)
        def _():
            z_wait(unit, 3)
            z_mid(unit, 3).start()

    def result_copy(unit, slot):
        size = shape_of(unit) // 2
        rows = span(size * (near if slot == 2 else far), size)
        target = down_out.at[rows, :] if unit == D_UNIT else units_out.at[unit, rows, :]
        return pltpu.make_async_copy(z_land(unit, slot), target, local_sem.at[16 + 2 * unit + slot - 2])

    def rs_done(unit):
        @pl.when(is_end)
        def _():
            z_wait(unit, 2)
            z_wait(unit, 3)

        for slot in (2, 3):
            result_copy(unit, slot).start()

    for index in range(7):
        param_copy(index, fs).start()
    hook("start")

    img_h = gm
    img_k = att
    img_v = h1
    img_gain[0:2, :] = pgain_ref[...].astype(F32)
    img_gain[2:8, :] = pshift_ref[...].astype(F32)
    phidden = phidden_ref[...].astype(F32)
    for q in range(24):
        img_gain[8 + q // 6 : 9 + q // 6, 128 * (q % 6) : 128 * (q % 6) + 128] = phidden[q : q + 1, :]
    img_h[pl.ds(400, 112), :] = jnp.zeros((112, 768), BF)
    patches_copy.wait()

    def image_normed(values):
        return norm_rows(values)[0] * img_gain[0:1, :] + img_gain[6:7, :]

    first_rows = img_h[pl.ds(512, 16), :].astype(F32)[0:8, :]
    face_rows[0] = first_rows
    face_rows[1] = image_normed(first_rows)

    def image_norm(i):
        img_h[span(80 * i, 80), :] = image_normed(img_h[span(512 + 80 * i, 80), :].astype(F32)).astype(BF)

    loop(5, image_norm)
    pqkv_copy.wait()

    def image_kv(i):
        r = span(i * TILE, TILE)
        img_k[r, :] = nn(img_h[r, :], act[pl.ds(0, 768), pl.ds(768, 768)]).astype(BF)
        img_v[r, :] = (nn(img_h[r, :], act[pl.ds(0, 768), pl.ds(1536, 768)]) + img_gain[3:4, :]).astype(BF)

    loop(2, image_kv)
    hook("keys")

    lane_head = lax.broadcasted_iota(jnp.int32, (8, 768), 1) // 64
    img_q = (nn(face_rows[1].astype(BF), act[pl.ds(0, 768), pl.ds(0, 768)]) + img_gain[2:3, :]) * 0.125
    img_q = img_q.astype(BF).astype(F32)
    stacked = jnp.concatenate([jnp.where(lane_head == h, img_q, 0.0) for h in range(12)], axis=0).astype(BF)
    scores = nt(stacked, img_k[pl.ds(0, 512), :])
    token = lax.broadcasted_iota(jnp.int32, (96, 512), 1)
    image_of = lax.broadcasted_iota(jnp.int32, (96, 512), 0) % 8
    scores = jnp.where((token % 8 == image_of) & (token < 400), scores, -1e30)
    expd = jnp.exp(scores - jnp.max(scores, axis=-1, keepdims=True))
    probs = (expd / jnp.sum(expd, axis=-1, keepdims=True)).astype(BF)
    mixed = nn(probs, img_v[pl.ds(0, 512), :])
    joined = jnp.zeros((8, 768), F32)
    for h in range(12):
        joined = joined + jnp.where(lane_head == h, mixed[8 * h : 8 * h + 8, :], 0.0)
    hook("mixed")
    pout_copy.wait()
    middle = face_rows[0] + (nn(joined.astype(BF), act[pl.ds(0, 768), pl.ds(2304, 768)]) + img_gain[4:5, :])
    scaled, _ = norm_rows(middle)
    normed = (scaled * img_gain[1:2, :] + img_gain[7:8, :]).astype(BF)
    face_rows[0] = middle
    pup_copy.wait()
    for j in range(4):
        hidden = nn(normed, dg[pl.ds(0, 768), pl.ds(768 * j, 768)]) + img_gain[8 + j : 9 + j, :]
        face_rows[2 + j] = hidden * normal_cdf(hidden)
    hook("image")
    pdown_copy.wait()
    total = face_rows[0] + img_gain[5:6, :]
    for j in range(4):
        total = total + nn(face_rows[2 + j].astype(BF), sdn[pl.ds(768 * j, 768), :])
    unit_norm = total * lax.rsqrt(jnp.mean(total * total, axis=-1, keepdims=True) + 1e-06)
    faces[dp, fs] = unit_norm.astype(BF)
    face_start(0)
    for index in range(7):
        param_copy(index, others[index]).wait_recv()

    flat_small = small_in[...].reshape(128, 128).astype(BF)
    for r in range(4):
        lane = lax.broadcasted_iota(jnp.int32, (128, 384), 0)
        column = lax.broadcasted_iota(jnp.int32, (128, 384), 1)
        pick = jnp.where((column == lane + 96 * r) & (lane < 96), 1.0, 0.0).astype(BF)
        spread = nn(flat_small, pick)
        for block in range(2):
            shard = 4 * block + r
            value = spread[16 * shard : 16 * shard + 8, :]
            cols = slice(384 * block, 384 * block + 384)
            if r == 0:
                params[0:8, cols] = value
            else:
                params[0:8, cols] = params[0:8, cols] + value
    for shard in range(8):
        for q in range(3):
            at = 384 * (shard % 2) + 128 * q
            params[8 + shard // 2 : 9 + shard // 2, at : at + 128] = small_in[shard, 8 + q : 9 + q, :]

    x_copy.wait()
    for copy in own_copies:
        copy.wait()

    def first_norm(i):
        r = span(ROWS * i, ROWS)
        scaled, _ = norm_rows(h2[r, :].astype(F32))
        h1[r, :] = (scaled * params[0:1, :] + params[6:7, :]).astype(BF)

    loop(1024 // ROWS, first_norm)
    for group in range(8):
        rows = [segment_ref[2 * group + k : 2 * group + k + 1, :] + CAPS * (2 * group + k) for k in range(2)]
        same = lax.broadcasted_iota(jnp.int32, (64, 128), 0) == jnp.concatenate(rows, axis=1)
        member[:, 128 * group : 128 * group + 128] = jnp.where(same, 1.0, 0.0).astype(BF)
    face_wait(0)
    face_start(1)
    hook("norm")

    def project(j):
        def body(i):
            r = span(TILE * i, TILE)
            value = nn(h1[r, :], wts[j])
            if j == 0:
                value = (value + params[2:3, :]) * 0.125
            if j == 2:
                value = value + params[3:4, :]
            qkv[r, pl.ds(768 * j, 768)] = value.astype(BF)

        loop(4, body)

    ready(0)
    project(0)
    hook("project0")
    ready(1)
    project(1)
    hook("project1")
    ready(2)
    project(2)
    face_wait(1)
    face_start(2)

    low_lane = lax.broadcasted_iota(jnp.int32, (128, 128), 1) < 64
    zero_block = jnp.zeros((128, 128), BF)

    def split_heads(block):
        return jnp.concatenate(
            [jnp.where(low_lane, block, zero_block), jnp.where(low_lane, zero_block, block)], axis=0
        )

    def join_heads(value):
        return jnp.where(low_lane, value[0:128, :], value[128:256, :])

    def same_caption(group):
        part = member[:, span(128 * group, 128, 128)]
        same = tn(part, part)
        return jnp.concatenate([same, same], axis=0) > 0.5

    def attention_probs(same, queries, keys):
        value = jnp.where(same, nt(queries, keys), -1e30)
        expd = jnp.exp(value - jnp.max(value, axis=-1, keepdims=True))
        return expd * (1.0 / jnp.sum(expd, axis=-1, keepdims=True))

    def attend(group):
        r = span(128 * group, 128)
        same = same_caption(group)
        for hp in range(6):
            queries = split_heads(qkv[r, pl.ds(128 * hp, 128)])
            probs = attention_probs(same, queries, qkv[r, pl.ds(768 + 128 * hp, 128)])
            mixed = nn(probs.astype(BF), qkv[r, pl.ds(1536 + 128 * hp, 128)])
            att[r, pl.ds(128 * hp, 128)] = join_heads(mixed).astype(BF)

    hook("project2")
    loop(8, attend, {i: [lambda i=i: hook(f"attend{i}")] for i in range(8)})
    face_wait(2)
    face_start(3)
    ready(3)

    def out_project(i):
        r = span(TILE * i, TILE)
        x1[r, :] = h2[r, :].astype(F32) + (nn(att[r, :], wts[3]) + params[4:5, :])

    loop(4, out_project)
    hook("out")

    def second_norm(i):
        r = span(ROWS * i, ROWS)
        scaled, _ = norm_rows(x1[r, :])
        h2[r, :] = (scaled * params[1:2, :] + params[7:8, :]).astype(BF)

    loop(1024 // ROWS, second_norm)
    hook("norm2")
    face_wait(3)
    face_start(4)
    face_start(5)

    def widen(j):
        def body(i):
            r = span(TILE * i, TILE)
            for at in range(0, 768, 256):
                hidden = nn(h2[r, :], wts[4 + j, :, pl.ds(at, 256)]) + params[8 + j : 9 + j, at : at + 256]
                cdf = normal_cdf(hidden)
                cols = pl.ds(768 * j + at, 256)
                act[r, cols] = (hidden * cdf).astype(BF)
                slope = cdf + hidden * (jnp.exp(-0.5 * hidden * hidden) * (1.0 / math.sqrt(2.0 * math.pi)))
                dg[r, cols] = slope.astype(BF)

        loop(4, body)

    for j in range(4):
        ready(4 + j)
        widen(j)
        hook(f"widen{j}")
    face_wait(4)
    face_start(6)

    for jd in range(3):
        ready(8 + jd)
        cols = pl.ds(256 * jd, 256)

        def narrow(i, cols=cols, jd=jd):
            r = span(TILE * i, TILE)
            value = nn(act[r, :], wdn[:, cols]) + params[5:6, 256 * jd : 256 * jd + 256]
            value = x1[r, cols] + value
            top = value.astype(BF)
            rest = (value - top.astype(F32)).astype(BF)
            lanes = span(TILE * i, TILE, 128)
            piece_sum = nn(member[:, lanes], top) + nn(member[:, lanes], rest)

            @pl.when(i == 0)
            def _():
                pooled[:, cols] = piece_sum

            @pl.when(i > 0)
            def _():
                pooled[:, cols] = pooled[:, cols] + piece_sum

        loop(4, narrow)

    face_wait(5)
    face_wait(6)

    count = jnp.sum(member[...].astype(F32), axis=-1, keepdims=True)
    mean_rows = pooled[...] / count
    inverse = lax.rsqrt(jnp.mean(mean_rows * mean_rows, axis=-1, keepdims=True) + 1e-06)
    embed = mean_rows * inverse
    face_all = faces[...].astype(F32).reshape(256, 768).astype(BF)
    amount = sharp_ref[0] * (1.0 / math.sqrt(768.0))
    match = amount * nt(embed.astype(BF), face_all) + offset_ref[0]
    slot = lax.broadcasted_iota(jnp.int32, (64, 256), 1)
    image_id = ((slot // 8) % 8) * 32 + (slot // 64) * 8 + slot % 8
    diagonal = lax.broadcasted_iota(jnp.int32, (64, 64), 0) == lax.broadcasted_iota(jnp.int32, (64, 64), 1)
    described = jnp.where(diagonal, described_ref[...].astype(F32), 0.0)
    positive = jnp.sum(described, axis=-1, keepdims=True) == image_id.astype(F32)
    signed = jnp.where(positive, -match, match)
    terms = jnp.maximum(signed, 0.0) + jnp.log1p(jnp.exp(-jnp.abs(signed)))
    row_loss = jnp.sum(terms, axis=-1, keepdims=True) * (1.0 / 256.0)
    loss_out[...] = jnp.sum(jnp.where(diagonal, row_loss, 0.0), axis=0, keepdims=True)
    slope = ((jax.nn.sigmoid(match) - jnp.where(positive, 1.0, 0.0)) * amount).astype(BF)
    grad_embed = nn(slope, face_all)
    grad_pooled = inverse * (grad_embed - embed * jnp.mean(grad_embed * embed, axis=-1, keepdims=True))
    per_caption = grad_pooled / count
    caption_hi[...] = per_caption.astype(BF)
    caption_lo[...] = (per_caption - caption_hi[...].astype(F32)).astype(BF)

    def spread_down(i):
        gm[span(TILE * i, TILE), :] = tn(member[:, span(TILE * i, TILE, 128)], caption_hi[...]).astype(BF)

    loop(4, spread_down)

    ag_drain()
    for index in range(7):
        param_copy(index, fs).wait_send()
    for step in range(7):
        face_copy(step, False).wait_send()

    ones = jnp.ones((16, 1024), BF)

    def column_sum(value):
        return nn(ones, value)[0:1, :]

    def down_piece(delta):
        def body(i):
            which = (1 - core) + i * (2 * core - 1)
            shard = piece_shard(delta, which)
            sdn[span(384 * shard, 384), :] = tn(act[:, span(384 * shard, 384, 128)], gm[...]).astype(BF)

            @pl.when(i == 0)
            def _():
                core_copy(D_UNIT, delta).start()

        loop(2, body)

    down_piece(3)
    down_piece(2)
    rs_first_piece(D_UNIT, 3)
    down_piece(1)
    rs_first_piece(D_UNIT, 2)
    down_piece(0)
    rs_first_piece(D_UNIT, 1)
    rs_first_piece(D_UNIT, 0)

    def hidden_back(i):
        r = span(TILE * i, TILE)
        for jj in range(3):
            cols = pl.ds(1024 * jj, 1024)
            value = nt(gm[r, :], wdn[pl.ds(1024 * jj, 1024), :])
            dg[r, cols] = (dg[r, cols].astype(F32) * value).astype(BF)

    loop(4, hidden_back, {1: [lambda: rs_second(D_UNIT)]})
    partial_rows = {}

    def up_unit(j):
        def body(i):
            act[span(TILE * i, TILE), pl.ds(768 * j, 768)] = tn(
                h2[:, span(TILE * i, TILE, 128)], dg[:, pl.ds(768 * j, 768)]
            ).astype(BF)

        loop(3, body)
        rs_core(4 + j)
        small_sum[0, 8 + j : 9 + j, :] = column_sum(dg[:, pl.ds(768 * j, 768)])

    up_unit(0)
    up_unit(1)
    rs_first(4)
    up_unit(2)
    rs_first(5)
    up_unit(3)
    rs_first(6)
    rs_own(D_UNIT)
    small_sum[0, 5:6, :] = column_sum(gm[...])
    partial[...] = jnp.zeros((4, 8, 768), F32)

    def fold(value):
        return value.reshape(value.shape[0] // 8, 8, 768).sum(axis=0)

    def middle_back(i):
        r = span(TILE * i, TILE)
        total = nt(dg[r, pl.ds(0, 768)], wts[4])
        for j in range(1, 4):
            total = total + nt(dg[r, pl.ds(768 * j, 768)], wts[4 + j])
        work[...] = total
        low[...] = tn(member[:, span(TILE * i, TILE, 128)], caption_lo[...]).astype(BF)

        def rows_back(k):
            inner = span(ROWS * k, ROWS)
            outer = span(TILE * i + ROWS * k, ROWS)
            upstream = work[inner, :]
            scaled, inverse = norm_rows(x1[outer, :])
            partial[0] = partial[0] + fold(upstream * scaled)
            partial[1] = partial[1] + fold(upstream)
            weighted = upstream * params[1:2, :]
            first_mean = jnp.mean(weighted, axis=-1, keepdims=True)
            second_mean = jnp.mean(weighted * scaled, axis=-1, keepdims=True)
            value = gm[outer, :].astype(F32) + low[inner, :].astype(F32)
            value = value + inverse * (weighted - first_mean - scaled * second_mean)
            x1[outer, :] = value
            gm[outer, :] = value.astype(BF)

        loop(TILE // ROWS, rows_back)

    loop(
        4,
        middle_back,
        {
            0: [lambda: rs_first(7)],
            1: [lambda: rs_second(4)],
            2: [lambda: rs_z2(D_UNIT)],
            3: [lambda: rs_second(5)],
        },
    )
    x_again = pltpu.make_async_copy(x_hbm, h2, local_sem.at[15])
    x_again.start()

    def out_unit(i):
        wts[7, span(TILE * i, TILE), :] = tn(att[:, span(TILE * i, TILE, 128)], gm[...]).astype(BF)

    loop(3, out_unit)
    rs_core(3)
    small_sum[0, 4:5, :] = column_sum(gm[...])

    def attended_back(i):
        r = span(TILE * i, TILE)
        att[r, :] = nt(gm[r, :], wts[3]).astype(BF)

    loop(4, attended_back)
    rs_second(6)
    rs_first(3)
    rs_own(4)
    rs_z3(D_UNIT)

    def attend_back(quad):
        def chain(group, same, half):
            r = span(128 * group, 128)
            at = 256 * quad + 128 * half
            qs = pl.ds(at, 128)
            queries = split_heads(qkv[r, qs])
            keys = qkv[r, pl.ds(768 + at, 128)]
            upstream = split_heads(att[r, qs])
            probs = attention_probs(same, queries, keys)
            probs_grad = nt(upstream, qkv[r, pl.ds(1536 + at, 128)])
            inner = jnp.sum(probs * probs_grad, axis=-1, keepdims=True)
            score_grad = (probs * (probs_grad - inner)).astype(BF)
            to = 768 * quad + 128 * half
            dg[r, pl.ds(to + 512, 128)] = tn(probs.astype(BF), upstream).astype(BF)
            dg[r, pl.ds(to + 256, 128)] = tn(score_grad, queries).astype(BF)
            query_grad = join_heads(nn(score_grad, keys)).astype(BF).astype(F32)
            dg[r, pl.ds(to, 128)] = (query_grad * 0.125).astype(BF)

        def body(i):
            for group in range(GROUPS):
                same = same_caption(GROUPS * i + group)
                for half in range(2):
                    chain(GROUPS * i + group, same, half)

        return body

    def qkv_unit(quad):
        def body(i):
            wts[4 + quad, span(TILE * i, TILE), :] = tn(
                h1[:, span(TILE * i, TILE, 128)], dg[:, pl.ds(768 * quad, 768)]
            ).astype(BF)

        loop(3, body)
        rs_core(quad)

    loop(
        8 // GROUPS,
        attend_back(0),
        {
            1: [lambda: rs_z2(4), lambda: rs_own(5), lambda: rs_second(7)],
            3: [lambda: rs_z2(5), lambda: rs_z3(4), lambda: rs_own(6), lambda: rs_second(3)],
        },
    )
    qkv_unit(0)
    loop(
        8 // GROUPS,
        attend_back(1),
        {
            0: [lambda: rs_first(0)],
            1: [lambda: rs_z4(D_UNIT), lambda: rs_z2(6), lambda: rs_z3(5), lambda: rs_own(7)],
            3: [lambda: rs_second(0), lambda: rs_z2(7), lambda: rs_z3(6), lambda: rs_z4(4), lambda: rs_own(3)],
        },
    )
    qkv_unit(1)
    loop(
        8 // GROUPS,
        attend_back(2),
        {
            0: [lambda: rs_first(1), lambda: rs_z2(3)],
            1: [lambda: rs_own(0), lambda: rs_z3(7), lambda: rs_z4(5)],
            3: [lambda: rs_second(1), lambda: rs_z2(0), lambda: rs_z3(3), lambda: rs_z4(6)],
        },
    )
    qkv_unit(2)
    rs_own(1)
    rs_z3(0)
    rs_z4(7)
    rs_first(2)
    for quad in range(3):
        to = slice(256 * quad, 256 * quad + 256)
        small_sum[0, 2:3, to] = column_sum(dg[:, pl.ds(768 * quad, 256)])
        small_sum[0, 3:4, to] = column_sum(dg[:, pl.ds(768 * quad + 512, 256)])
    x_again.wait()

    def input_back(i):
        r = span(TILE * i, TILE)
        total = jnp.zeros((TILE, 768), F32)
        for quad in range(3):
            for j in range(3):
                part = dg[r, pl.ds(768 * quad + 256 * j, 256)]
                total = total + nt(part, wts[j, :, pl.ds(256 * quad, 256)])
        work[...] = total

        def rows_back(k):
            inner = span(ROWS * k, ROWS)
            outer = span(TILE * i + ROWS * k, ROWS)
            upstream = work[inner, :]
            scaled, inverse = norm_rows(h2[outer, :].astype(F32))
            partial[2] = partial[2] + fold(upstream * scaled)
            partial[3] = partial[3] + fold(upstream)
            weighted = upstream * params[0:1, :]
            first_mean = jnp.mean(weighted, axis=-1, keepdims=True)
            second_mean = jnp.mean(weighted * scaled, axis=-1, keepdims=True)
            value = x1[outer, :] + inverse * (weighted - first_mean - scaled * second_mean)
            att[outer, :] = value.astype(BF)

        loop(TILE // ROWS, rows_back)

    loop(
        4,
        input_back,
        {
            0: [lambda: rs_second(2), lambda: rs_z2(1), lambda: rs_z4(3)],
            1: [lambda: rs_own(2), lambda: rs_z4(0)],
            2: [lambda: rs_z3(1)],
            3: [lambda: rs_z2(2)],
        },
    )
    input_copy = pltpu.make_async_copy(att, input_out, local_sem.at[34])
    input_copy.start()
    for row, index in ((0, 2), (1, 0), (6, 3), (7, 1)):
        small_sum[0, row : row + 1, :] = jnp.sum(partial[index], axis=0, keepdims=True)
    small_sum[0, 12:16, :] = jnp.zeros((4, 768), F32)
    sum_start(0)
    rs_z4(1)
    rs_z3(2)
    sum_wait(0)
    sum_start(1)
    for unit in (D_UNIT, 4, 5, 6, 7, 3, 0):
        rs_done(unit)
    sum_wait(1)
    sum_start(2)
    rs_z4(2)
    sum_wait(2)
    sum_start(3)
    rs_done(1)
    sum_wait(3)
    sum_start(4)
    rs_done(2)
    sum_wait(4)
    small_out[...] = small_sum[5]

    input_copy.wait()
    for unit in range(9):
        for slot in (2, 3):
            result_copy(unit, slot).wait()
        for delta in range(4):
            core_copy(unit, delta).wait_send()
        for kind in range(6):
            xy_copy(unit, kind).wait_send()

        @pl.when(is_end)
        def _(unit=unit):
            for index in range(2):
                z_end(unit, index).wait_send()

        @pl.when(is_mid)
        def _(unit=unit):
            for index in range(4):
                z_mid(unit, index).wait_send()

    for step in range(5):
        sum_copy(step).wait_send()


def finish_kernel(
    units_hbm,
    down_hbm,
    input_hbm,
    small_ref,
    loss_ref,
    qkv_out,
    out_out,
    up_out,
    down_out,
    gain_out,
    shift_out,
    hidden_out,
    input_out,
    loss_out,
    units,
    down,
    tokens,
    qkv,
    out,
    up,
    down_wide,
    sem,
):
    fs = lax.axis_index("fsdp")

    def move(src, dst, index):
        copy = pltpu.make_async_copy(src, dst, sem.at[index])
        copy.start()
        return copy

    tokens_in = move(input_hbm, tokens, 2)
    units_in = move(units_hbm, units, 0)
    down_in = move(down_hbm, down, 1)
    for shard in range(8):

        @pl.when(fs == shard)
        def _(shard=shard):
            gain_out[...] = small_ref[0:2, 96 * shard : 96 * shard + 96]
            shift_out[...] = small_ref[2:8, 96 * shard : 96 * shard + 96]
            for q in range(3):
                at = 384 * (shard % 2) + 128 * q
                hidden_out[q : q + 1, :] = small_ref[8 + shard // 2 : 9 + shard // 2, at : at + 128]

    loss_out[...] = loss_ref[...]
    tokens_in.wait()
    moves = [move(tokens, input_out, 7)]
    units_in.wait()
    for quad in range(3):
        for j in range(3):
            at = 768 * j + 256 * quad
            qkv[:, at : at + 256] = units[quad, :, 256 * j : 256 * j + 256].astype(F32)
    moves.append(move(qkv, qkv_out, 3))
    out[...] = units[3].astype(F32)
    moves.append(move(out, out_out, 4))
    for j in range(4):
        up[:, 768 * j : 768 * j + 768] = units[4 + j].astype(F32)
    moves.append(move(up, up_out, 5))
    down_in.wait()
    down_wide[...] = down[...].astype(F32)
    moves.append(move(down_wide, down_out, 6))
    for copy in moves:
        copy.wait()


def fused_step(
    incoming_word_states,
    sentence_number_per_word,
    described_picture,
    lookup_matrices,
    mixer_exit_matrix,
    widening_matrix,
    narrowing_matrix,
    normalizer_multipliers,
    word_offsets,
    widened_offset,
    picture_patches,
    picture_lookup_matrices,
    picture_mixer_exit_matrix,
    picture_widening_matrix,
    picture_narrowing_matrix,
    picture_normalizer_multipliers,
    picture_offsets,
    picture_widened_offset,
    sharpness_coefficient,
    objective_offset,
):
    rows, length, width = incoming_word_states.shape
    tokens = rows * length
    vmem = pl.BlockSpec(memory_space=pltpu.VMEM)
    hbm = pl.BlockSpec(memory_space=pl.ANY)
    smem = pl.BlockSpec(memory_space=pltpu.SMEM)
    dma = pltpu.SemaphoreType.DMA
    outs = pl.pallas_call(
        fused_kernel,
        out_shape=(
            jax.ShapeDtypeStruct((8, 96, width), BF),
            jax.ShapeDtypeStruct((384, width), BF),
            jax.ShapeDtypeStruct((tokens, width), BF),
            jax.ShapeDtypeStruct((16, width), F32),
            jax.ShapeDtypeStruct((1, 64), F32),
        ),
        in_specs=[smem, smem, hbm, vmem, vmem, *[hbm] * 4, *[vmem] * 3, *[hbm] * 5, *[vmem] * 3],
        out_specs=(hbm, hbm, hbm, vmem, vmem),
        scratch_shapes=[
            pltpu.VMEM((8, 768, 768), BF),
            pltpu.VMEM((3072, 768), BF),
            pltpu.VMEM((1024, 768), BF),
            pltpu.VMEM((1024, 2304), BF),
            pltpu.VMEM((1024, 768), BF),
            pltpu.VMEM((1024, 768), F32),
            pltpu.VMEM((1024, 768), BF),
            pltpu.VMEM((1024, 3072), BF),
            pltpu.VMEM((1024, 3072), BF),
            pltpu.VMEM((1024, 768), BF),
            pltpu.VMEM((3072, 768), BF),
            pltpu.VMEM((8, 4, 96, 768), BF),
            pltpu.VMEM((4, 384, 768), BF),
            pltpu.VMEM((8, 3, 48, 768), BF),
            pltpu.VMEM((3, 192, 768), BF),
            pltpu.VMEM((8, 3, 48, 768), BF),
            pltpu.VMEM((3, 192, 768), BF),
            pltpu.VMEM((8, 4, 48, 768), BF),
            pltpu.VMEM((4, 192, 768), BF),
            pltpu.VMEM((TILE, 768), F32),
            pltpu.VMEM((TILE, 768), BF),
            pltpu.VMEM((4, 8, 8, 768), BF),
            pltpu.VMEM((8, 16, 128), F32),
            pltpu.VMEM((16, 768), F32),
            pltpu.VMEM((16, 768), F32),
            pltpu.VMEM((64, 1024), BF),
            pltpu.VMEM((64, 768), F32),
            pltpu.VMEM((64, 768), BF),
            pltpu.VMEM((64, 768), BF),
            pltpu.VMEM((4, 8, 768), F32),
            pltpu.VMEM((6, 16, 768), F32),
            pltpu.VMEM((5, 16, 768), F32),
            pltpu.VMEM((6, 8, 768), F32),
            dma((N_AG, 13)),
            dma((N_AG, 13)),
            dma((9, 4)),
            dma((9, 4)),
            dma((9, 6)),
            dma((9, 6)),
            dma((9, 4)),
            dma((9, 4)),
            dma((21,)),
            dma((21,)),
            dma((35,)),
        ],
        compiler_params=pltpu.CompilerParams(
            collective_id=0, has_side_effects=True, vmem_limit_bytes=67043328
        ),
        name="lit_step",
    )(
        sharpness_coefficient,
        objective_offset,
        incoming_word_states.reshape(tokens, width),
        sentence_number_per_word,
        described_picture.reshape(1, -1),
        lookup_matrices,
        mixer_exit_matrix,
        widening_matrix,
        narrowing_matrix,
        normalizer_multipliers,
        word_offsets,
        widened_offset.reshape(3, 128),
        picture_patches.transpose(1, 0, 2).reshape(-1, width),
        picture_lookup_matrices,
        picture_mixer_exit_matrix,
        picture_widening_matrix,
        picture_narrowing_matrix,
        picture_normalizer_multipliers,
        picture_offsets,
        picture_widened_offset.reshape(24, 128),
    )
    finished = pl.pallas_call(
        finish_kernel,
        out_shape=(
            jax.ShapeDtypeStruct((96, 2304), F32),
            jax.ShapeDtypeStruct((96, width), F32),
            jax.ShapeDtypeStruct((96, 3072), F32),
            jax.ShapeDtypeStruct((384, width), F32),
            jax.ShapeDtypeStruct((2, 96), F32),
            jax.ShapeDtypeStruct((6, 96), F32),
            jax.ShapeDtypeStruct((3, 128), F32),
            jax.ShapeDtypeStruct((tokens, width), BF),
            jax.ShapeDtypeStruct((1, 64), F32),
        ),
        in_specs=[hbm, hbm, hbm, vmem, vmem],
        out_specs=(hbm, hbm, hbm, hbm, vmem, vmem, vmem, hbm, vmem),
        scratch_shapes=[
            pltpu.VMEM((8, 96, width), BF),
            pltpu.VMEM((384, width), BF),
            pltpu.VMEM((tokens, width), BF),
            pltpu.VMEM((96, 2304), F32),
            pltpu.VMEM((96, width), F32),
            pltpu.VMEM((96, 3072), F32),
            pltpu.VMEM((384, width), F32),
            dma((8,)),
        ],
        compiler_params=pltpu.CompilerParams(vmem_limit_bytes=60 * 2**20),
        name="lit_finish",
    )(*outs)
    finished = list(finished)
    finished[6] = finished[6].reshape(-1)
    finished[7] = finished[7].reshape(rows, length, width)
    finished[8] = finished[8].reshape(-1)
    return tuple(finished)


def solution(mesh):
    fits = mesh.shape["fsdp"] == 8 and mesh.shape["dp"] == 4
    return jax.shard_map(
        fused_step if fits else per_device,
        mesh=mesh,
        in_specs=(
            P(("fsdp", "dp"), None, None),
            P(("fsdp", "dp"), None),
            P(("fsdp", "dp")),
            P("fsdp", None),
            P("fsdp", None),
            P("fsdp", None),
            P("fsdp", None),
            P(None, "fsdp"),
            P(None, "fsdp"),
            P("fsdp"),
            P(("fsdp", "dp"), None, None),
            P(),
            P(),
            P(),
            P(),
            P(),
            P(),
            P(),
            P(),
            P(),
        ),
        out_specs=(
            P("fsdp", None),
            P("fsdp", None),
            P("fsdp", None),
            P("fsdp", None),
            P(None, "fsdp"),
            P(None, "fsdp"),
            P("fsdp"),
            P(("fsdp", "dp"), None, None),
            P(("fsdp", "dp")),
        ),
        check_vma=False,
    )
```
